32 devices in a mesh: gx: 8 (over z, y), yz: 4 (over x, core).
Axes of the slice: x: 2, y: 2, z: 4, core: 2. Of those that a mesh axis runs over, the one named last changes fastest.
Arguments:
- solvent_vel: float32 [3, 256, 128, 2, 128], P(None, 'gx', 'yz'), may hold values from -6 to 6
- occupancy: int32 [256, 128, 128], P('gx', 'yz'), may hold values from 0 to 2
- grid_shift: int32 [3], replicated, may hold values from 1 to 3
- axis_index: int32 [64, 32, 64], P('gx', 'yz'), may hold values from 0 to 63
- colloid_pos: float32 [3, 8, 4, 128], P(None, 'gx', 'yz'), may hold values from 0 to 64, as said below
- colloid_vel: float32 [3, 8, 4, 128], P(None, 'gx', 'yz'), may hold values from -6 to 6
- colloid_mass: float32 [8, 4, 128], P('gx', 'yz'), may hold values from 2 to 20
- colloid_count: int32 [8, 4], P('gx', 'yz'), may hold values from 21 to 128, as said below
Outputs:
- solvent_out: float32 [3, 256, 128, 2, 128], P(None, 'gx', 'yz')
- colloid_pos_out: float32 [3, 8, 4, 128], P(None, 'gx', 'yz')
- colloid_vel_out: float32 [3, 8, 4, 128], P(None, 'gx', 'yz')
The draws below stay inside these ranges and needn't reach their ends.
Inputs may be any that keep to these rules, and one draw needn't show every extreme that they name: `colloid_pos`: component 0 lies in [0, 8), component 1 in [0, 8), component 2 in [0, 64). `colloid_count`: some device holds 128 live colloids in every draw.
All inputs are finite; a program needn't handle non-finite values.
Results may differ from the reference program's by a relative error of at most 0.0003.
Values sent between devices are 32-bit elements; how exact they have to be, the bound alone decides.
A program may use at most 320 MiB of HBM per device.

```python
import math
import jax
import jax.numpy as jnp
from jax import lax

CX = 8
CY = 8
CZ = 64
CMAX = 128
SUB = 4
SLOTS = 2
SUBSTEPS = 4
DIRECTIONS = 64
FX = 32
FY = 32
FZ = 128
NXF = 256
NYF = 128
NX = 64
NY = 32
N_GX = 8
N_YZ = 4


def draw_occupancy(key, part):
    block = 2 * SUB
    blocks_x = (NXF + block - 1) // block
    blocks_y = (NYF + block - 1) // block
    blocks_z = (FZ + 7) // 8
    slots_used = jax.random.randint(jax.random.fold_in(key, 21), (NXF, NYF, FZ), 0, SLOTS + 1)
    sparse = jax.random.randint(jax.random.fold_in(key, 22), (blocks_x * blocks_y * blocks_z,), 0, 4) == 0
    chosen = jax.random.randint(jax.random.fold_in(key, 23), (), 0, blocks_x * blocks_y * blocks_z)
    sparse = jnp.logical_or(sparse, jnp.arange(blocks_x * blocks_y * blocks_z) == chosen)
    sparse = sparse.reshape(blocks_x, blocks_y, blocks_z)
    spread = jnp.repeat(jnp.repeat(jnp.repeat(sparse, block, axis=0), block, axis=1), 8, axis=2)[:NXF, :NYF, :FZ]
    thin_keep = jax.random.randint(jax.random.fold_in(key, 24), (NXF, NYF, FZ), 0, 4) == 0
    keeping = jnp.logical_or(jnp.logical_not(spread), thin_keep)
    return jnp.where(keeping, slots_used, 0).astype(jnp.int32)


def draw_colloid_pos(key, part):
    unit = jax.random.uniform(jax.random.fold_in(key, 5), (3, N_GX, N_YZ, CMAX), jnp.float32)
    extent = jnp.array([CX, CY, CZ], jnp.float32)
    return unit * extent[:, None, None, None] * 0.999


def draw_colloid_count(key, part):
    devices = N_GX * N_YZ
    counts = jax.random.randint(jax.random.fold_in(key, 11), (devices,), CMAX // 6, CMAX // 2 + 1)
    chosen = jax.random.randint(jax.random.fold_in(key, 12), (), 0, devices)
    counts = jnp.where(jnp.arange(devices) == chosen, CMAX, counts)
    return counts.reshape(N_GX, N_YZ).astype(jnp.int32)


def touch_ends(entries, rng, low, high):
    dims = entries.shape
    index_at = [jax.random.randint(jax.random.fold_in(rng, axis), (), 0, dims[axis]) for axis in range(len(dims))]
    entries = entries.at[tuple(index_at)].set(low)
    longest = dims.index(max(dims))
    index_at[longest] = (index_at[longest] + 1) % dims[longest]
    return entries.at[tuple(index_at)].set(high)


def block_levels(key, dims, cuts, low, high):
    def one(dim, parts):
        draws = jax.random.uniform(jax.random.fold_in(jax.random.fold_in(key, 6), dim), (parts,), jnp.float32, low / len(cuts), high / len(cuts))
        return jnp.repeat(jnp.exp(draws), dims[dim] // parts).reshape((-1,) + (1,) * (len(dims) - dim - 1))

    loudness = one(*cuts[0])
    for cut in cuts[1:]:
        loudness = loudness * one(*cut)
    return loudness


def noise(stream_key, dims, scale, bound, split=(), dtype=jnp.bfloat16):
    loudness = block_levels(stream_key, dims, split, -0.22, 0.18) if split else 1.0
    values = jax.random.normal(stream_key, dims, jnp.float32) * scale * loudness
    return jnp.minimum(jnp.maximum(values, -bound), bound).astype(dtype)


def setup_inputs(seed: int = 0) -> dict:
    key_of = jax.random.split(jax.random.key(seed), 9)
    solvent_vel = noise(key_of[0], (3, NXF, NYF, SLOTS, FZ), 1.0, 6.0, ((1, 8), (2, 4)), jnp.float32)
    occupancy = draw_occupancy(jax.random.fold_in(key_of[8], 71), 0)
    grid_shift = jax.random.randint(key_of[2], (3,), 1, SUB).astype(jnp.int32)
    axis_index = touch_ends(jax.random.randint(key_of[3], (NX, NY, CZ), 0, DIRECTIONS), jax.random.fold_in(key_of[3], 1), 0, DIRECTIONS - 1).astype(jnp.int32)
    colloid_pos = draw_colloid_pos(jax.random.fold_in(key_of[8], 71), 0)
    colloid_vel = noise(key_of[5], (3, N_GX, N_YZ, CMAX), 1.0, 6.0, ((1, 8), (2, 4)), jnp.float32)
    colloid_mass = jnp.clip(jnp.exp(math.log(20.0) - 2.3025851 * jax.random.uniform(key_of[6], (N_GX, N_YZ, CMAX), jnp.float32) ** block_levels(key_of[6], (N_GX, N_YZ, CMAX), ((0, 8), (1, 4)), -0.2, 0.2)), 2.0, 20.0)
    colloid_count = draw_colloid_count(jax.random.fold_in(key_of[8], 71), 0)
    return {"solvent_vel": solvent_vel, "occupancy": occupancy, "grid_shift": grid_shift, "axis_index": axis_index, "colloid_pos": colloid_pos, "colloid_vel": colloid_vel, "colloid_mass": colloid_mass, "colloid_count": colloid_count}


turn_angle = 130.0 * math.pi / 180.0
cos_angle = math.cos(turn_angle)
sin_angle = math.sin(turn_angle)
golden = math.pi * (3.0 - math.sqrt(5.0))
cutoff = 1.5
stiffness = 20.0
timestep = 0.05
fill_mass = 16.0

def directions(index):
    number = index.astype(jnp.float32)
    height = 1.0 - (2.0 * number + 1.0) / DIRECTIONS
    radius = jnp.sqrt(1.0 - height * height)
    phase = number * golden
    return jnp.stack([radius * jnp.cos(phase), radius * jnp.sin(phase), height])

def rotate(mean, axis, velocity):
    rel = velocity - mean
    cross = jnp.stack([axis[1] * rel[2] - axis[2] * rel[1], axis[2] * rel[0] - axis[0] * rel[2], axis[0] * rel[1] - axis[1] * rel[0]])
    along = lax.optimization_barrier(jnp.sum(axis * rel, axis=0))
    return mean + cos_angle * rel + sin_angle * cross + (1.0 - cos_angle) * along[None] * axis

def cell_fields(totals, axis_index):
    width_x, width_y, width_z = (totals.shape[1], totals.shape[2], totals.shape[3])
    cells_x, cells_y, cells_z = (width_x // SUB, width_y // SUB, width_z // 2)
    cell = totals.reshape(4, cells_x, SUB, cells_y, SUB, cells_z, 2).sum(axis=(2, 4, 6))
    mean = cell[:3] / jnp.maximum(cell[3], fill_mass)[None]
    both = jnp.concatenate([mean, directions(axis_index)])
    spread = jnp.broadcast_to(both[:, :, None, :, None, :, None], (6, cells_x, SUB, cells_y, SUB, cells_z, 2))
    return spread.reshape(6, width_x, width_y, width_z)

def pair_parts(own, other, other_live):
    diff_x = own[0][..., :, None] - other[0][..., None, :]
    diff_y = own[1][..., :, None] - other[1][..., None, :]
    height = own[2][..., :, None] - other[2][..., None, :]
    height = jnp.where(height > 0.5 * CZ, height - CZ, jnp.where(height < -0.5 * CZ, height + CZ, height))
    radius_sq = diff_x * diff_x + diff_y * diff_y + height * height
    reach = 1.0 - radius_sq / (cutoff * cutoff)
    weight = jnp.where(radius_sq < cutoff * cutoff, reach * reach, 0.0) * other_live[..., None, :]
    return (weight, diff_x, diff_y, height)

def pair_force(own, other, other_live):
    weight, diff_x, diff_y, height = pair_parts(own, other, other_live)
    return stiffness * jnp.stack([lax.optimization_barrier(jnp.sum(weight * diff_x, axis=-1)), lax.optimization_barrier(jnp.sum(weight * diff_y, axis=-1)), lax.optimization_barrier(jnp.sum(weight * height, axis=-1))])

def all_forces(position, alive):
    total = jnp.zeros_like(position)
    for step_x in (-1, 0, 1):
        for step_y in (-1, 0, 1):
            other = jnp.roll(position, (-step_x, -step_y), axis=(1, 2))
            other = jnp.stack([other[0] + step_x * CX, other[1] + step_y * CY, other[2]])
            other_live = jnp.roll(alive, (-step_x, -step_y), axis=(0, 1))
            total = total + pair_force(position, other, other_live)
    return total

def reference(solvent_vel, occupancy, grid_shift, axis_index, colloid_pos, colloid_vel, colloid_mass, colloid_count):
    nxf, nyf, nzf = occupancy.shape
    live = (lax.broadcasted_iota(jnp.int32, solvent_vel.shape[1:], 2) < occupancy[:, :, None, :]).astype(jnp.float32)
    moment = solvent_vel * live[None]
    alive = (lax.broadcasted_iota(jnp.int32, colloid_mass.shape, 2) < colloid_count[:, :, None]).astype(jnp.float32)
    row = lax.broadcasted_iota(jnp.int32, colloid_mass.shape, 0)
    column = lax.broadcasted_iota(jnp.int32, colloid_mass.shape, 1)
    cell_x = row * FX + jnp.clip(jnp.floor(colloid_pos[0] * SUB).astype(jnp.int32), 0, FX - 1)
    cell_y = column * FY + jnp.clip(jnp.floor(colloid_pos[1] * SUB).astype(jnp.int32), 0, FY - 1)
    cell_z = jnp.clip(jnp.floor(colloid_pos[2] * 2.0).astype(jnp.int32), 0, FZ - 1)
    flat = ((cell_x * nyf + cell_y) * nzf + cell_z).reshape(-1)
    weight = colloid_mass * alive
    values = jnp.concatenate([colloid_vel * weight[None], weight[None]]).reshape(4, -1)
    deposit = jnp.zeros((4, nxf * nyf * nzf), jnp.float32).at[:, flat].add(values).reshape(4, nxf, nyf, nzf)
    totals = jnp.concatenate([lax.optimization_barrier(jnp.sum(moment, axis=3)), lax.optimization_barrier(jnp.sum(live, axis=2))[None]]) + deposit
    forward = (grid_shift[0], grid_shift[1], grid_shift[2])
    backward = (-grid_shift[0], -grid_shift[1], -grid_shift[2])
    totals = jnp.roll(totals, forward, axis=(1, 2, 3))
    fields = jnp.roll(cell_fields(totals, axis_index), backward, axis=(1, 2, 3))
    turned = rotate(fields[:3, :, :, None], fields[3:, :, :, None], solvent_vel)
    solvent_out = jnp.where(live[None] > 0, turned, solvent_vel)
    picked = fields.reshape(6, -1)[:, flat].reshape((6,) + colloid_mass.shape)
    velocity = jnp.where(alive[None] > 0, rotate(picked[:3], picked[3:], colloid_vel), colloid_vel)
    position = colloid_pos
    for step in range(SUBSTEPS):
        force = all_forces(position, alive)
        velocity = velocity + timestep * force / colloid_mass[None]
        position = position + timestep * velocity
    keep = alive[None] > 0
    return (solvent_out, jnp.where(keep, position, colloid_pos), jnp.where(keep, velocity, colloid_vel))
```

```python
import functools
import math

import jax
import jax.numpy as jnp
from jax import lax
from jax.experimental import pallas as pl
from jax.experimental.pallas import tpu as pltpu
from jax.sharding import PartitionSpec as P

SUB = 4
SUBSTEPS = 4
DIRECTIONS = 64

turn_angle = 130.0 * math.pi / 180.0
cos_angle = math.cos(turn_angle)
sin_angle = math.sin(turn_angle)
golden = math.pi * (3.0 - math.sqrt(5.0))
cutoff = 1.5
stiffness = 20.0
timestep = 0.05
fill_mass = 16.0
far_away = 1.0e9
MESH = pl.DeviceIdType.MESH
f32 = jnp.float32
bf16 = jnp.bfloat16
AROUND = [(a, b) for a in (-1, 0, 1) for b in (-1, 0, 1) if (a, b) != (0, 0)]
OWN = 4


def iota(shape, dim):
    return lax.broadcasted_iota(jnp.int32, shape, dim)


def slot_of(a, b):
    return (a + 1) * 3 + b + 1


def terms(value, number):
    out = []
    for _ in range(number - 1):
        part = value.astype(bf16)
        out.append(part)
        value = value - part.astype(f32)
    return out + [value.astype(bf16)]


def dot(left, right, contract=((1,), (0,))):
    return lax.dot_general(left, right, (contract, ((), ())), preferred_element_type=f32)


def wrapped(value, size):
    return jnp.where(value >= size, value - size, value)


def layer_of(row, scale, width):
    return jnp.clip(jnp.floor(row * scale).astype(jnp.int32), 0, width - 1)


def fold(values):
    row = iota(values[0].shape, 0)
    low = row < 4
    values = [
        jnp.where(low, a, b) + pltpu.roll(jnp.where(low, b, a), 4, 0)
        for a, b in zip(values[:4], values[4:])
    ]
    for dist in (2, 1):
        low = (row & dist) == 0
        values = [
            jnp.where(low, a, b) + jnp.where(low, pltpu.roll(a, 8 - dist, 0), pltpu.roll(b, dist, 0))
            for a, b in zip(values[:dist], values[dist:])
        ]
    return values[0]


def stacked(rows):
    comp = iota((8, rows[0].shape[1]), 0)
    out = jnp.zeros((8, rows[0].shape[1]), f32)
    for c, row in enumerate(rows):
        out = jnp.where(comp == c, row, out)
    return out


def axes_of(number):
    height = 1.0 - (2.0 * number + 1.0) / DIRECTIONS
    radius = jnp.sqrt(1.0 - height * height)
    phase = number * golden
    return [radius * jnp.cos(phase), radius * jnp.sin(phase), height]


def pair_sums(own_rows, source):
    dx, dy, dz = [o - s for o, s in zip(own_rows, source[:3])]
    period = source[3]
    half = 0.5 * period
    dz = dz + jnp.where(dz > half, -period, jnp.where(dz < -half, period, 0.0))
    reach = jnp.maximum(1.0 - (dx * dx + dy * dy + dz * dz), 0.0)
    weight = reach * reach
    return [weight * dx, weight * dy, weight * dz]


def force_pass(own, force, sources, first):
    slots = own.shape[1]
    wide = 32 if slots % 32 == 0 else 8

    def block(r, carry):
        at = pl.ds(pl.multiple_of(r * wide, wide), wide)
        rows = [own[c, at, :] for c in range(3)]
        total = None if first else [force[c, at, :] for c in range(3)]
        for source in sources:
            parts = pair_sums(rows, source())
            total = parts if total is None else [t + p for t, p in zip(total, parts)]
        for c in range(3):
            force[c, at, :] = total[c]
        return carry

    lax.fori_loop(0, slots // wide, block, 0)


def force_rows(force):
    slots = force.shape[1]
    comp = iota((8, slots), 0)
    out = None
    for c in range(3):
        pick = (comp == c).astype(f32).astype(bf16)
        for term in terms(force[c], 2)[::-1]:
            part = dot(pick, term, ((1,), (1,)))
            out = part if out is None else out + part
    return out


def own_columns(own, tile):
    slots = tile.shape[1]
    block = jnp.concatenate([tile, jnp.zeros((slots - 8, slots), f32)], axis=0).T
    for c in range(3):
        own[c] = jnp.broadcast_to(block[:, c : c + 1], (slots, slots))


def collide_kernel(
    shape, shift, count, solvent_hbm, occupancy_hbm, axis_hbm, pos_hbm, vel_hbm, mass_hbm,
    out, force, own, late, tiles,
    pos, vel, mass, axis, occupancy, held, acc, cell, sums, total, index, edge_x, edge_y, edge_c,
    normals, fields, halo_x, halo_y, halo_c, src,
    small_sem, chunk_sem, occ_sem, halo_send, halo_got, edge_send, edge_got, src_send, src_got,
):
    width_x, width_y, width_z = shape
    n_x, n_y = (width_x // SUB, width_y // SUB)
    rows = 2 * width_y
    slots = mass.shape[2]
    me_x, me_y = (lax.axis_index("gx"), lax.axis_index("yz"))
    size_x, size_y = (lax.axis_size("gx"), lax.axis_size("yz"))
    shift_x, shift_y, shift_z = (shift[0], shift[1], shift[2])
    high_rows = (n_y * SUB, n_y * SUB + 4)

    def device(a, b):
        return (lax.rem(me_x + a + size_x, size_x), lax.rem(me_y + b + size_y, size_y))

    def remote(source, target, send, receive, where):
        return pltpu.make_async_remote_copy(
            src_ref=source, dst_ref=target, send_sem=send, recv_sem=receive,
            device_id=where, device_id_type=MESH,
        )

    edge_c[...] = jnp.zeros_like(edge_c)
    barrier = pltpu.get_barrier_semaphore()
    for a, b in AROUND:
        pl.semaphore_signal(barrier, inc=1, device_id=device(a, b), device_id_type=MESH)

    small = [
        pltpu.make_async_copy(source, target, small_sem.at[k])
        for k, (source, target) in enumerate(
            [(pos_hbm, pos), (vel_hbm, vel), (mass_hbm, mass), (axis_hbm, axis)]
        )
    ]
    for copy in small:
        copy.start()

    def chunk(i):
        at = pl.ds(i * SUB, SUB)
        return (
            pltpu.make_async_copy(occupancy_hbm.at[at], occupancy.at[at], occ_sem.at[i]),
            pltpu.make_async_copy(solvent_hbm.at[:, at], out.at[:, at], chunk_sem.at[i]),
        )

    for i in range(n_x):
        for copy in chunk(i):
            copy.start()
    for copy in small:
        copy.wait()

    alive = iota((1, slots), 1) < count[0, 0]
    cell_x = (layer_of(pos[0, 0], SUB, width_x) + shift_x) >> 2
    cell_y = (layer_of(pos[1, 0], SUB, width_y) + shift_y) >> 2
    layer_z = layer_of(pos[2, 0], 2.0, width_z)
    cell_z = wrapped(layer_z + shift_z, width_z) >> 1
    place = cell_x * (n_y + 1) + cell_y
    weight = jnp.where(alive, mass[0], 0.0)
    comp = iota((8, slots), 0)
    four = comp & 3
    values = jnp.where(
        four == 0, vel[0, 0] * weight,
        jnp.where(four == 1, vel[1, 0] * weight, jnp.where(four == 2, vel[2, 0] * weight, weight)),
    )
    place_half = place - (comp >> 2)
    place_last = jnp.where(comp < 4, place, -1)
    tiles_y = (n_y + 2) // 2

    def in_tile(i, t):
        return (place_half if 2 * t < n_y else place_last) == i * (n_y + 1) + 2 * t

    spread = [
        jnp.where(in_tile(i, t), values, 0.0) for i in range(n_x + 1) for t in range(tiles_y)
    ]
    near = (wrapped(iota((width_z, slots), 0) + shift_z, width_z) >> 1) == cell_z
    near = near.astype(f32).astype(bf16)
    deposit = sum(
        dot(term, near, ((1,), (1,))) for term in terms(jnp.concatenate(spread, axis=0), 3)[::-1]
    )
    sums[...] = deposit.reshape(n_x + 1, tiles_y * 8, width_z)

    cell_row = wrapped(iota((width_z // 2, width_z), 1) + shift_z, width_z) >> 1
    expand = (cell_row == iota((width_z // 2, width_z), 0)).astype(f32).astype(bf16)
    number = axis[...].reshape(n_x * n_y, width_z // 2).astype(f32).astype(bf16)
    index[...] = dot(number, expand).reshape(n_x, n_y, width_z)

    start = stacked([jnp.where(alive, pos[0, 0], far_away), pos[1, 0], pos[2, 0]])
    src[0, OWN] = start * (1.0 / cutoff)

    double = (iota((rows, width_y), 0) >> 1 == iota((rows, width_y), 1)).astype(bf16)
    row = iota((8, width_z), 0)
    second = (row & 1).astype(f32)
    stays_1 = jnp.broadcast_to(shift_x, (8, width_z)) <= 2
    stays_2 = jnp.broadcast_to(shift_x, (8, width_z)) <= 1
    later = ((row >> 1) + shift_y) >= SUB
    even = ((iota((8, width_z), 1) + shift_z) & 1) == 0
    halves = jnp.where((row & 3) == 3, 0.5, 1.0)
    blank = jnp.zeros((8, width_z), f32)
    acc[...] = jnp.zeros_like(acc)

    def finish(i, ref):
        def straddling(c, j):
            now = ref[c, pl.ds(8 * j, 8), :] if j < n_y else blank
            before = ref[c, pl.ds(8 * (j - 1), 8), :] if j > 0 else blank
            return jnp.where(later, before, now)

        for t in range(tiles_y):
            blocks = [
                straddling(q & 3, 2 * t + (q >> 2)) if 2 * t + (q >> 2) <= n_y else blank
                for q in range(8)
            ]
            tile = fold(blocks) * halves
            partner = jnp.where(even, pltpu.roll(tile, width_z - 1, 1), pltpu.roll(tile, 1, 1))
            sums[i, pl.ds(8 * t, 8), :] += tile + partner

    def gather(i, carry):
        for copy in chunk(i):
            copy.wait()
        for r in range(SUB):
            held[i * SUB + r] = dot(double, occupancy[i * SUB + r].astype(f32).astype(bf16))
        for b in range(n_y):
            at = pl.ds(8 * b, 8)
            filled = [held[i * SUB + r, at, :] for r in range(SUB)]
            live = [f > second for f in filled]
            for c in range(4):
                v = filled
                if c < 3:
                    v = [jnp.where(live[r], out[c, i * SUB + r, at, :], 0.0) for r in range(SUB)]
                front = v[0] + v[1]
                back = v[3] + v[2]
                stay = jnp.where(stays_1, jnp.where(stays_2, front + v[2], front), v[0])
                move = jnp.where(stays_1, jnp.where(stays_2, v[3], back), back + v[1])
                cell[c, at, :] = acc[c, at, :] + stay
                acc[c, at, :] = move
        finish(i, cell)
        return carry

    lax.fori_loop(0, n_x, gather, 0)
    finish(n_x, acc)

    pl.semaphore_wait(barrier, len(AROUND))

    def exchange(step):
        mine = src.at[step, OWN, pl.ds(0, 4)]
        copies = {}
        for a, b in AROUND:
            k = slot_of(a, b)
            copies[k] = remote(
                mine, src.at[step, 8 - k, pl.ds(0, 4)],
                src_send.at[step, k], src_got.at[step, 8 - k], device(a, b),
            )
            copies[k].start()
        return list(copies.values())

    sends = exchange(0)

    at_low, at_high = (pl.ds(0, 4), pl.ds(n_y * SUB, 4))
    every = pl.ds(0, n_x + 1)
    halo = [
        (sums.at[n_x], halo_x.at[0], (1, 0)),
        (sums.at[0], halo_x.at[1], (-1, 0)),
        (sums.at[every, at_high], halo_y.at[0, every, at_low], (0, 1)),
        (sums.at[every, at_low], halo_y.at[1, every, at_low], (0, -1)),
        (sums.at[n_x, at_high], halo_c.at[0, at_low], (1, 1)),
        (sums.at[n_x, at_low], halo_c.at[1, at_low], (1, -1)),
        (sums.at[0, at_high], halo_c.at[2, at_low], (-1, 1)),
        (sums.at[0, at_low], halo_c.at[3, at_low], (-1, -1)),
    ]
    halo = [
        remote(source, target, halo_send.at[k], halo_got.at[k], device(*where))
        for k, (source, target, where) in enumerate(halo)
    ]
    for copy in halo:
        copy.start()
    edges = [
        (index.at[0], edge_x, (-1, 0)),
        (index.at[pl.ds(0, n_x), 0], edge_y, (0, -1)),
        (index.at[0, pl.ds(0, 1)], edge_c.at[pl.ds(0, 1)], (-1, -1)),
    ]
    edges = [
        remote(source, target, edge_send.at[k], edge_got.at[k], device(*where))
        for k, (source, target, where) in enumerate(edges)
    ]
    for copy in edges:
        copy.start()

    period = (width_z // 2) / cutoff
    step_x, step_y = (n_x / cutoff, n_y / cutoff)
    side = 1 - 2 * (me_x & 1)
    quick, slow = (side, -side)

    def source(step, a, b):
        slot = slot_of(a, b)
        offset = None if isinstance(a, int) else a.astype(f32) * step_x

        def read():
            x, y, z = [src[step, slot, pl.ds(c, 1), :] for c in range(3)]
            x = x if offset is None else x + offset
            return (x, y if b == 0 else y + b * step_y, z, period)

        return read

    def arrived(step, a, b):
        slot = slot_of(a, b)
        remote(
            src.at[step, OWN, pl.ds(0, 4)], src.at[step, slot, pl.ds(0, 4)],
            src_send.at[step, slot], src_got.at[step, slot], device(0, 1),
        ).wait_recv()

    def early_forces(step):
        for b in (-1, 1):
            arrived(step, 0, b)
        force_pass(own, force, [source(step, 0, b) for b in (0, -1, 1)], True)
        for b in (-1, 0, 1):
            arrived(step, quick, b)
        force_pass(own, force, [source(step, quick, b) for b in (-1, 0, 1)], False)

    def late_arrivals(step):
        for b in (-1, 0, 1):
            arrived(step, slow, b)

    def late_forces(step):
        late_arrivals(step)
        force_pass(own, force, [source(step, slow, b) for b in (-1, 0, 1)], False)
        return force_rows(force)

    own_columns(own, src[0, OWN])
    early_forces(0)
    push = late_forces(0)

    for copy in halo:
        copy.wait_recv()
    total[...] = sums[...]
    total[0] += halo_x[0]
    total[n_x] += halo_x[1]
    for i in range(n_x + 1):
        total[i, at_low, :] += halo_y[0, i, at_low, :]
        total[i, at_high, :] += halo_y[1, i, at_low, :]
    total[0, at_low, :] += halo_c[0, at_low, :]
    total[0, at_high, :] += halo_c[1, at_low, :]
    total[n_x, at_low, :] += halo_c[2, at_low, :]
    total[n_x, at_high, :] += halo_c[3, at_low, :]
    for copy in edges:
        copy.wait_recv()

    chosen = (iota((width_z, slots), 0) == layer_z).astype(f32).astype(bf16)
    block = total[...].reshape((n_x + 1) * tiles_y * 8, width_z)
    at_z = sum(dot(term, chosen) for term in terms(block, 2)[::-1])
    picked = jnp.zeros((8, slots), f32)
    for i in range(n_x + 1):
        for t in range(tiles_y):
            n = 8 * (i * tiles_y + t)
            picked = picked + jnp.where(in_tile(i, t), at_z[n : n + 8], 0.0)
    picked = picked + pltpu.roll(picked, 4, 0)
    numbers = jnp.concatenate(
        [index[...].reshape(n_x * n_y, width_z), edge_x[...], edge_y[...], edge_c[...]], axis=0
    )
    at_z = dot(numbers.astype(bf16), chosen)
    wanted = [place - comp == i * (n_y + 1) for i in range(n_x + 1)]
    wanted.append(place - comp * (n_y + 1) == n_y)
    wanted.append(jnp.logical_and(comp == 0, place == n_x * (n_y + 1) + n_y))
    found = jnp.zeros((8, slots), f32)
    for n, mask in enumerate(wanted):
        found = found + jnp.where(mask, at_z[8 * n : 8 * n + 8], 0.0)
    found = jnp.sum(found, axis=0, keepdims=True)
    heavy = jnp.maximum(picked[3:4], fill_mass)
    mean = [picked[c : c + 1] / heavy for c in range(3)]
    n = axes_of(found)
    rel = [vel[c, 0] - mean[c] for c in range(3)]
    cross = [n[1] * rel[2] - n[2] * rel[1], n[2] * rel[0] - n[0] * rel[2], n[0] * rel[1] - n[1] * rel[0]]
    along = n[0] * rel[0] + n[1] * rel[1] + n[2] * rel[2]
    speed = stacked([
        mean[c] + cos_angle * rel[c] + sin_angle * cross[c] + (1.0 - cos_angle) * along * n[c]
        for c in range(3)
    ])
    kick = jnp.broadcast_to((timestep * stiffness * cutoff) / mass[0], (8, slots))
    place_now = start

    def cell_fields(i, rows_of):
        for b in range(n_y):
            pair = [
                [jnp.where(later, total[i, pl.ds(4 * (b + 1) + c, 1), :], total[i, pl.ds(4 * b + c, 1), :])
                 for c in range(4)],
                [jnp.where(later, normals[c, pl.ds(rows_of(b + 1), 1), :], normals[c, pl.ds(rows_of(b), 1), :])
                 for c in range(3)],
            ]
            scale = 1.0 / jnp.maximum(pair[0][3], fill_mass)
            for c in range(3):
                fields[i, b, c] = pair[0][c] * scale
                fields[i, b, 3 + c] = pair[1][c]

    def turn(x, carry):
        at_cell = (x + shift_x) >> 2
        for b in range(n_y):
            at = pl.ds(8 * b, 8)
            mean = [fields[at_cell, b, c] for c in range(3)]
            n = [fields[at_cell, b, 3 + c] for c in range(3)]
            old = [out[c, x, at, :] for c in range(3)]
            rel = [old[c] - mean[c] for c in range(3)]
            along = (1.0 - cos_angle) * (n[0] * rel[0] + n[1] * rel[1] + n[2] * rel[2])
            cross = [
                n[1] * rel[2] - n[2] * rel[1],
                n[2] * rel[0] - n[0] * rel[2],
                n[0] * rel[1] - n[1] * rel[0],
            ]
            live = held[x, at, :] > second
            for c in range(3):
                new = mean[c] + cos_angle * rel[c] + sin_angle * cross[c] + along * n[c]
                out[c, x, at, :] = jnp.where(live, new, old[c])
        return carry

    def idle_work(step):
        if step == 1:
            for c, part in enumerate(axes_of(numbers)):
                normals[c] = part

            def inner(i, carry):
                cell_fields(i, lambda b: i * n_y + b if b < n_y else n_x * n_y + 8 + i)
                return carry

            lax.fori_loop(0, n_x, inner, 0)
            cell_fields(n_x, lambda b: n_x * n_y + b if b < n_y else n_x * n_y + 16)
            lax.fori_loop(0, width_x // 2, turn, 0)
        if step == 2:
            lax.fori_loop(width_x // 2, width_x, turn, 0)

    for step in range(1, SUBSTEPS):
        speed = speed + push * kick
        place_now = place_now + timestep * speed
        src[step, OWN] = place_now * (1.0 / cutoff)
        sends = sends + exchange(step)
        own_columns(own, src[step, OWN])
        idle_work(step)
        early_forces(step)
        if step < SUBSTEPS - 1:
            push = late_forces(step)

    tiles[0] = place_now
    tiles[1] = speed
    tiles[2] = kick
    tiles[3] = stacked([pos[c, 0] for c in range(3)])
    tiles[4] = stacked([vel[c, 0] for c in range(3)])
    tiles[5] = jnp.broadcast_to(jnp.where(alive, 1.0, 0.0), (8, slots))
    late_arrivals(SUBSTEPS - 1)
    for b in (-1, 0, 1):
        x, y, z, _ = source(SUBSTEPS - 1, slow, b)()
        late[b + 1] = stacked([x, y, z])
    for copy in sends + halo + edges:
        copy.wait_send()


def finish_kernel(shape, turned, force, own, late, tiles, out, pos_out, vel_out, sem):
    width_x, width_y, width_z = shape
    parts = 2
    thin = width_x // parts
    copies = []
    for c in range(3):
        for h in range(parts):
            at = pl.ds(h * thin, thin)
            copies.append(
                pltpu.make_async_copy(turned.at[c, at], out.at[c, at], sem.at[c * parts + h])
            )
            copies[-1].start()

    period = (width_z // 2) / cutoff

    def source(k):
        return lambda: tuple(late[k, pl.ds(c, 1), :] for c in range(3)) + (period,)

    force_pass(own, force, [source(k) for k in range(3)], False)
    push = force_rows(force)
    speed = tiles[1] + push * tiles[2]
    place = tiles[0] + timestep * speed
    alive = tiles[5] > 0
    place = jnp.where(alive, place, tiles[3])
    speed = jnp.where(alive, speed, tiles[4])
    for c in range(3):
        pos_out[c, 0] = place[c : c + 1]
        vel_out[c, 0] = speed[c : c + 1]
    for copy in copies:
        copy.wait()


def per_device(
    solvent_vel, occupancy, grid_shift, axis_index, colloid_pos, colloid_vel, colloid_mass, colloid_count
):
    shape = occupancy.shape
    width_x, width_y, width_z = shape
    rows = 2 * width_y
    n_x, n_y = (width_x // SUB, width_y // SUB)
    slots = colloid_mass.shape[2]
    solvent = solvent_vel.reshape(3, width_x, rows, width_z)
    smem = pl.BlockSpec(memory_space=pltpu.SMEM)
    vmem = pl.BlockSpec(memory_space=pltpu.VMEM)
    hbm = pl.BlockSpec(memory_space=pltpu.HBM)
    tall = (n_y + 2) // 2 * 8
    dma = pltpu.SemaphoreType.DMA

    def in_hbm(x):
        return pltpu.with_memory_space_constraint(x, pltpu.HBM)

    turned, force, own, late, tiles = pl.pallas_call(
        functools.partial(collide_kernel, shape),
        out_shape=[
            pltpu.VMEM(solvent.shape, f32),
            pltpu.VMEM((3, slots, slots), f32),
            pltpu.VMEM((3, slots, slots), f32),
            pltpu.VMEM((3, 8, slots), f32),
            pltpu.VMEM((6, 8, slots), f32),
        ],
        in_specs=[smem, smem] + [hbm] * 6,
        out_specs=[vmem] * 5,
        scratch_shapes=[
            pltpu.VMEM(colloid_pos.shape, f32),
            pltpu.VMEM(colloid_vel.shape, f32),
            pltpu.VMEM(colloid_mass.shape, f32),
            pltpu.VMEM(axis_index.shape, jnp.int32),
            pltpu.VMEM(shape, jnp.int32),
            pltpu.VMEM((width_x, rows, width_z), f32),
            pltpu.VMEM((4, rows, width_z), f32),
            pltpu.VMEM((4, rows, width_z), f32),
            pltpu.VMEM((n_x + 1, tall, width_z), f32),
            pltpu.VMEM((n_x + 1, tall, width_z), f32),
            pltpu.VMEM((n_x, n_y, width_z), f32),
            pltpu.VMEM((8, width_z), f32),
            pltpu.VMEM((8, width_z), f32),
            pltpu.VMEM((8, width_z), f32),
            pltpu.VMEM((3, n_x * n_y + 24, width_z), f32),
            pltpu.VMEM((n_x + 1, n_y, 6, 8, width_z), f32),
            pltpu.VMEM((2, tall, width_z), f32),
            pltpu.VMEM((2, n_x + 1, 8, width_z), f32),
            pltpu.VMEM((4, 8, width_z), f32),
            pltpu.VMEM((SUBSTEPS, 9, 8, slots), f32),
            dma((4,)),
            dma((n_x,)),
            dma((n_x,)),
            dma((8,)),
            dma((8,)),
            dma((3,)),
            dma((3,)),
            dma((SUBSTEPS, 9)),
            dma((SUBSTEPS, 9)),
        ],
        compiler_params=pltpu.CompilerParams(
            collective_id=0, has_side_effects=True, vmem_limit_bytes=32 * 2**20
        ),
        name="collide",
    )(
        grid_shift, colloid_count, in_hbm(solvent), in_hbm(occupancy), in_hbm(axis_index),
        in_hbm(colloid_pos), in_hbm(colloid_vel), in_hbm(colloid_mass),
    )

    parts = 2
    solvent_out, pos_out, vel_out = pl.pallas_call(
        functools.partial(finish_kernel, shape),
        out_shape=[
            jax.ShapeDtypeStruct(solvent.shape, f32),
            jax.ShapeDtypeStruct(colloid_pos.shape, f32),
            jax.ShapeDtypeStruct(colloid_vel.shape, f32),
        ],
        in_specs=[vmem] * 5,
        out_specs=[hbm, vmem, vmem],
        scratch_shapes=[dma((3 * parts,))],
        input_output_aliases={},
        compiler_params=pltpu.CompilerParams(vmem_limit_bytes=8 * 2**20),
        name="finish",
    )(turned, force, own, late, tiles)
    return (solvent_out.reshape(solvent_vel.shape), pos_out, vel_out)


def solution(mesh):
    return jax.shard_map(
        per_device,
        mesh=mesh,
        in_specs=(
            P(None, "gx", "yz", None, None),
            P("gx", "yz", None),
            P(),
            P("gx", "yz", None),
            P(None, "gx", "yz", None),
            P(None, "gx", "yz", None),
            P("gx", "yz", None),
            P("gx", "yz"),
        ),
        out_specs=(
            P(None, "gx", "yz", None, None),
            P(None, "gx", "yz", None),
            P(None, "gx", "yz", None),
        ),
        check_vma=False,
    )
```

```python
import functools
import math

import jax
import jax.numpy as jnp
from jax import lax
from jax.experimental import pallas as pl
from jax.experimental.pallas import tpu as pltpu
from jax.sharding import PartitionSpec as P

SUB = 4
SUBSTEPS = 4
DIRECTIONS = 64

turn_angle = 130.0 * math.pi / 180.0
cos_angle = math.cos(turn_angle)
sin_angle = math.sin(turn_angle)
golden = math.pi * (3.0 - math.sqrt(5.0))
cutoff = 1.5
stiffness = 20.0
timestep = 0.05
fill_mass = 16.0
far_away = 1.0e9
MESH = pl.DeviceIdType.MESH
f32 = jnp.float32
bf16 = jnp.bfloat16
AROUND = [(a, b) for a in (-1, 0, 1) for b in (-1, 0, 1) if (a, b) != (0, 0)]
OWN = 4


def iota(shape, dim):
    return lax.broadcasted_iota(jnp.int32, shape, dim)


def slot_of(a, b):
    return (a + 1) * 3 + b + 1


def terms(value, number):
    out = []
    for _ in range(number - 1):
        part = value.astype(bf16)
        out.append(part)
        value = value - part.astype(f32)
    return out + [value.astype(bf16)]


def dot(left, right, contract=((1,), (0,))):
    return lax.dot_general(left, right, (contract, ((), ())), preferred_element_type=f32)


def wrapped(value, size):
    return jnp.where(value >= size, value - size, value)


def layer_of(row, scale, width):
    return jnp.clip(jnp.floor(row * scale).astype(jnp.int32), 0, width - 1)


def fold(values):
    row = iota(values[0].shape, 0)
    low = row < 4
    values = [
        jnp.where(low, a, b) + pltpu.roll(jnp.where(low, b, a), 4, 0)
        for a, b in zip(values[:4], values[4:])
    ]
    for dist in (2, 1):
        low = (row & dist) == 0
        values = [
            jnp.where(low, a, b) + jnp.where(low, pltpu.roll(a, 8 - dist, 0), pltpu.roll(b, dist, 0))
            for a, b in zip(values[:dist], values[dist:])
        ]
    return values[0]


def stacked(rows):
    comp = iota((8, rows[0].shape[1]), 0)
    out = jnp.zeros((8, rows[0].shape[1]), f32)
    for c, row in enumerate(rows):
        out = jnp.where(comp == c, row, out)
    return out


def axes_of(number):
    height = 1.0 - (2.0 * number + 1.0) / DIRECTIONS
    radius = jnp.sqrt(1.0 - height * height)
    phase = number * golden
    return [radius * jnp.cos(phase), radius * jnp.sin(phase), height]


def pair_sums(own_rows, source):
    dx, dy, dz = [o - s for o, s in zip(own_rows, source[:3])]
    period = source[3]
    half = 0.5 * period
    dz = dz + jnp.where(dz > half, -period, jnp.where(dz < -half, period, 0.0))
    reach = jnp.maximum(1.0 - (dx * dx + dy * dy + dz * dz), 0.0)
    weight = reach * reach
    return [weight * dx, weight * dy, weight * dz]


def force_pass(own, force, sources, first):
    slots = own.shape[1]
    wide = 32 if slots % 32 == 0 else 8

    def block(r, carry):
        at = pl.ds(pl.multiple_of(r * wide, wide), wide)
        rows = [own[c, at, :] for c in range(3)]
        total = None if first else [force[c, at, :] for c in range(3)]
        for source in sources:
            parts = pair_sums(rows, source())
            total = parts if total is None else [t + p for t, p in zip(total, parts)]
        for c in range(3):
            force[c, at, :] = total[c]
        return carry

    lax.fori_loop(0, slots // wide, block, 0)


def force_rows(force):
    slots = force.shape[1]
    comp = iota((8, slots), 0)
    out = None
    for c in range(3):
        pick = (comp == c).astype(f32).astype(bf16)
        for term in terms(force[c], 2)[::-1]:
            part = dot(pick, term, ((1,), (1,)))
            out = part if out is None else out + part
    return out


def own_columns(own, tile):
    slots = tile.shape[1]
    block = jnp.concatenate([tile, jnp.zeros((slots - 8, slots), f32)], axis=0).T
    for c in range(3):
        own[c] = jnp.broadcast_to(block[:, c : c + 1], (slots, slots))


def collide_kernel(
    shape, shift_hbm, count, solvent_hbm, occupancy_hbm, axis_hbm, pos_hbm, vel_hbm, mass_hbm,
    out, force, own, late, tiles,
    shift, pos, vel, mass, axis, occupancy, held, cell, sums, total, index, edge_x, edge_y, edge_c,
    normals, fields, halo_x, halo_y, halo_c, src,
    small_sem, chunk_sem, halo_send, halo_got, edge_send, edge_got, src_send, src_got,
):
    width_x, width_y, width_z = shape
    n_x, n_y = (width_x // SUB, width_y // SUB)
    rows = 2 * width_y
    slots = mass.shape[2]
    me_x, me_y = (lax.axis_index("gx"), lax.axis_index("yz"))
    size_x, size_y = (lax.axis_size("gx"), lax.axis_size("yz"))

    def device(a, b):
        return (lax.rem(me_x + a + size_x, size_x), lax.rem(me_y + b + size_y, size_y))

    def remote(source, target, send, receive, where):
        return pltpu.make_async_remote_copy(
            src_ref=source, dst_ref=target, send_sem=send, recv_sem=receive,
            device_id=where, device_id_type=MESH,
        )

    edge_c[...] = jnp.zeros_like(edge_c)
    barrier = pltpu.get_barrier_semaphore()
    for a, b in AROUND:
        pl.semaphore_signal(barrier, inc=1, device_id=device(a, b), device_id_type=MESH)

    small = [
        pltpu.make_async_copy(source, target, small_sem.at[k])
        for k, (source, target) in enumerate(
            [
                (shift_hbm, shift), (pos_hbm, pos), (vel_hbm, vel),
                (mass_hbm, mass), (axis_hbm, axis), (occupancy_hbm, occupancy),
            ]
        )
    ]
    chunks = [
        pltpu.make_async_copy(
            solvent_hbm.at[:, pl.ds(i * SUB, SUB)], out.at[:, pl.ds(i * SUB, SUB)], chunk_sem.at[i]
        )
        for i in range(n_x)
    ]
    for copy in small + chunks:
        copy.start()
    for copy in small[:-1]:
        copy.wait()
    shift_x, shift_y, shift_z = (shift[0], shift[1], shift[2])

    alive = iota((1, slots), 1) < count[0, 0]
    cell_x = (layer_of(pos[0, 0], SUB, width_x) + shift_x) >> 2
    cell_y = (layer_of(pos[1, 0], SUB, width_y) + shift_y) >> 2
    layer_z = layer_of(pos[2, 0], 2.0, width_z)
    cell_z = wrapped(layer_z + shift_z, width_z) >> 1
    place = cell_x * (n_y + 1) + cell_y
    weight = jnp.where(alive, mass[0], 0.0)
    comp = iota((8, slots), 0)
    four = comp & 3
    values = jnp.where(
        four == 0, vel[0, 0] * weight,
        jnp.where(four == 1, vel[1, 0] * weight, jnp.where(four == 2, vel[2, 0] * weight, weight)),
    )
    place_half = place - (comp >> 2)
    place_last = jnp.where(comp < 4, place, -1)
    tiles_y = (n_y + 2) // 2

    def in_tile(i, t):
        return (place_half if 2 * t < n_y else place_last) == i * (n_y + 1) + 2 * t

    spread = [
        jnp.where(in_tile(i, t), values, 0.0) for i in range(n_x + 1) for t in range(tiles_y)
    ]
    near = (wrapped(iota((width_z, slots), 0) + shift_z, width_z) >> 1) == cell_z
    near = near.astype(f32).astype(bf16)
    deposit = sum(
        dot(term, near, ((1,), (1,))) for term in terms(jnp.concatenate(spread, axis=0), 3)[::-1]
    )
    sums[...] = deposit.reshape(n_x + 1, tiles_y * 8, width_z)

    cell_row = wrapped(iota((width_z // 2, width_z), 1) + shift_z, width_z) >> 1
    expand = (cell_row == iota((width_z // 2, width_z), 0)).astype(f32).astype(bf16)
    number = axis[...].reshape(n_x * n_y, width_z // 2).astype(f32).astype(bf16)
    index[...] = dot(number, expand).reshape(n_x, n_y, width_z)

    start = stacked([jnp.where(alive, pos[0, 0], far_away), pos[1, 0], pos[2, 0]])
    src[0, OWN] = start * (1.0 / cutoff)

    double = (iota((SUB * rows, SUB * width_y), 0) >> 1 == iota((SUB * rows, SUB * width_y), 1)).astype(bf16)
    small[-1].wait()
    for i in range(n_x):
        at = pl.ds(i * SUB, SUB)
        filled = occupancy[at].reshape(SUB * width_y, width_z).astype(f32).astype(bf16)
        held[at] = dot(double, filled).reshape(SUB, rows, width_z)
    row = iota((8, width_z), 0)
    second = (row & 1).astype(f32)
    stays_1 = jnp.broadcast_to(shift_x, (8, width_z)) <= 2
    stays_2 = jnp.broadcast_to(shift_x, (8, width_z)) <= 1
    later = ((row >> 1) + shift_y) >= SUB
    even = ((iota((8, width_z), 1) + shift_z) & 1) == 0
    halves = jnp.where((row & 3) == 3, 0.5, 1.0)
    blank = jnp.zeros((8, width_z), f32)

    def finish(i):
        def straddling(c, j):
            now = cell[i, c, pl.ds(8 * j, 8), :] if j < n_y else blank
            before = cell[i, c, pl.ds(8 * (j - 1), 8), :] if j > 0 else blank
            return jnp.where(later, before, now)

        for t in range(tiles_y):
            blocks = [
                straddling(q & 3, 2 * t + (q >> 2)) if 2 * t + (q >> 2) <= n_y else blank
                for q in range(8)
            ]
            tile = fold(blocks) * halves
            partner = jnp.where(even, pltpu.roll(tile, width_z - 1, 1), pltpu.roll(tile, 1, 1))
            sums[i, pl.ds(8 * t, 8), :] += tile + partner

    def gather(i):
        for b in range(n_y):
            at = pl.ds(8 * b, 8)
            filled = [held[i * SUB + r, at, :] for r in range(SUB)]
            live = [f > second for f in filled]
            for c in range(4):
                v = filled
                if c < 3:
                    v = [jnp.where(live[r], out[c, i * SUB + r, at, :], 0.0) for r in range(SUB)]
                front = v[0] + v[1]
                back = v[3] + v[2]
                stay = jnp.where(stays_1, jnp.where(stays_2, front + v[2], front), v[0])
                move = jnp.where(stays_1, jnp.where(stays_2, v[3], back), back + v[1])
                cell[i, c, at, :] = stay if i == 0 else cell[i, c, at, :] + stay
                cell[i + 1, c, at, :] = move

    for i in range(n_x):
        chunks[i].wait()
        gather(i)
        if i > 0:
            finish(i - 1)
    finish(n_x - 1)
    finish(n_x)

    pl.semaphore_wait(barrier, len(AROUND))

    def exchange(step):
        mine = src.at[step, OWN, pl.ds(0, 4)]
        copies = {}
        for a, b in AROUND:
            k = slot_of(a, b)
            copies[k] = remote(
                mine, src.at[step, 8 - k, pl.ds(0, 4)],
                src_send.at[step, k], src_got.at[step, 8 - k], device(a, b),
            )
            copies[k].start()
        return list(copies.values())

    sends = exchange(0)

    at_low, at_high = (pl.ds(0, 4), pl.ds(n_y * SUB, 4))
    every = pl.ds(0, n_x + 1)
    halo = [
        (sums.at[n_x], halo_x.at[0], (1, 0)),
        (sums.at[0], halo_x.at[1], (-1, 0)),
        (sums.at[every, at_high], halo_y.at[0, every, at_low], (0, 1)),
        (sums.at[every, at_low], halo_y.at[1, every, at_low], (0, -1)),
        (sums.at[n_x, at_high], halo_c.at[0, at_low], (1, 1)),
        (sums.at[n_x, at_low], halo_c.at[1, at_low], (1, -1)),
        (sums.at[0, at_high], halo_c.at[2, at_low], (-1, 1)),
        (sums.at[0, at_low], halo_c.at[3, at_low], (-1, -1)),
    ]
    halo = [
        remote(source, target, halo_send.at[k], halo_got.at[k], device(*where))
        for k, (source, target, where) in enumerate(halo)
    ]
    for copy in halo:
        copy.start()
    edges = [
        (index.at[0], edge_x, (-1, 0)),
        (index.at[pl.ds(0, n_x), 0], edge_y, (0, -1)),
        (index.at[0, pl.ds(0, 1)], edge_c.at[pl.ds(0, 1)], (-1, -1)),
    ]
    edges = [
        remote(source, target, edge_send.at[k], edge_got.at[k], device(*where))
        for k, (source, target, where) in enumerate(edges)
    ]
    for copy in edges:
        copy.start()

    period = (width_z // 2) / cutoff
    step_x, step_y = (n_x / cutoff, n_y / cutoff)
    side = 1 - 2 * (me_x & 1)
    quick, slow = (side, -side)

    def source(step, a, b):
        slot = slot_of(a, b)
        offset = None if isinstance(a, int) else a.astype(f32) * step_x

        def read():
            x, y, z = [src[step, slot, pl.ds(c, 1), :] for c in range(3)]
            x = x if offset is None else x + offset
            return (x, y if b == 0 else y + b * step_y, z, period)

        return read

    def arrived(step, a, b):
        slot = slot_of(a, b)
        remote(
            src.at[step, OWN, pl.ds(0, 4)], src.at[step, slot, pl.ds(0, 4)],
            src_send.at[step, slot], src_got.at[step, slot], device(0, 1),
        ).wait_recv()

    def early_forces(step):
        for b in (-1, 1):
            arrived(step, 0, b)
        force_pass(own, force, [source(step, 0, b) for b in (0, -1, 1)], True)
        for b in (-1, 0, 1):
            arrived(step, quick, b)
        force_pass(own, force, [source(step, quick, b) for b in (-1, 0, 1)], False)

    def late_arrivals(step):
        for b in (-1, 0, 1):
            arrived(step, slow, b)

    def late_forces(step):
        late_arrivals(step)
        force_pass(own, force, [source(step, slow, b) for b in (-1, 0, 1)], False)
        return force_rows(force)

    own_columns(own, src[0, OWN])
    early_forces(0)
    push = late_forces(0)

    for copy in halo:
        copy.wait_recv()
    total[...] = sums[...]
    total[0] += halo_x[0]
    total[n_x] += halo_x[1]
    for i in range(n_x + 1):
        total[i, at_low, :] += halo_y[0, i, at_low, :]
        total[i, at_high, :] += halo_y[1, i, at_low, :]
    total[0, at_low, :] += halo_c[0, at_low, :]
    total[0, at_high, :] += halo_c[1, at_low, :]
    total[n_x, at_low, :] += halo_c[2, at_low, :]
    total[n_x, at_high, :] += halo_c[3, at_low, :]
    for copy in edges:
        copy.wait_recv()

    chosen = (iota((width_z, slots), 0) == layer_z).astype(f32).astype(bf16)
    block = total[...].reshape((n_x + 1) * tiles_y * 8, width_z)
    at_z = sum(dot(term, chosen) for term in terms(block, 2)[::-1])
    picked = jnp.zeros((8, slots), f32)
    for i in range(n_x + 1):
        for t in range(tiles_y):
            n = 8 * (i * tiles_y + t)
            picked = picked + jnp.where(in_tile(i, t), at_z[n : n + 8], 0.0)
    picked = picked + pltpu.roll(picked, 4, 0)
    numbers = jnp.concatenate(
        [index[...].reshape(n_x * n_y, width_z), edge_x[...], edge_y[...], edge_c[...]], axis=0
    )
    at_z = dot(numbers.astype(bf16), chosen)
    wanted = [place - comp == i * (n_y + 1) for i in range(n_x + 1)]
    wanted.append(place - comp * (n_y + 1) == n_y)
    wanted.append(jnp.logical_and(comp == 0, place == n_x * (n_y + 1) + n_y))
    found = jnp.zeros((8, slots), f32)
    for n, mask in enumerate(wanted):
        found = found + jnp.where(mask, at_z[8 * n : 8 * n + 8], 0.0)
    found = jnp.sum(found, axis=0, keepdims=True)
    heavy = jnp.maximum(picked[3:4], fill_mass)
    mean = [picked[c : c + 1] / heavy for c in range(3)]
    n = axes_of(found)
    rel = [vel[c, 0] - mean[c] for c in range(3)]
    cross = [n[1] * rel[2] - n[2] * rel[1], n[2] * rel[0] - n[0] * rel[2], n[0] * rel[1] - n[1] * rel[0]]
    along = n[0] * rel[0] + n[1] * rel[1] + n[2] * rel[2]
    speed = stacked([
        mean[c] + cos_angle * rel[c] + sin_angle * cross[c] + (1.0 - cos_angle) * along * n[c]
        for c in range(3)
    ])
    kick = jnp.broadcast_to((timestep * stiffness * cutoff) / mass[0], (8, slots))
    place_now = start

    def cell_fields(i, rows_of):
        for b in range(n_y):
            pair = [
                [jnp.where(later, total[i, pl.ds(4 * (b + 1) + c, 1), :], total[i, pl.ds(4 * b + c, 1), :])
                 for c in range(4)],
                [jnp.where(later, normals[c, pl.ds(rows_of(b + 1), 1), :], normals[c, pl.ds(rows_of(b), 1), :])
                 for c in range(3)],
            ]
            scale = 1.0 / jnp.maximum(pair[0][3], fill_mass)
            for c in range(3):
                fields[i, b, c] = pair[0][c] * scale
                fields[i, b, 3 + c] = pair[1][c]

    def turn(x, carry):
        at_cell = (x + shift_x) >> 2
        for b in range(n_y):
            at = pl.ds(8 * b, 8)
            mean = [fields[at_cell, b, c] for c in range(3)]
            n = [fields[at_cell, b, 3 + c] for c in range(3)]
            old = [out[c, x, at, :] for c in range(3)]
            rel = [old[c] - mean[c] for c in range(3)]
            along = (1.0 - cos_angle) * (n[0] * rel[0] + n[1] * rel[1] + n[2] * rel[2])
            cross = [
                n[1] * rel[2] - n[2] * rel[1],
                n[2] * rel[0] - n[0] * rel[2],
                n[0] * rel[1] - n[1] * rel[0],
            ]
            live = held[x, at, :] > second
            for c in range(3):
                new = mean[c] + cos_angle * rel[c] + sin_angle * cross[c] + along * n[c]
                out[c, x, at, :] = jnp.where(live, new, old[c])
        return carry

    def idle_work(step):
        if step == 1:
            for c, part in enumerate(axes_of(numbers)):
                normals[c] = part

            def inner(i, carry):
                cell_fields(i, lambda b: i * n_y + b if b < n_y else n_x * n_y + 8 + i)
                return carry

            lax.fori_loop(0, n_x, inner, 0)
            cell_fields(n_x, lambda b: n_x * n_y + b if b < n_y else n_x * n_y + 16)
            lax.fori_loop(0, width_x // 2, turn, 0)
        if step == 2:
            lax.fori_loop(width_x // 2, width_x, turn, 0)

    for step in range(1, SUBSTEPS):
        speed = speed + push * kick
        place_now = place_now + timestep * speed
        src[step, OWN] = place_now * (1.0 / cutoff)
        sends = sends + exchange(step)
        own_columns(own, src[step, OWN])
        idle_work(step)
        early_forces(step)
        if step < SUBSTEPS - 1:
            push = late_forces(step)

    tiles[0] = place_now
    tiles[1] = speed
    tiles[2] = kick
    tiles[3] = stacked([pos[c, 0] for c in range(3)])
    tiles[4] = stacked([vel[c, 0] for c in range(3)])
    tiles[5] = jnp.broadcast_to(jnp.where(alive, 1.0, 0.0), (8, slots))
    late_arrivals(SUBSTEPS - 1)
    for b in (-1, 0, 1):
        x, y, z, _ = source(SUBSTEPS - 1, slow, b)()
        late[b + 1] = stacked([x, y, z])
    for copy in sends + halo + edges:
        copy.wait_send()


def finish_kernel(shape, turned, force, own, late, tiles, out, pos_out, vel_out, sem):
    width_x, width_y, width_z = shape
    parts = 2
    thin = width_x // parts
    copies = []
    for c in range(3):
        for h in range(parts):
            at = pl.ds(h * thin, thin)
            copies.append(
                pltpu.make_async_copy(turned.at[c, at], out.at[c, at], sem.at[c * parts + h])
            )
            copies[-1].start()

    period = (width_z // 2) / cutoff

    def source(k):
        return lambda: tuple(late[k, pl.ds(c, 1), :] for c in range(3)) + (period,)

    force_pass(own, force, [source(k) for k in range(3)], False)
    push = force_rows(force)
    speed = tiles[1] + push * tiles[2]
    place = tiles[0] + timestep * speed
    alive = tiles[5] > 0
    place = jnp.where(alive, place, tiles[3])
    speed = jnp.where(alive, speed, tiles[4])
    for c in range(3):
        pos_out[c, 0] = place[c : c + 1]
        vel_out[c, 0] = speed[c : c + 1]
    for copy in copies:
        copy.wait()


def per_device(
    solvent_vel, occupancy, grid_shift, axis_index, colloid_pos, colloid_vel, colloid_mass, colloid_count
):
    shape = occupancy.shape
    width_x, width_y, width_z = shape
    rows = 2 * width_y
    n_x, n_y = (width_x // SUB, width_y // SUB)
    slots = colloid_mass.shape[2]
    solvent = solvent_vel.reshape(3, width_x, rows, width_z)
    smem = pl.BlockSpec(memory_space=pltpu.SMEM)
    vmem = pl.BlockSpec(memory_space=pltpu.VMEM)
    hbm = pl.BlockSpec(memory_space=pltpu.HBM)
    tall = (n_y + 2) // 2 * 8
    dma = pltpu.SemaphoreType.DMA

    def in_hbm(x):
        return pltpu.with_memory_space_constraint(x, pltpu.HBM)

    turned, force, own, late, tiles = pl.pallas_call(
        functools.partial(collide_kernel, shape),
        out_shape=[
            pltpu.VMEM(solvent.shape, f32),
            pltpu.VMEM((3, slots, slots), f32),
            pltpu.VMEM((3, slots, slots), f32),
            pltpu.VMEM((3, 8, slots), f32),
            pltpu.VMEM((6, 8, slots), f32),
        ],
        in_specs=[hbm, smem] + [hbm] * 6,
        out_specs=[vmem] * 5,
        scratch_shapes=[
            pltpu.SMEM(grid_shift.shape, jnp.int32),
            pltpu.VMEM(colloid_pos.shape, f32),
            pltpu.VMEM(colloid_vel.shape, f32),
            pltpu.VMEM(colloid_mass.shape, f32),
            pltpu.VMEM(axis_index.shape, jnp.int32),
            pltpu.VMEM(shape, jnp.int32),
            pltpu.VMEM((width_x, rows, width_z), f32),
            pltpu.VMEM((n_x + 1, 4, rows, width_z), f32),
            pltpu.VMEM((n_x + 1, tall, width_z), f32),
            pltpu.VMEM((n_x + 1, tall, width_z), f32),
            pltpu.VMEM((n_x, n_y, width_z), f32),
            pltpu.VMEM((8, width_z), f32),
            pltpu.VMEM((8, width_z), f32),
            pltpu.VMEM((8, width_z), f32),
            pltpu.VMEM((3, n_x * n_y + 24, width_z), f32),
            pltpu.VMEM((n_x + 1, n_y, 6, 8, width_z), f32),
            pltpu.VMEM((2, tall, width_z), f32),
            pltpu.VMEM((2, n_x + 1, 8, width_z), f32),
            pltpu.VMEM((4, 8, width_z), f32),
            pltpu.VMEM((SUBSTEPS, 9, 8, slots), f32),
            dma((6,)),
            dma((n_x,)),
            dma((8,)),
            dma((8,)),
            dma((3,)),
            dma((3,)),
            dma((SUBSTEPS, 9)),
            dma((SUBSTEPS, 9)),
        ],
        compiler_params=pltpu.CompilerParams(
            collective_id=0, has_side_effects=True, vmem_limit_bytes=32 * 2**20
        ),
        name="collide",
    )(
        in_hbm(grid_shift), colloid_count, in_hbm(solvent), in_hbm(occupancy), in_hbm(axis_index),
        in_hbm(colloid_pos), in_hbm(colloid_vel), in_hbm(colloid_mass),
    )

    parts = 2
    solvent_out, pos_out, vel_out = pl.pallas_call(
        functools.partial(finish_kernel, shape),
        out_shape=[
            jax.ShapeDtypeStruct(solvent.shape, f32),
            jax.ShapeDtypeStruct(colloid_pos.shape, f32),
            jax.ShapeDtypeStruct(colloid_vel.shape, f32),
        ],
        in_specs=[vmem] * 5,
        out_specs=[hbm, vmem, vmem],
        scratch_shapes=[dma((3 * parts,))],
        input_output_aliases={},
        compiler_params=pltpu.CompilerParams(vmem_limit_bytes=8 * 2**20),
        name="finish",
    )(turned, force, own, late, tiles)
    return (solvent_out.reshape(solvent_vel.shape), pos_out, vel_out)


def solution(mesh):
    return jax.shard_map(
        per_device,
        mesh=mesh,
        in_specs=(
            P(None, "gx", "yz", None, None),
            P("gx", "yz", None),
            P(),
            P("gx", "yz", None),
            P(None, "gx", "yz", None),
            P(None, "gx", "yz", None),
            P("gx", "yz", None),
            P("gx", "yz"),
        ),
        out_specs=(
            P(None, "gx", "yz", None, None),
            P(None, "gx", "yz", None),
            P(None, "gx", "yz", None),
        ),
        check_vma=False,
    )
```

```python
import functools
import math

import jax
import jax.numpy as jnp
from jax import lax
from jax.experimental import pallas as pl
from jax.experimental.pallas import tpu as pltpu
from jax.sharding import PartitionSpec as P

SUB = 4
SUBSTEPS = 4
DIRECTIONS = 64

turn_angle = 130.0 * math.pi / 180.0
cos_angle = math.cos(turn_angle)
sin_angle = math.sin(turn_angle)
golden = math.pi * (3.0 - math.sqrt(5.0))
cutoff = 1.5
stiffness = 20.0
timestep = 0.05
fill_mass = 16.0
far_away = 1.0e9
MESH = pl.DeviceIdType.MESH
f32 = jnp.float32
bf16 = jnp.bfloat16
RING = [(a, b) for a in (-1, 0, 1) for b in (-1, 0, 1)]
AROUND = [pair for pair in RING if pair != (0, 0)]
WIDE = [(a, b) for a in (-1, 1, -2, 2, 0) for b in (-1, 0, 1, -2, 2) if (a, b) != (0, 0)]
OWN = 4


def iota(shape, dim):
    return lax.broadcasted_iota(jnp.int32, shape, dim)


def slot_of(a, b):
    return (a + 1) * 3 + b + 1


def wide_slot(a, b):
    return (a + 2) * 5 + b + 2


def terms(value, number):
    out = []
    for _ in range(number - 1):
        part = value.astype(bf16)
        out.append(part)
        value = value - part.astype(f32)
    return out + [value.astype(bf16)]


def dot(left, right, contract=((1,), (0,))):
    return lax.dot_general(left, right, (contract, ((), ())), preferred_element_type=f32)


def wrapped(value, size):
    return jnp.where(value >= size, value - size, value)


def layer_of(row, scale, width):
    return jnp.clip(jnp.floor(row * scale).astype(jnp.int32), 0, width - 1)


def fold(values):
    row = iota(values[0].shape, 0)
    low = row < 4
    values = [
        jnp.where(low, a, b) + pltpu.roll(jnp.where(low, b, a), 4, 0)
        for a, b in zip(values[:4], values[4:])
    ]
    for dist in (2, 1):
        low = (row & dist) == 0
        values = [
            jnp.where(low, a, b) + jnp.where(low, pltpu.roll(a, 8 - dist, 0), pltpu.roll(b, dist, 0))
            for a, b in zip(values[:dist], values[dist:])
        ]
    return values[0]


def stacked(rows):
    comp = iota((8, rows[0].shape[1]), 0)
    out = jnp.zeros((8, rows[0].shape[1]), f32)
    for c, row in enumerate(rows):
        out = jnp.where(comp == c, row, out)
    return out


def axes_of(number):
    height = 1.0 - (2.0 * number + 1.0) / DIRECTIONS
    radius = jnp.sqrt(1.0 - height * height)
    phase = number * golden
    return [radius * jnp.cos(phase), radius * jnp.sin(phase), height]


def pair_sums(own_rows, source):
    dx, dy, dz = [o - s for o, s in zip(own_rows, source[:3])]
    period = source[3]
    half = 0.5 * period
    dz = dz + jnp.where(dz > half, -period, jnp.where(dz < -half, period, 0.0))
    reach = jnp.maximum(1.0 - (dx * dx + dy * dy + dz * dz), 0.0)
    weight = reach * reach
    return [weight * dx, weight * dy, weight * dz]


def force_pass(own, force, sources, first):
    slots = own.shape[1]
    wide = 32 if slots % 32 == 0 else 8

    def block(r, carry):
        at = pl.ds(pl.multiple_of(r * wide, wide), wide)
        rows = [own[c, at, :] for c in range(3)]
        total = None if first else [force[c, at, :] for c in range(3)]
        for source in sources:
            parts = pair_sums(rows, source())
            total = parts if total is None else [t + p for t, p in zip(total, parts)]
        for c in range(3):
            force[c, at, :] = total[c]
        return carry

    lax.fori_loop(0, slots // wide, block, 0)


def force_rows(force):
    slots = force.shape[1]
    comp = iota((8, slots), 0)
    out = None
    for c in range(3):
        pick = (comp == c).astype(f32).astype(bf16)
        for term in terms(force[c], 2)[::-1]:
            part = dot(pick, term, ((1,), (1,)))
            out = part if out is None else out + part
    return out


def own_columns(own, tile):
    slots = tile.shape[1]
    block = jnp.concatenate([tile, jnp.zeros((slots - 8, slots), f32)], axis=0).T
    for c in range(3):
        own[c] = jnp.broadcast_to(block[:, c : c + 1], (slots, slots))


def collide_kernel(
    shape, shift_hbm, count, solvent_hbm, occupancy_hbm, axis_hbm, pos_hbm, vel_hbm, mass_hbm,
    out, first, second, third, tiles,
    shift, pos, vel, mass, axis, occupancy, held, cell, sums, total, index, edge_x, edge_y, edge_c,
    normals, fields, halo_x, halo_y, halo_c, src, wide, force, own,
    small_sem, chunk_sem, halo_send, halo_got, edge_send, edge_got, src_send, src_got,
    wide_send, wide_got,
):
    width_x, width_y, width_z = shape
    n_x, n_y = (width_x // SUB, width_y // SUB)
    rows = 2 * width_y
    slots = mass.shape[2]
    me_x, me_y = (lax.axis_index("gx"), lax.axis_index("yz"))
    size_x, size_y = (lax.axis_size("gx"), lax.axis_size("yz"))

    def device(a, b):
        return (lax.rem(me_x + a + size_x, size_x), lax.rem(me_y + b + size_y, size_y))

    def remote(source, target, send, receive, where):
        return pltpu.make_async_remote_copy(
            src_ref=source, dst_ref=target, send_sem=send, recv_sem=receive,
            device_id=where, device_id_type=MESH,
        )

    edge_c[...] = jnp.zeros_like(edge_c)
    barrier = pltpu.get_barrier_semaphore()
    for a, b in WIDE:
        pl.semaphore_signal(barrier, inc=1, device_id=device(a, b), device_id_type=MESH)

    small = [
        pltpu.make_async_copy(source, target, small_sem.at[k])
        for k, (source, target) in enumerate(
            [
                (shift_hbm, shift), (pos_hbm, pos), (vel_hbm, vel),
                (mass_hbm, mass), (axis_hbm, axis), (occupancy_hbm, occupancy),
            ]
        )
    ]
    chunks = [
        pltpu.make_async_copy(
            solvent_hbm.at[:, pl.ds(i * SUB, SUB)], out.at[:, pl.ds(i * SUB, SUB)], chunk_sem.at[i]
        )
        for i in range(n_x)
    ]
    for copy in small + chunks:
        copy.start()
    for copy in small[:-1]:
        copy.wait()
    shift_x, shift_y, shift_z = (shift[0], shift[1], shift[2])

    alive = iota((1, slots), 1) < count[0, 0]
    cell_x = (layer_of(pos[0, 0], SUB, width_x) + shift_x) >> 2
    cell_y = (layer_of(pos[1, 0], SUB, width_y) + shift_y) >> 2
    layer_z = layer_of(pos[2, 0], 2.0, width_z)
    cell_z = wrapped(layer_z + shift_z, width_z) >> 1
    place = cell_x * (n_y + 1) + cell_y
    weight = jnp.where(alive, mass[0], 0.0)
    comp = iota((8, slots), 0)
    four = comp & 3
    values = jnp.where(
        four == 0, vel[0, 0] * weight,
        jnp.where(four == 1, vel[1, 0] * weight, jnp.where(four == 2, vel[2, 0] * weight, weight)),
    )
    place_half = place - (comp >> 2)
    place_last = jnp.where(comp < 4, place, -1)
    tiles_y = (n_y + 2) // 2

    def in_tile(i, t):
        return (place_half if 2 * t < n_y else place_last) == i * (n_y + 1) + 2 * t

    spread = [
        jnp.where(in_tile(i, t), values, 0.0) for i in range(n_x + 1) for t in range(tiles_y)
    ]
    near = (wrapped(iota((width_z, slots), 0) + shift_z, width_z) >> 1) == cell_z
    near = near.astype(f32).astype(bf16)
    deposit = sum(
        dot(term, near, ((1,), (1,))) for term in terms(jnp.concatenate(spread, axis=0), 3)[::-1]
    )
    sums[...] = deposit.reshape(n_x + 1, tiles_y * 8, width_z)

    cell_row = wrapped(iota((width_z // 2, width_z), 1) + shift_z, width_z) >> 1
    expand = (cell_row == iota((width_z // 2, width_z), 0)).astype(f32).astype(bf16)
    number = axis[...].reshape(n_x * n_y, width_z // 2).astype(f32).astype(bf16)
    index[...] = dot(number, expand).reshape(n_x, n_y, width_z)

    start = stacked([jnp.where(alive, pos[0, 0], far_away), pos[1, 0], pos[2, 0]])
    kick = jnp.broadcast_to((timestep * stiffness * cutoff) / mass[0], (8, slots))
    src[0, OWN] = jnp.where(comp == 3, kick, start * (1.0 / cutoff))

    double = (iota((SUB * rows, SUB * width_y), 0) >> 1 == iota((SUB * rows, SUB * width_y), 1)).astype(bf16)
    small[-1].wait()
    for i in range(n_x):
        at = pl.ds(i * SUB, SUB)
        filled = occupancy[at].reshape(SUB * width_y, width_z).astype(f32).astype(bf16)
        held[at] = dot(double, filled).reshape(SUB, rows, width_z)
    row = iota((8, width_z), 0)
    odd = (row & 1).astype(f32)
    stays_1 = jnp.broadcast_to(shift_x, (8, width_z)) <= 2
    stays_2 = jnp.broadcast_to(shift_x, (8, width_z)) <= 1
    later = ((row >> 1) + shift_y) >= SUB
    even = ((iota((8, width_z), 1) + shift_z) & 1) == 0
    halves = jnp.where((row & 3) == 3, 0.5, 1.0)
    blank = jnp.zeros((8, width_z), f32)

    def finish(i):
        def straddling(c, j):
            now = cell[i, c, pl.ds(8 * j, 8), :] if j < n_y else blank
            before = cell[i, c, pl.ds(8 * (j - 1), 8), :] if j > 0 else blank
            return jnp.where(later, before, now)

        for t in range(tiles_y):
            blocks = [
                straddling(q & 3, 2 * t + (q >> 2)) if 2 * t + (q >> 2) <= n_y else blank
                for q in range(8)
            ]
            tile = fold(blocks) * halves
            partner = jnp.where(even, pltpu.roll(tile, width_z - 1, 1), pltpu.roll(tile, 1, 1))
            sums[i, pl.ds(8 * t, 8), :] += tile + partner

    def gather(i):
        for b in range(n_y):
            at = pl.ds(8 * b, 8)
            filled = [held[i * SUB + r, at, :] for r in range(SUB)]
            live = [f > odd for f in filled]
            for c in range(4):
                v = filled
                if c < 3:
                    v = [jnp.where(live[r], out[c, i * SUB + r, at, :], 0.0) for r in range(SUB)]
                front = v[0] + v[1]
                back = v[3] + v[2]
                stay = jnp.where(stays_1, jnp.where(stays_2, front + v[2], front), v[0])
                move = jnp.where(stays_1, jnp.where(stays_2, v[3], back), back + v[1])
                cell[i, c, at, :] = stay if i == 0 else cell[i, c, at, :] + stay
                cell[i + 1, c, at, :] = move

    for i in range(n_x):
        chunks[i].wait()
        gather(i)
        if i > 0:
            finish(i - 1)
    finish(n_x - 1)
    finish(n_x)

    pl.semaphore_wait(barrier, len(WIDE))

    def exchange(step):
        mine = src.at[step, OWN, pl.ds(0, 4)]
        copies = {}
        for a, b in AROUND:
            k = slot_of(a, b)
            copies[k] = remote(
                mine, src.at[step, 8 - k, pl.ds(0, 4)],
                src_send.at[step, k], src_got.at[step, 8 - k], device(a, b),
            )
            copies[k].start()
        return list(copies.values())

    sends = exchange(0)

    at_low, at_high = (pl.ds(0, 4), pl.ds(n_y * SUB, 4))
    every = pl.ds(0, n_x + 1)
    halo = [
        (sums.at[n_x], halo_x.at[0], (1, 0)),
        (sums.at[0], halo_x.at[1], (-1, 0)),
        (sums.at[every, at_high], halo_y.at[0, every, at_low], (0, 1)),
        (sums.at[every, at_low], halo_y.at[1, every, at_low], (0, -1)),
        (sums.at[n_x, at_high], halo_c.at[0, at_low], (1, 1)),
        (sums.at[n_x, at_low], halo_c.at[1, at_low], (1, -1)),
        (sums.at[0, at_high], halo_c.at[2, at_low], (-1, 1)),
        (sums.at[0, at_low], halo_c.at[3, at_low], (-1, -1)),
    ]
    halo = [
        remote(source, target, halo_send.at[k], halo_got.at[k], device(*where))
        for k, (source, target, where) in enumerate(halo)
    ]
    for copy in halo:
        copy.start()
    edges = [
        (index.at[0], edge_x, (-1, 0)),
        (index.at[pl.ds(0, n_x), 0], edge_y, (0, -1)),
        (index.at[0, pl.ds(0, 1)], edge_c.at[pl.ds(0, 1)], (-1, -1)),
    ]
    edges = [
        remote(source, target, edge_send.at[k], edge_got.at[k], device(*where))
        for k, (source, target, where) in enumerate(edges)
    ]
    for copy in edges:
        copy.start()

    period = (width_z // 2) / cutoff
    step_x, step_y = (n_x / cutoff, n_y / cutoff)
    side = 1 - 2 * (me_x & 1)
    quick, slow = (side, -side)

    def source(step, a, b):
        slot = slot_of(a, b)
        offset = None if isinstance(a, int) else a.astype(f32) * step_x

        def read():
            x, y, z = [src[step, slot, pl.ds(c, 1), :] for c in range(3)]
            x = x if offset is None else x + offset
            return (x, y if b == 0 else y + b * step_y, z, period)

        return read

    def arrived(step, a, b):
        slot = slot_of(a, b)
        remote(
            src.at[step, OWN, pl.ds(0, 4)], src.at[step, slot, pl.ds(0, 4)],
            src_send.at[step, slot], src_got.at[step, slot], device(0, 1),
        ).wait_recv()

    def early_forces(step):
        for b in (-1, 1):
            arrived(step, 0, b)
        force_pass(own, force, [source(step, 0, b) for b in (0, -1, 1)], True)
        for b in (-1, 0, 1):
            arrived(step, quick, b)
        force_pass(own, force, [source(step, quick, b) for b in (-1, 0, 1)], False)

    def late_arrivals(step):
        for b in (-1, 0, 1):
            arrived(step, slow, b)

    def late_forces(step):
        late_arrivals(step)
        force_pass(own, force, [source(step, slow, b) for b in (-1, 0, 1)], False)
        return force_rows(force)

    own_columns(own, src[0, OWN])
    early_forces(0)
    push = late_forces(0)

    for copy in halo:
        copy.wait_recv()
    total[...] = sums[...]
    total[0] += halo_x[0]
    total[n_x] += halo_x[1]
    for i in range(n_x + 1):
        total[i, at_low, :] += halo_y[0, i, at_low, :]
        total[i, at_high, :] += halo_y[1, i, at_low, :]
    total[0, at_low, :] += halo_c[0, at_low, :]
    total[0, at_high, :] += halo_c[1, at_low, :]
    total[n_x, at_low, :] += halo_c[2, at_low, :]
    total[n_x, at_high, :] += halo_c[3, at_low, :]
    for copy in edges:
        copy.wait_recv()

    chosen = (iota((width_z, slots), 0) == layer_z).astype(f32).astype(bf16)
    block = total[...].reshape((n_x + 1) * tiles_y * 8, width_z)
    at_z = sum(dot(term, chosen) for term in terms(block, 2)[::-1])
    picked = jnp.zeros((8, slots), f32)
    for i in range(n_x + 1):
        for t in range(tiles_y):
            n = 8 * (i * tiles_y + t)
            picked = picked + jnp.where(in_tile(i, t), at_z[n : n + 8], 0.0)
    picked = picked + pltpu.roll(picked, 4, 0)
    numbers = jnp.concatenate(
        [index[...].reshape(n_x * n_y, width_z), edge_x[...], edge_y[...], edge_c[...]], axis=0
    )
    at_z = dot(numbers.astype(bf16), chosen)
    wanted = [place - comp == i * (n_y + 1) for i in range(n_x + 1)]
    wanted.append(place - comp * (n_y + 1) == n_y)
    wanted.append(jnp.logical_and(comp == 0, place == n_x * (n_y + 1) + n_y))
    found = jnp.zeros((8, slots), f32)
    for n, mask in enumerate(wanted):
        found = found + jnp.where(mask, at_z[8 * n : 8 * n + 8], 0.0)
    found = jnp.sum(found, axis=0, keepdims=True)
    heavy = jnp.maximum(picked[3:4], fill_mass)
    mean = [picked[c : c + 1] / heavy for c in range(3)]
    n = axes_of(found)
    rel = [vel[c, 0] - mean[c] for c in range(3)]
    cross = [n[1] * rel[2] - n[2] * rel[1], n[2] * rel[0] - n[0] * rel[2], n[0] * rel[1] - n[1] * rel[0]]
    along = n[0] * rel[0] + n[1] * rel[1] + n[2] * rel[2]
    speed = stacked([
        mean[c] + cos_angle * rel[c] + sin_angle * cross[c] + (1.0 - cos_angle) * along * n[c]
        for c in range(3)
    ])
    place_now = start

    def cell_fields(i, rows_of):
        for b in range(n_y):
            pair = [
                [jnp.where(later, total[i, pl.ds(4 * (b + 1) + c, 1), :], total[i, pl.ds(4 * b + c, 1), :])
                 for c in range(4)],
                [jnp.where(later, normals[c, pl.ds(rows_of(b + 1), 1), :], normals[c, pl.ds(rows_of(b), 1), :])
                 for c in range(3)],
            ]
            scale = 1.0 / jnp.maximum(pair[0][3], fill_mass)
            for c in range(3):
                fields[i, b, c] = pair[0][c] * scale
                fields[i, b, 3 + c] = pair[1][c]

    def turn(x, carry):
        at_cell = (x + shift_x) >> 2
        for b in range(n_y):
            at = pl.ds(8 * b, 8)
            mean = [fields[at_cell, b, c] for c in range(3)]
            n = [fields[at_cell, b, 3 + c] for c in range(3)]
            old = [out[c, x, at, :] for c in range(3)]
            rel = [old[c] - mean[c] for c in range(3)]
            along = (1.0 - cos_angle) * (n[0] * rel[0] + n[1] * rel[1] + n[2] * rel[2])
            cross = [
                n[1] * rel[2] - n[2] * rel[1],
                n[2] * rel[0] - n[0] * rel[2],
                n[0] * rel[1] - n[1] * rel[0],
            ]
            live = held[x, at, :] > odd
            for c in range(3):
                new = mean[c] + cos_angle * rel[c] + sin_angle * cross[c] + along * n[c]
                out[c, x, at, :] = jnp.where(live, new, old[c])
        return carry

    def idle_work(step):
        if step == 1:
            for c, part in enumerate(axes_of(numbers)):
                normals[c] = part

            def inner(i, carry):
                cell_fields(i, lambda b: i * n_y + b if b < n_y else n_x * n_y + 8 + i)
                return carry

            lax.fori_loop(0, n_x, inner, 0)
            cell_fields(n_x, lambda b: n_x * n_y + b if b < n_y else n_x * n_y + 16)
            lax.fori_loop(0, width_x // 2, turn, 0)
        if step == 2:
            lax.fori_loop(width_x // 2, width_x, turn, 0)

    speed = speed + push * kick
    place_now = place_now + timestep * speed
    src[1, OWN] = place_now * (1.0 / cutoff)
    sends = sends + exchange(1)
    own_columns(own, src[1, OWN])
    idle_work(1)
    early_forces(1)
    push = late_forces(1)

    speed = speed + push * kick
    place_now = place_now + timestep * speed
    mine = wide_slot(0, 0)
    wide[mine] = place_now * (1.0 / cutoff)
    spread = []
    for a, b in WIDE:
        k = wide_slot(a, b)
        spread.append(
            remote(
                wide.at[mine, pl.ds(0, 4)], wide.at[24 - k, pl.ds(0, 4)],
                wide_send.at[k], wide_got.at[24 - k], device(a, b),
            )
        )
    for copy in spread:
        copy.start()
    idle_work(2)
    first[...] = src[0]
    second[...] = src[1]
    tiles[0] = place_now
    tiles[1] = speed
    tiles[2] = stacked([pos[c, 0] for c in range(3)])
    tiles[3] = stacked([vel[c, 0] for c in range(3)])
    tiles[4] = jnp.broadcast_to(jnp.where(alive, 1.0, 0.0), (8, slots))
    for copy in spread:
        copy.wait_recv()
    third[...] = wide[...]
    for copy in sends + halo + edges + spread:
        copy.wait_send()


def finish_kernel(
    shape, turned, first, second, third, tiles, out, pos_out, vel_out, own, force, later, sem
):
    width_x, width_y, width_z = shape
    n_x, n_y = (width_x // SUB, width_y // SUB)
    slots = first.shape[2]
    copies = []
    for c in range(3):
        copies.append(pltpu.make_async_copy(turned.at[c], out.at[c], sem.at[c]))
        copies[-1].start()

    period = (width_z // 2) / cutoff
    step_x, step_y = (n_x / cutoff, n_y / cutoff)
    lane = iota((slots, slots), 1)
    block = 16 if slots % 16 == 0 else 8

    def columns(group):
        pad = jnp.zeros((slots - 8 * len(group), slots), f32)
        flipped = jnp.concatenate(group + [pad], axis=0).T
        for n in range(len(group)):
            for c in range(3):
                own[n, c] = jnp.broadcast_to(flipped[:, 8 * n + c : 8 * n + c + 1], (slots, slots))

    def pushes(n, trips, sources):
        def body(r, carry):
            at = pl.ds(pl.multiple_of(r * block, block), block)
            rows = [own[n, c, at, :] for c in range(3)]
            total = None
            for ref, k, a, b in sources:
                x, y, z = [ref[k, pl.ds(c, 1), :] for c in range(3)]
                x = x if a == 0 else x + a * step_x
                y = y if b == 0 else y + b * step_y
                parts = pair_sums(rows, (x, y, z, period))
                total = parts if total is None else [t + p for t, p in zip(total, parts)]
            for c in range(3):
                force[n, c, at, :] = total[c]
            return carry

        lax.fori_loop(0, trips, body, 0)

    def rows_of(number):
        out = jnp.zeros((slots, slots), f32)
        for n in range(number):
            for c in range(3):
                out = jnp.where(lane == 8 * n + c, jnp.sum(force[n, c], axis=1, keepdims=True), out)
        return out.T

    dead = [third[wide_slot(a, b), pl.ds(0, 1), :] > 0.1 * far_away for a, b in RING]
    trips = [
        (jnp.sum(jnp.where(gone, 0.0, 1.0)).astype(jnp.int32) + (block - 1)) // block for gone in dead
    ]
    columns([third[wide_slot(a, b)] for a, b in RING])
    for n, (a, b) in enumerate(RING):
        pushes(n, trips[n], [(third, wide_slot(a + p, b + q), p, q) for p, q in RING])
    push = rows_of(len(RING))
    speed, place = (tiles[1], tiles[0])
    for n, (a, b) in enumerate(RING):
        now = third[wide_slot(a, b)]
        mine = push[8 * n : 8 * n + 8]
        kick = jnp.broadcast_to(first[n, pl.ds(3, 1), :], (8, slots))
        if n == OWN:
            speed = speed + mine * kick
            place = place + timestep * speed
            moved = place * (1.0 / cutoff)
        else:
            moved = now + (now - second[n]) + (timestep / cutoff) * (mine * kick)
        later[n] = jnp.where(jnp.broadcast_to(dead[n], (8, slots)), now, moved)
    columns([later[OWN]])
    pushes(0, trips[OWN], [(later, n, a, b) for n, (a, b) in enumerate(RING)])
    kick = jnp.broadcast_to(first[OWN, pl.ds(3, 1), :], (8, slots))
    speed = speed + rows_of(1)[:8] * kick
    place = place + timestep * speed
    alive = tiles[4] > 0
    place = jnp.where(alive, place, tiles[2])
    speed = jnp.where(alive, speed, tiles[3])
    for c in range(3):
        pos_out[c, 0] = place[c : c + 1]
        vel_out[c, 0] = speed[c : c + 1]
    for copy in copies:
        copy.wait()


def per_device(
    solvent_vel, occupancy, grid_shift, axis_index, colloid_pos, colloid_vel, colloid_mass, colloid_count
):
    shape = occupancy.shape
    width_x, width_y, width_z = shape
    rows = 2 * width_y
    n_x, n_y = (width_x // SUB, width_y // SUB)
    slots = colloid_mass.shape[2]
    solvent = solvent_vel.reshape(3, width_x, rows, width_z)
    smem = pl.BlockSpec(memory_space=pltpu.SMEM)
    vmem = pl.BlockSpec(memory_space=pltpu.VMEM)
    hbm = pl.BlockSpec(memory_space=pltpu.HBM)
    tall = (n_y + 2) // 2 * 8
    dma = pltpu.SemaphoreType.DMA

    def in_hbm(x):
        return pltpu.with_memory_space_constraint(x, pltpu.HBM)

    turned, *states = pl.pallas_call(
        functools.partial(collide_kernel, shape),
        out_shape=[
            pltpu.VMEM(solvent.shape, f32),
            pltpu.VMEM((9, 8, slots), f32),
            pltpu.VMEM((9, 8, slots), f32),
            pltpu.VMEM((25, 8, slots), f32),
            pltpu.VMEM((5, 8, slots), f32),
        ],
        in_specs=[hbm, smem] + [hbm] * 6,
        out_specs=[vmem] * 5,
        scratch_shapes=[
            pltpu.SMEM(grid_shift.shape, jnp.int32),
            pltpu.VMEM(colloid_pos.shape, f32),
            pltpu.VMEM(colloid_vel.shape, f32),
            pltpu.VMEM(colloid_mass.shape, f32),
            pltpu.VMEM(axis_index.shape, jnp.int32),
            pltpu.VMEM(shape, jnp.int32),
            pltpu.VMEM((width_x, rows, width_z), f32),
            pltpu.VMEM((n_x + 1, 4, rows, width_z), f32),
            pltpu.VMEM((n_x + 1, tall, width_z), f32),
            pltpu.VMEM((n_x + 1, tall, width_z), f32),
            pltpu.VMEM((n_x, n_y, width_z), f32),
            pltpu.VMEM((8, width_z), f32),
            pltpu.VMEM((8, width_z), f32),
            pltpu.VMEM((8, width_z), f32),
            pltpu.VMEM((3, n_x * n_y + 24, width_z), f32),
            pltpu.VMEM((n_x + 1, n_y, 6, 8, width_z), f32),
            pltpu.VMEM((2, tall, width_z), f32),
            pltpu.VMEM((2, n_x + 1, 8, width_z), f32),
            pltpu.VMEM((4, 8, width_z), f32),
            pltpu.VMEM((2, 9, 8, slots), f32),
            pltpu.VMEM((25, 8, slots), f32),
            pltpu.VMEM((3, slots, slots), f32),
            pltpu.VMEM((3, slots, slots), f32),
            dma((6,)),
            dma((n_x,)),
            dma((8,)),
            dma((8,)),
            dma((3,)),
            dma((3,)),
            dma((2, 9)),
            dma((2, 9)),
            dma((25,)),
            dma((25,)),
        ],
        compiler_params=pltpu.CompilerParams(
            collective_id=0, has_side_effects=True, vmem_limit_bytes=32 * 2**20
        ),
        name="collide",
    )(
        in_hbm(grid_shift), colloid_count, in_hbm(solvent), in_hbm(occupancy), in_hbm(axis_index),
        in_hbm(colloid_pos), in_hbm(colloid_vel), in_hbm(colloid_mass),
    )

    solvent_out, pos_out, vel_out = pl.pallas_call(
        functools.partial(finish_kernel, shape),
        out_shape=[
            jax.ShapeDtypeStruct(solvent.shape, f32),
            jax.ShapeDtypeStruct(colloid_pos.shape, f32),
            jax.ShapeDtypeStruct(colloid_vel.shape, f32),
        ],
        in_specs=[vmem] * 5,
        out_specs=[hbm, vmem, vmem],
        scratch_shapes=[
            pltpu.VMEM((9, 3, slots, slots), f32),
            pltpu.VMEM((9, 3, slots, slots), f32),
            pltpu.VMEM((9, 8, slots), f32),
            dma((3,)),
        ],
        compiler_params=pltpu.CompilerParams(vmem_limit_bytes=16 * 2**20),
        name="finish",
    )(turned, *states)
    return (solvent_out.reshape(solvent_vel.shape), pos_out, vel_out)


def solution(mesh):
    return jax.shard_map(
        per_device,
        mesh=mesh,
        in_specs=(
            P(None, "gx", "yz", None, None),
            P("gx", "yz", None),
            P(),
            P("gx", "yz", None),
            P(None, "gx", "yz", None),
            P(None, "gx", "yz", None),
            P("gx", "yz", None),
            P("gx", "yz"),
        ),
        out_specs=(
            P(None, "gx", "yz", None, None),
            P(None, "gx", "yz", None),
            P(None, "gx", "yz", None),
        ),
        check_vma=False,
    )
```

```python
import functools
import math

import jax
import jax.numpy as jnp
from jax import lax
from jax.experimental import pallas as pl
from jax.experimental.pallas import tpu as pltpu
from jax.sharding import PartitionSpec as P

SUB = 4
SUBSTEPS = 4
DIRECTIONS = 64

turn_angle = 130.0 * math.pi / 180.0
cos_angle = math.cos(turn_angle)
sin_angle = math.sin(turn_angle)
golden = math.pi * (3.0 - math.sqrt(5.0))
cutoff = 1.5
stiffness = 20.0
timestep = 0.05
fill_mass = 16.0
far_away = 1.0e9
MESH = pl.DeviceIdType.MESH
f32 = jnp.float32
bf16 = jnp.bfloat16
RING = [(a, b) for a in (-1, 0, 1) for b in (-1, 0, 1)]
AROUND = [pair for pair in RING if pair != (0, 0)]
OWN = 4


def iota(shape, dim):
    return lax.broadcasted_iota(jnp.int32, shape, dim)


def slot_of(a, b):
    return (a + 1) * 3 + b + 1


def folded(b, size_y):
    return 2 if b == -2 and size_y == 4 else b


def wide_slot(a, b, size_y):
    return (a + 2) * 5 + folded(b, size_y) + 2


def wide_pairs(size_y):
    return [
        (a, b) for a in (-1, 1, -2, 2, 0) for b in (-1, 0, 1, -2, 2)
        if (a, b) != (0, 0) and folded(b, size_y) == b
    ]


def sides(me_x):
    quick = 1 - 2 * (me_x & 1)
    return (0, quick, -quick)


def reader(ref, slot, p, q, steps):
    period, step_x, step_y = steps

    def read():
        x, y, z = [ref[slot, pl.ds(c, 1), :] for c in range(3)]
        if not isinstance(p, int):
            x = x + p.astype(f32) * step_x
        elif p != 0:
            x = x + p * step_x
        return (x, y if q == 0 else y + q * step_y, z, period)

    return read


def terms(value, number):
    out = []
    for _ in range(number - 1):
        part = value.astype(bf16)
        out.append(part)
        value = value - part.astype(f32)
    return out + [value.astype(bf16)]


def dot(left, right, contract=((1,), (0,))):
    return lax.dot_general(left, right, (contract, ((), ())), preferred_element_type=f32)


def wrapped(value, size):
    return jnp.where(value >= size, value - size, value)


def layer_of(row, scale, width):
    return jnp.clip(jnp.floor(row * scale).astype(jnp.int32), 0, width - 1)


def fold(values):
    row = iota(values[0].shape, 0)
    low = row < 4
    values = [
        jnp.where(low, a, b) + pltpu.roll(jnp.where(low, b, a), 4, 0)
        for a, b in zip(values[:4], values[4:])
    ]
    for dist in (2, 1):
        low = (row & dist) == 0
        values = [
            jnp.where(low, a, b) + jnp.where(low, pltpu.roll(a, 8 - dist, 0), pltpu.roll(b, dist, 0))
            for a, b in zip(values[:dist], values[dist:])
        ]
    return values[0]


def stacked(rows):
    comp = iota((8, rows[0].shape[1]), 0)
    out = jnp.zeros((8, rows[0].shape[1]), f32)
    for c, row in enumerate(rows):
        out = jnp.where(comp == c, row, out)
    return out


def axes_of(number):
    height = 1.0 - (2.0 * number + 1.0) / DIRECTIONS
    radius = jnp.sqrt(1.0 - height * height)
    phase = number * golden
    return [radius * jnp.cos(phase), radius * jnp.sin(phase), height]


def pair_sums(own_rows, source):
    dx, dy, dz = [o - s for o, s in zip(own_rows, source[:3])]
    period = source[3]
    half = 0.5 * period
    dz = dz + jnp.where(dz > half, -period, jnp.where(dz < -half, period, 0.0))
    reach = jnp.maximum(1.0 - (dx * dx + dy * dy + dz * dz), 0.0)
    weight = reach * reach
    return [weight * dx, weight * dy, weight * dz]


def force_pass(own, force, sources, first):
    slots = own.shape[-1]
    wide = 32 if slots % 32 == 0 else 8

    def block(r, carry):
        at = pl.ds(pl.multiple_of(r * wide, wide), wide)
        rows = [own[c, at, :] for c in range(3)]
        total = None if first else [force[c, at, :] for c in range(3)]
        for source in sources:
            parts = pair_sums(rows, source())
            total = parts if total is None else [t + p for t, p in zip(total, parts)]
        for c in range(3):
            force[c, at, :] = total[c]
        return carry

    lax.fori_loop(0, slots // wide, block, 0)


def force_rows(force):
    slots = force.shape[1]
    comp = iota((8, slots), 0)
    out = None
    for c in range(3):
        pick = (comp == c).astype(f32).astype(bf16)
        for term in terms(force[c], 2)[::-1]:
            part = dot(pick, term, ((1,), (1,)))
            out = part if out is None else out + part
    return out


def flipped(tiles):
    slots = tiles[0].shape[1]
    pad = jnp.zeros((slots - 8 * len(tiles), slots), f32)
    return jnp.concatenate(tiles + [pad], axis=0).T


def own_columns(own, tile):
    slots = tile.shape[1]
    block = flipped([tile])
    for c in range(3):
        own[c] = jnp.broadcast_to(block[:, c : c + 1], (slots, slots))


def collide_kernel(
    shape, shift_hbm, count, solvent_hbm, occupancy_hbm, axis_hbm, pos_hbm, vel_hbm, mass_hbm,
    out, first, second, third, tiles, early, begun,
    shift, pos, vel, mass, axis, occupancy, held, cell, sums, total, index, edge_x, edge_y, edge_c,
    normals, fields, halo_x, halo_y, halo_c, src, wide, force, own,
    small_sem, chunk_sem, halo_send, halo_got, edge_send, edge_got, src_send, src_got,
    wide_send, wide_got,
):
    width_x, width_y, width_z = shape
    n_x, n_y = (width_x // SUB, width_y // SUB)
    rows = 2 * width_y
    slots = mass.shape[2]
    me_x, me_y = (lax.axis_index("gx"), lax.axis_index("yz"))
    size_x, size_y = (lax.axis_size("gx"), lax.axis_size("yz"))

    def device(a, b):
        return (lax.rem(me_x + a + size_x, size_x), lax.rem(me_y + b + size_y, size_y))

    def remote(source, target, send, receive, where):
        return pltpu.make_async_remote_copy(
            src_ref=source, dst_ref=target, send_sem=send, recv_sem=receive,
            device_id=where, device_id_type=MESH,
        )

    around = wide_pairs(size_y)
    edge_c[...] = jnp.zeros_like(edge_c)
    barrier = pltpu.get_barrier_semaphore()
    for a, b in around:
        pl.semaphore_signal(barrier, inc=1, device_id=device(a, b), device_id_type=MESH)

    small = [
        pltpu.make_async_copy(source, target, small_sem.at[k])
        for k, (source, target) in enumerate(
            [
                (shift_hbm, shift), (pos_hbm, pos), (vel_hbm, vel),
                (mass_hbm, mass), (axis_hbm, axis), (occupancy_hbm, occupancy),
            ]
        )
    ]
    chunks = [
        pltpu.make_async_copy(
            solvent_hbm.at[:, pl.ds(i * SUB, SUB)], out.at[:, pl.ds(i * SUB, SUB)], chunk_sem.at[i]
        )
        for i in range(n_x)
    ]
    for copy in small + chunks:
        copy.start()
    for copy in small[:-1]:
        copy.wait()
    shift_x, shift_y, shift_z = (shift[0], shift[1], shift[2])

    alive = iota((1, slots), 1) < count[0, 0]
    cell_x = (layer_of(pos[0, 0], SUB, width_x) + shift_x) >> 2
    cell_y = (layer_of(pos[1, 0], SUB, width_y) + shift_y) >> 2
    layer_z = layer_of(pos[2, 0], 2.0, width_z)
    cell_z = wrapped(layer_z + shift_z, width_z) >> 1
    place = cell_x * (n_y + 1) + cell_y
    weight = jnp.where(alive, mass[0], 0.0)
    comp = iota((8, slots), 0)
    four = comp & 3
    values = jnp.where(
        four == 0, vel[0, 0] * weight,
        jnp.where(four == 1, vel[1, 0] * weight, jnp.where(four == 2, vel[2, 0] * weight, weight)),
    )
    place_half = place - (comp >> 2)
    place_last = jnp.where(comp < 4, place, -1)
    tiles_y = (n_y + 2) // 2

    def in_tile(i, t):
        return (place_half if 2 * t < n_y else place_last) == i * (n_y + 1) + 2 * t

    spread = [
        jnp.where(in_tile(i, t), values, 0.0) for i in range(n_x + 1) for t in range(tiles_y)
    ]
    near = (wrapped(iota((width_z, slots), 0) + shift_z, width_z) >> 1) == cell_z
    near = near.astype(f32).astype(bf16)
    deposit = sum(
        dot(term, near, ((1,), (1,))) for term in terms(jnp.concatenate(spread, axis=0), 3)[::-1]
    )
    sums[...] = deposit.reshape(n_x + 1, tiles_y * 8, width_z)

    cell_row = wrapped(iota((width_z // 2, width_z), 1) + shift_z, width_z) >> 1
    expand = (cell_row == iota((width_z // 2, width_z), 0)).astype(f32).astype(bf16)
    number = axis[...].reshape(n_x * n_y, width_z // 2).astype(f32).astype(bf16)
    index[...] = dot(number, expand).reshape(n_x, n_y, width_z)

    start = stacked([jnp.where(alive, pos[0, 0], far_away), pos[1, 0], pos[2, 0]])
    kick = jnp.broadcast_to((timestep * stiffness * cutoff) / mass[0], (8, slots))
    src[0, OWN] = jnp.where(comp == 3, kick, start * (1.0 / cutoff))

    double = (iota((SUB * rows, SUB * width_y), 0) >> 1 == iota((SUB * rows, SUB * width_y), 1)).astype(bf16)
    small[-1].wait()
    for i in range(n_x):
        at = pl.ds(i * SUB, SUB)
        filled = occupancy[at].reshape(SUB * width_y, width_z).astype(f32).astype(bf16)
        held[at] = dot(double, filled).reshape(SUB, rows, width_z)
    row = iota((8, width_z), 0)
    odd = (row & 1).astype(f32)
    stays_1 = jnp.broadcast_to(shift_x, (8, width_z)) <= 2
    stays_2 = jnp.broadcast_to(shift_x, (8, width_z)) <= 1
    later = ((row >> 1) + shift_y) >= SUB
    even = ((iota((8, width_z), 1) + shift_z) & 1) == 0
    halves = jnp.where((row & 3) == 3, 0.5, 1.0)
    blank = jnp.zeros((8, width_z), f32)

    def finish(i):
        def straddling(c, j):
            now = cell[i, c, pl.ds(8 * j, 8), :] if j < n_y else blank
            before = cell[i, c, pl.ds(8 * (j - 1), 8), :] if j > 0 else blank
            return jnp.where(later, before, now)

        for t in range(tiles_y):
            blocks = [
                straddling(q & 3, 2 * t + (q >> 2)) if 2 * t + (q >> 2) <= n_y else blank
                for q in range(8)
            ]
            tile = fold(blocks) * halves
            partner = jnp.where(even, pltpu.roll(tile, width_z - 1, 1), pltpu.roll(tile, 1, 1))
            sums[i, pl.ds(8 * t, 8), :] += tile + partner

    def gather(i):
        for b in range(n_y):
            at = pl.ds(8 * b, 8)
            filled = [held[i * SUB + r, at, :] for r in range(SUB)]
            live = [f > odd for f in filled]
            for c in range(4):
                v = filled
                if c < 3:
                    v = [jnp.where(live[r], out[c, i * SUB + r, at, :], 0.0) for r in range(SUB)]
                front = v[0] + v[1]
                back = v[3] + v[2]
                stay = jnp.where(stays_1, jnp.where(stays_2, front + v[2], front), v[0])
                move = jnp.where(stays_1, jnp.where(stays_2, v[3], back), back + v[1])
                cell[i, c, at, :] = stay if i == 0 else cell[i, c, at, :] + stay
                cell[i + 1, c, at, :] = move

    for i in range(n_x):
        chunks[i].wait()
        gather(i)
        if i > 0:
            finish(i - 1)
    finish(n_x - 1)
    finish(n_x)

    pl.semaphore_wait(barrier, len(around))

    def exchange(step):
        mine = src.at[step, OWN, pl.ds(0, 4)]
        copies = {}
        for a, b in AROUND:
            k = slot_of(a, b)
            copies[k] = remote(
                mine, src.at[step, 8 - k, pl.ds(0, 4)],
                src_send.at[step, k], src_got.at[step, 8 - k], device(a, b),
            )
            copies[k].start()
        return list(copies.values())

    sends = exchange(0)

    at_low, at_high = (pl.ds(0, 4), pl.ds(n_y * SUB, 4))
    every = pl.ds(0, n_x + 1)
    halo = [
        (sums.at[n_x], halo_x.at[0], (1, 0)),
        (sums.at[0], halo_x.at[1], (-1, 0)),
        (sums.at[every, at_high], halo_y.at[0, every, at_low], (0, 1)),
        (sums.at[every, at_low], halo_y.at[1, every, at_low], (0, -1)),
        (sums.at[n_x, at_high], halo_c.at[0, at_low], (1, 1)),
        (sums.at[n_x, at_low], halo_c.at[1, at_low], (1, -1)),
        (sums.at[0, at_high], halo_c.at[2, at_low], (-1, 1)),
        (sums.at[0, at_low], halo_c.at[3, at_low], (-1, -1)),
    ]
    halo = [
        remote(source, target, halo_send.at[k], halo_got.at[k], device(*where))
        for k, (source, target, where) in enumerate(halo)
    ]
    for copy in halo:
        copy.start()
    edges = [
        (index.at[0], edge_x, (-1, 0)),
        (index.at[pl.ds(0, n_x), 0], edge_y, (0, -1)),
        (index.at[0, pl.ds(0, 1)], edge_c.at[pl.ds(0, 1)], (-1, -1)),
    ]
    edges = [
        remote(source, target, edge_send.at[k], edge_got.at[k], device(*where))
        for k, (source, target, where) in enumerate(edges)
    ]
    for copy in edges:
        copy.start()

    steps = ((width_z // 2) / cutoff, n_x / cutoff, n_y / cutoff)
    columns_x = sides(me_x)
    quick, slow = columns_x[1:]

    def source(step, a, b):
        return reader(src.at[step], slot_of(a, b), a, b, steps)

    def arrived(step, a, b):
        slot = slot_of(a, b)
        remote(
            src.at[step, OWN, pl.ds(0, 4)], src.at[step, slot, pl.ds(0, 4)],
            src_send.at[step, slot], src_got.at[step, slot], device(0, 1),
        ).wait_recv()

    def early_forces(step):
        for b in (-1, 1):
            arrived(step, 0, b)
        force_pass(own, force, [source(step, 0, b) for b in (0, -1, 1)], True)
        for b in (-1, 0, 1):
            arrived(step, quick, b)
        force_pass(own, force, [source(step, quick, b) for b in (-1, 0, 1)], False)

    def late_arrivals(step):
        for b in (-1, 0, 1):
            arrived(step, slow, b)

    def late_forces(step):
        late_arrivals(step)
        force_pass(own, force, [source(step, slow, b) for b in (-1, 0, 1)], False)
        return force_rows(force)

    own_columns(own, src[0, OWN])
    early_forces(0)
    push = late_forces(0)

    for copy in halo:
        copy.wait_recv()
    total[...] = sums[...]
    total[0] += halo_x[0]
    total[n_x] += halo_x[1]
    for i in range(n_x + 1):
        total[i, at_low, :] += halo_y[0, i, at_low, :]
        total[i, at_high, :] += halo_y[1, i, at_low, :]
    total[0, at_low, :] += halo_c[0, at_low, :]
    total[0, at_high, :] += halo_c[1, at_low, :]
    total[n_x, at_low, :] += halo_c[2, at_low, :]
    total[n_x, at_high, :] += halo_c[3, at_low, :]
    for copy in edges:
        copy.wait_recv()

    chosen = (iota((width_z, slots), 0) == layer_z).astype(f32).astype(bf16)
    block = total[...].reshape((n_x + 1) * tiles_y * 8, width_z)
    at_z = sum(dot(term, chosen) for term in terms(block, 2)[::-1])
    picked = jnp.zeros((8, slots), f32)
    for i in range(n_x + 1):
        for t in range(tiles_y):
            n = 8 * (i * tiles_y + t)
            picked = picked + jnp.where(in_tile(i, t), at_z[n : n + 8], 0.0)
    picked = picked + pltpu.roll(picked, 4, 0)
    numbers = jnp.concatenate(
        [index[...].reshape(n_x * n_y, width_z), edge_x[...], edge_y[...], edge_c[...]], axis=0
    )
    at_z = dot(numbers.astype(bf16), chosen)
    wanted = [place - comp == i * (n_y + 1) for i in range(n_x + 1)]
    wanted.append(place - comp * (n_y + 1) == n_y)
    wanted.append(jnp.logical_and(comp == 0, place == n_x * (n_y + 1) + n_y))
    found = jnp.zeros((8, slots), f32)
    for n, mask in enumerate(wanted):
        found = found + jnp.where(mask, at_z[8 * n : 8 * n + 8], 0.0)
    found = jnp.sum(found, axis=0, keepdims=True)
    heavy = jnp.maximum(picked[3:4], fill_mass)
    mean = [picked[c : c + 1] / heavy for c in range(3)]
    n = axes_of(found)
    rel = [vel[c, 0] - mean[c] for c in range(3)]
    cross = [n[1] * rel[2] - n[2] * rel[1], n[2] * rel[0] - n[0] * rel[2], n[0] * rel[1] - n[1] * rel[0]]
    along = n[0] * rel[0] + n[1] * rel[1] + n[2] * rel[2]
    speed = stacked([
        mean[c] + cos_angle * rel[c] + sin_angle * cross[c] + (1.0 - cos_angle) * along * n[c]
        for c in range(3)
    ])
    place_now = start

    def cell_fields(i, rows_of):
        for b in range(n_y):
            pair = [
                [jnp.where(later, total[i, pl.ds(4 * (b + 1) + c, 1), :], total[i, pl.ds(4 * b + c, 1), :])
                 for c in range(4)],
                [jnp.where(later, normals[c, pl.ds(rows_of(b + 1), 1), :], normals[c, pl.ds(rows_of(b), 1), :])
                 for c in range(3)],
            ]
            scale = 1.0 / jnp.maximum(pair[0][3], fill_mass)
            for c in range(3):
                fields[i, b, c] = pair[0][c] * scale
                fields[i, b, 3 + c] = pair[1][c]

    def turn(x, carry):
        at_cell = (x + shift_x) >> 2
        for b in range(n_y):
            at = pl.ds(8 * b, 8)
            mean = [fields[at_cell, b, c] for c in range(3)]
            n = [fields[at_cell, b, 3 + c] for c in range(3)]
            old = [out[c, x, at, :] for c in range(3)]
            rel = [old[c] - mean[c] for c in range(3)]
            along = (1.0 - cos_angle) * (n[0] * rel[0] + n[1] * rel[1] + n[2] * rel[2])
            cross = [
                n[1] * rel[2] - n[2] * rel[1],
                n[2] * rel[0] - n[0] * rel[2],
                n[0] * rel[1] - n[1] * rel[0],
            ]
            live = held[x, at, :] > odd
            for c in range(3):
                new = mean[c] + cos_angle * rel[c] + sin_angle * cross[c] + along * n[c]
                out[c, x, at, :] = jnp.where(live, new, old[c])
        return carry

    def idle_work(step):
        if step == 1:
            for c, part in enumerate(axes_of(numbers)):
                normals[c] = part

            def inner(i, carry):
                cell_fields(i, lambda b: i * n_y + b if b < n_y else n_x * n_y + 8 + i)
                return carry

            lax.fori_loop(0, n_x, inner, 0)
            cell_fields(n_x, lambda b: n_x * n_y + b if b < n_y else n_x * n_y + 16)
            lax.fori_loop(0, width_x // 2, turn, 0)
        if step == 2:
            lax.fori_loop(width_x // 2, width_x, turn, 0)

    speed = speed + push * kick
    place_now = place_now + timestep * speed
    src[1, OWN] = place_now * (1.0 / cutoff)
    sends = sends + exchange(1)
    own_columns(own, src[1, OWN])
    idle_work(1)
    early_forces(1)
    push = late_forces(1)

    speed = speed + push * kick
    place_now = place_now + timestep * speed
    def at_wide(a, b):
        return wide_slot(a, b, size_y)

    mine = at_wide(0, 0)
    wide[mine] = place_now * (1.0 / cutoff)
    spread = {}
    for a, b in around:
        k, target = (at_wide(a, b), at_wide(-a, -b))
        spread[a, b] = remote(
            wide.at[mine, pl.ds(0, 4)], wide.at[target, pl.ds(0, 4)],
            wide_send.at[k], wide_got.at[target], device(a, b),
        )
        spread[a, b].start()

    def wide_arrived(a):
        for b in (-1, 0, 1, -2, 2):
            if (isinstance(a, int) and b == 0) or folded(b, size_y) != b:
                continue
            k = at_wide(a, b)
            remote(
                wide.at[mine, pl.ds(0, 4)], wide.at[k, pl.ds(0, 4)],
                wide_send.at[k], wide_got.at[k], device(0, 1),
            ).wait_recv()

    idle_work(2)
    first[...] = src[0]
    second[...] = src[1]
    tiles[0] = place_now
    tiles[1] = speed
    tiles[2] = stacked([pos[c, 0] for c in range(3)])
    tiles[3] = stacked([vel[c, 0] for c in range(3)])
    tiles[4] = jnp.broadcast_to(jnp.where(alive, 1.0, 0.0), (8, slots))
    for k, a in enumerate(columns_x[:2]):
        wide_arrived(a)
        block = flipped([wide[at_wide(a, b)] for b in (-1, 0, 1)])
        for m in range(3):
            for c in range(3):
                column = block[:, 8 * m + c : 8 * m + c + 1]
                early[3 * k + m, c] = jnp.broadcast_to(column, (slots, slots))
        for m in range(3):
            around_m = [reader(wide, at_wide(a, m - 1 + q), a, q, steps) for q in (-1, 0, 1)]
            force_pass(early.at[m], begun.at[m], around_m, k == 0)
    wide_arrived(slow)
    for a in (-2 * quick, 2 * quick):
        wide_arrived(a)
    third[...] = wide[...]
    for copy in sends + halo + edges + list(spread.values()):
        copy.wait_send()


def finish_kernel(
    shape, turned, first, second, third, tiles, early, begun,
    out, pos_out, vel_out, own, force, later, sums, sem
):
    width_x, width_y, width_z = shape
    n_x, n_y = (width_x // SUB, width_y // SUB)
    slots = first.shape[2]
    size_y = lax.axis_size("yz")
    columns_x = sides(lax.axis_index("gx"))
    copies = []
    for c in range(3):
        copies.append(pltpu.make_async_copy(turned.at[c], out.at[c], sem.at[c]))
        copies[-1].start()

    steps = ((width_z // 2) / cutoff, n_x / cutoff, n_y / cutoff)
    block = 16 if slots % 16 == 0 else 8
    half = slots // 2
    group = [(k, b) for k in range(3) for b in (-1, 0, 1)]

    def at_wide(k, b, p=0):
        return wide_slot(columns_x[k] + p, b, size_y)

    def halves(most, work):
        work(0)
        pl.when(most * block > half)(lambda: work(half))

    def columns(tiles, most):
        sums[...] = flipped(tiles)

        def work(start):
            at = pl.ds(start, half)
            for n in range(len(tiles)):
                for c in range(3):
                    column = sums[at, 8 * n + c : 8 * n + c + 1]
                    own[n, c, at, :] = jnp.broadcast_to(column, (half, slots))

        halves(most, work)

    def pushes(m, columns_of, trips, sources, before=None):
        def body(r, carry):
            at = pl.ds(pl.multiple_of(r * block, block), block)
            rows = [columns_of[c, at, :] for c in range(3)]
            total = None if before is None else [before[c, at, :] for c in range(3)]
            for source in sources:
                parts = pair_sums(rows, source())
                total = parts if total is None else [t + p for t, p in zip(total, parts)]
            for c in range(3):
                force[m, c, at, :] = total[c]
            return carry

        lax.fori_loop(0, trips, body, 0)

    def rows_of(number, most):
        lane = iota((half, slots), 1)

        def work(start):
            at = pl.ds(start, half)
            block = jnp.zeros((half, slots), f32)
            for n in range(number):
                for c in range(3):
                    total = jnp.sum(force[n, c, at, :], axis=1, keepdims=True)
                    block = jnp.where(lane == 8 * n + c, total, block)
            sums[at, :] = block

        halves(most, work)
        return sums[...].T

    dead = [third[at_wide(k, b), pl.ds(0, 1), :] > 0.1 * far_away for k, b in group]
    trips = [
        (jnp.sum(jnp.where(gone, 0.0, 1.0)).astype(jnp.int32) + (block - 1)) // block for gone in dead
    ]
    most = functools.reduce(jnp.maximum, trips)
    columns([third[at_wide(2, b)] for b in (-1, 0, 1)], most)
    for m, (k, b) in enumerate(group):
        if k == 0:
            slow = columns_x[2]
            around_m = [reader(third, at_wide(2, b + q), slow, q, steps) for q in (-1, 0, 1)]
            pushes(m, early.at[m], trips[m], around_m, begun.at[m])
        else:
            around_m = [
                reader(third, at_wide(k, b + q, p), p, q, steps) for p in (-1, 0, 1) for q in (-1, 0, 1)
            ]
            pushes(m, early.at[m] if k == 1 else own.at[m - 6], trips[m], around_m)
    push = rows_of(len(group), most)
    speed, place = (tiles[1], tiles[0])
    for m, (k, b) in enumerate(group):
        near = slot_of(columns_x[k], b)
        now = third[at_wide(k, b)]
        mine = push[8 * m : 8 * m + 8]
        kick = jnp.broadcast_to(first[near, pl.ds(3, 1), :], (8, slots))
        if (k, b) == (0, 0):
            speed = speed + mine * kick
            place = place + timestep * speed
            moved = place * (1.0 / cutoff)
            own_kick, own_trips = (kick, trips[m])
        else:
            moved = now + (now - second[near]) + (timestep / cutoff) * (mine * kick)
        later[m] = jnp.where(jnp.broadcast_to(dead[m], (8, slots)), now, moved)
    columns([later[1]], own_trips)
    around_m = [reader(later, m, columns_x[k], b, steps) for m, (k, b) in enumerate(group)]
    pushes(0, own.at[0], own_trips, around_m)
    speed = speed + rows_of(1, own_trips)[:8] * own_kick
    place = place + timestep * speed
    alive = tiles[4] > 0
    place = jnp.where(alive, place, tiles[2])
    speed = jnp.where(alive, speed, tiles[3])
    for c in range(3):
        pos_out[c, 0] = place[c : c + 1]
        vel_out[c, 0] = speed[c : c + 1]
    for copy in copies:
        copy.wait()


def per_device(
    solvent_vel, occupancy, grid_shift, axis_index, colloid_pos, colloid_vel, colloid_mass, colloid_count
):
    shape = occupancy.shape
    width_x, width_y, width_z = shape
    rows = 2 * width_y
    n_x, n_y = (width_x // SUB, width_y // SUB)
    slots = colloid_mass.shape[2]
    solvent = solvent_vel.reshape(3, width_x, rows, width_z)
    smem = pl.BlockSpec(memory_space=pltpu.SMEM)
    vmem = pl.BlockSpec(memory_space=pltpu.VMEM)
    hbm = pl.BlockSpec(memory_space=pltpu.HBM)
    tall = (n_y + 2) // 2 * 8
    dma = pltpu.SemaphoreType.DMA

    def in_hbm(x):
        return pltpu.with_memory_space_constraint(x, pltpu.HBM)

    turned, *states = pl.pallas_call(
        functools.partial(collide_kernel, shape),
        out_shape=[
            pltpu.VMEM(solvent.shape, f32),
            pltpu.VMEM((9, 8, slots), f32),
            pltpu.VMEM((9, 8, slots), f32),
            pltpu.VMEM((25, 8, slots), f32),
            pltpu.VMEM((5, 8, slots), f32),
            pltpu.VMEM((6, 3, slots, slots), f32),
            pltpu.VMEM((3, 3, slots, slots), f32),
        ],
        in_specs=[hbm, smem] + [hbm] * 6,
        out_specs=[vmem] * 7,
        scratch_shapes=[
            pltpu.SMEM(grid_shift.shape, jnp.int32),
            pltpu.VMEM(colloid_pos.shape, f32),
            pltpu.VMEM(colloid_vel.shape, f32),
            pltpu.VMEM(colloid_mass.shape, f32),
            pltpu.VMEM(axis_index.shape, jnp.int32),
            pltpu.VMEM(shape, jnp.int32),
            pltpu.VMEM((width_x, rows, width_z), f32),
            pltpu.VMEM((n_x + 1, 4, rows, width_z), f32),
            pltpu.VMEM((n_x + 1, tall, width_z), f32),
            pltpu.VMEM((n_x + 1, tall, width_z), f32),
            pltpu.VMEM((n_x, n_y, width_z), f32),
            pltpu.VMEM((8, width_z), f32),
            pltpu.VMEM((8, width_z), f32),
            pltpu.VMEM((8, width_z), f32),
            pltpu.VMEM((3, n_x * n_y + 24, width_z), f32),
            pltpu.VMEM((n_x + 1, n_y, 6, 8, width_z), f32),
            pltpu.VMEM((2, tall, width_z), f32),
            pltpu.VMEM((2, n_x + 1, 8, width_z), f32),
            pltpu.VMEM((4, 8, width_z), f32),
            pltpu.VMEM((2, 9, 8, slots), f32),
            pltpu.VMEM((25, 8, slots), f32),
            pltpu.VMEM((3, slots, slots), f32),
            pltpu.VMEM((3, slots, slots), f32),
            dma((6,)),
            dma((n_x,)),
            dma((8,)),
            dma((8,)),
            dma((3,)),
            dma((3,)),
            dma((2, 9)),
            dma((2, 9)),
            dma((25,)),
            dma((25,)),
        ],
        compiler_params=pltpu.CompilerParams(
            collective_id=0, has_side_effects=True, vmem_limit_bytes=32 * 2**20
        ),
        name="collide",
    )(
        in_hbm(grid_shift), colloid_count, in_hbm(solvent), in_hbm(occupancy), in_hbm(axis_index),
        in_hbm(colloid_pos), in_hbm(colloid_vel), in_hbm(colloid_mass),
    )

    solvent_out, pos_out, vel_out = pl.pallas_call(
        functools.partial(finish_kernel, shape),
        out_shape=[
            jax.ShapeDtypeStruct(solvent.shape, f32),
            jax.ShapeDtypeStruct(colloid_pos.shape, f32),
            jax.ShapeDtypeStruct(colloid_vel.shape, f32),
        ],
        in_specs=[vmem] * 7,
        out_specs=[hbm, vmem, vmem],
        scratch_shapes=[
            pltpu.VMEM((3, 3, slots, slots), f32),
            pltpu.VMEM((9, 3, slots, slots), f32),
            pltpu.VMEM((9, 8, slots), f32),
            pltpu.VMEM((slots, slots), f32),
            dma((3,)),
        ],
        compiler_params=pltpu.CompilerParams(vmem_limit_bytes=16 * 2**20),
        name="finish",
    )(turned, *states)
    return (solvent_out.reshape(solvent_vel.shape), pos_out, vel_out)


def solution(mesh):
    return jax.shard_map(
        per_device,
        mesh=mesh,
        in_specs=(
            P(None, "gx", "yz", None, None),
            P("gx", "yz", None),
            P(),
            P("gx", "yz", None),
            P(None, "gx", "yz", None),
            P(None, "gx", "yz", None),
            P("gx", "yz", None),
            P("gx", "yz"),
        ),
        out_specs=(
            P(None, "gx", "yz", None, None),
            P(None, "gx", "yz", None),
            P(None, "gx", "yz", None),
        ),
        check_vma=False,
    )
```

```python
import functools
import math

import jax
import jax.numpy as jnp
from jax import lax
from jax.experimental import pallas as pl
from jax.experimental.pallas import tpu as pltpu
from jax.sharding import PartitionSpec as P

SUB = 4
SUBSTEPS = 4
DIRECTIONS = 64

turn_angle = 130.0 * math.pi / 180.0
cos_angle = math.cos(turn_angle)
sin_angle = math.sin(turn_angle)
golden = math.pi * (3.0 - math.sqrt(5.0))
cutoff = 1.5
stiffness = 20.0
timestep = 0.05
fill_mass = 16.0
far_away = 1.0e9
MESH = pl.DeviceIdType.MESH
f32 = jnp.float32
bf16 = jnp.bfloat16
RING = [(a, b) for a in (-1, 0, 1) for b in (-1, 0, 1)]
AROUND = [pair for pair in RING if pair != (0, 0)]
OWN = 4


def iota(shape, dim):
    return lax.broadcasted_iota(jnp.int32, shape, dim)


def slot_of(a, b):
    return (a + 1) * 3 + b + 1


def folded(b, size_y):
    return 2 if b == -2 and size_y == 4 else b


def wide_slot(a, b, size_y):
    return (a + 2) * 5 + folded(b, size_y) + 2


def wide_pairs(size_y):
    return [
        (a, b) for a in (-1, 1, -2, 2, 0) for b in (-1, 0, 1, -2, 2)
        if (a, b) != (0, 0) and folded(b, size_y) == b
    ]


def sides(me_x):
    quick = 1 - 2 * (me_x & 1)
    return (0, quick, -quick)


def reader(ref, slot, p, q, steps):
    period, step_x, step_y = steps

    def read():
        x, y, z = [ref[slot, pl.ds(c, 1), :] for c in range(3)]
        if not isinstance(p, int):
            x = x + p.astype(f32) * step_x
        elif p != 0:
            x = x + p * step_x
        return (x, y if q == 0 else y + q * step_y, z, period)

    return read


def terms(value, number):
    out = []
    for _ in range(number - 1):
        part = value.astype(bf16)
        out.append(part)
        value = value - part.astype(f32)
    return out + [value.astype(bf16)]


def dot(left, right, contract=((1,), (0,))):
    return lax.dot_general(left, right, (contract, ((), ())), preferred_element_type=f32)


def wrapped(value, size):
    return jnp.where(value >= size, value - size, value)


def layer_of(row, scale, width):
    return jnp.clip(jnp.floor(row * scale).astype(jnp.int32), 0, width - 1)


def fold(values):
    row = iota(values[0].shape, 0)
    low = row < 4
    values = [
        jnp.where(low, a, b) + pltpu.roll(jnp.where(low, b, a), 4, 0)
        for a, b in zip(values[:4], values[4:])
    ]
    for dist in (2, 1):
        low = (row & dist) == 0
        values = [
            jnp.where(low, a, b) + jnp.where(low, pltpu.roll(a, 8 - dist, 0), pltpu.roll(b, dist, 0))
            for a, b in zip(values[:dist], values[dist:])
        ]
    return values[0]


def stacked(rows):
    comp = iota((8, rows[0].shape[1]), 0)
    out = jnp.zeros((8, rows[0].shape[1]), f32)
    for c, row in enumerate(rows):
        out = jnp.where(comp == c, row, out)
    return out


def axes_of(number):
    height = 1.0 - (2.0 * number + 1.0) / DIRECTIONS
    radius = jnp.sqrt(1.0 - height * height)
    phase = number * golden
    return [radius * jnp.cos(phase), radius * jnp.sin(phase), height]


def pair_sums(own_rows, source):
    dx, dy, dz = [o - s for o, s in zip(own_rows, source[:3])]
    period = source[3]
    half = 0.5 * period
    dz = dz + jnp.where(dz > half, -period, jnp.where(dz < -half, period, 0.0))
    reach = jnp.maximum(1.0 - (dx * dx + dy * dy + dz * dz), 0.0)
    weight = reach * reach
    return [weight * dx, weight * dy, weight * dz]


def force_pass(own, force, sources, first):
    slots = own.shape[-1]
    wide = 32 if slots % 32 == 0 else 8

    def block(r, carry):
        at = pl.ds(pl.multiple_of(r * wide, wide), wide)
        rows = [own[c, at, :] for c in range(3)]
        total = None if first else [force[c, at, :] for c in range(3)]
        for source in sources:
            parts = pair_sums(rows, source())
            total = parts if total is None else [t + p for t, p in zip(total, parts)]
        for c in range(3):
            force[c, at, :] = total[c]
        return carry

    lax.fori_loop(0, slots // wide, block, 0)


def force_rows(force):
    slots = force.shape[1]
    comp = iota((8, slots), 0)
    out = None
    for c in range(3):
        pick = (comp == c).astype(f32).astype(bf16)
        for term in terms(force[c], 2)[::-1]:
            part = dot(pick, term, ((1,), (1,)))
            out = part if out is None else out + part
    return out


def flipped(tiles):
    slots = tiles[0].shape[1]
    pad = jnp.zeros((slots - 8 * len(tiles), slots), f32)
    return jnp.concatenate(tiles + [pad], axis=0).T


def own_columns(own, tile):
    slots = tile.shape[1]
    block = flipped([tile])
    for c in range(3):
        own[c] = jnp.broadcast_to(block[:, c : c + 1], (slots, slots))


def collide_kernel(
    shape, shift_hbm, count, solvent_hbm, occupancy_hbm, axis_hbm, pos_hbm, vel_hbm, mass_hbm,
    out, first, second, third, tiles, early, begun,
    shift, pos, vel, mass, axis, occupancy, held, cell, sums, total, index, edge_x, edge_y, edge_c,
    normals, fields, halo_x, halo_y, halo_c, src, wide, force, own,
    small_sem, chunk_sem, halo_send, halo_got, edge_send, edge_got, src_send, src_got,
    wide_send, wide_got,
):
    width_x, width_y, width_z = shape
    n_x, n_y = (width_x // SUB, width_y // SUB)
    rows = 2 * width_y
    slots = mass.shape[2]
    me_x, me_y = (lax.axis_index("gx"), lax.axis_index("yz"))
    size_x, size_y = (lax.axis_size("gx"), lax.axis_size("yz"))

    def device(a, b):
        return (lax.rem(me_x + a + size_x, size_x), lax.rem(me_y + b + size_y, size_y))

    def remote(source, target, send, receive, where):
        return pltpu.make_async_remote_copy(
            src_ref=source, dst_ref=target, send_sem=send, recv_sem=receive,
            device_id=where, device_id_type=MESH,
        )

    around = wide_pairs(size_y)
    edge_c[...] = jnp.zeros_like(edge_c)
    small = [
        pltpu.make_async_copy(source, target, small_sem.at[k])
        for k, (source, target) in enumerate(
            [
                (shift_hbm, shift), (pos_hbm, pos), (vel_hbm, vel),
                (mass_hbm, mass), (axis_hbm, axis), (occupancy_hbm, occupancy),
            ]
        )
    ]
    chunks = [
        pltpu.make_async_copy(
            solvent_hbm.at[:, pl.ds(i * SUB, SUB)], out.at[:, pl.ds(i * SUB, SUB)], chunk_sem.at[i]
        )
        for i in range(n_x)
    ]
    barrier = pltpu.get_barrier_semaphore()

    def greet(pairs):
        for a, b in pairs:
            pl.semaphore_signal(barrier, inc=1, device_id=device(a, b), device_id_type=MESH)

    for copy in small:
        copy.start()
    greet(around[:6])
    for copy in chunks:
        copy.start()
    greet(around[6:])
    for copy in small[:-1]:
        copy.wait()
    shift_x, shift_y, shift_z = (shift[0], shift[1], shift[2])

    alive = iota((1, slots), 1) < count[0, 0]
    cell_x = (layer_of(pos[0, 0], SUB, width_x) + shift_x) >> 2
    cell_y = (layer_of(pos[1, 0], SUB, width_y) + shift_y) >> 2
    layer_z = layer_of(pos[2, 0], 2.0, width_z)
    cell_z = wrapped(layer_z + shift_z, width_z) >> 1
    place = cell_x * (n_y + 1) + cell_y
    weight = jnp.where(alive, mass[0], 0.0)
    comp = iota((8, slots), 0)
    four = comp & 3
    values = jnp.where(
        four == 0, vel[0, 0] * weight,
        jnp.where(four == 1, vel[1, 0] * weight, jnp.where(four == 2, vel[2, 0] * weight, weight)),
    )
    place_half = place - (comp >> 2)
    place_last = jnp.where(comp < 4, place, -1)
    tiles_y = (n_y + 2) // 2

    def in_tile(i, t):
        return (place_half if 2 * t < n_y else place_last) == i * (n_y + 1) + 2 * t

    spread = [
        jnp.where(in_tile(i, t), values, 0.0) for i in range(n_x + 1) for t in range(tiles_y)
    ]
    near = (wrapped(iota((width_z, slots), 0) + shift_z, width_z) >> 1) == cell_z
    near = near.astype(f32).astype(bf16)
    deposit = sum(
        dot(term, near, ((1,), (1,))) for term in terms(jnp.concatenate(spread, axis=0), 3)[::-1]
    )
    sums[...] = deposit.reshape(n_x + 1, tiles_y * 8, width_z)

    cell_row = wrapped(iota((width_z // 2, width_z), 1) + shift_z, width_z) >> 1
    expand = (cell_row == iota((width_z // 2, width_z), 0)).astype(f32).astype(bf16)
    number = axis[...].reshape(n_x * n_y, width_z // 2).astype(f32).astype(bf16)
    index[...] = dot(number, expand).reshape(n_x, n_y, width_z)

    start = stacked([jnp.where(alive, pos[0, 0], far_away), pos[1, 0], pos[2, 0]])
    kick = jnp.broadcast_to((timestep * stiffness * cutoff) / mass[0], (8, slots))
    src[0, OWN] = jnp.where(comp == 3, kick, start * (1.0 / cutoff))

    double = (iota((SUB * rows, SUB * width_y), 0) >> 1 == iota((SUB * rows, SUB * width_y), 1)).astype(bf16)
    small[-1].wait()
    for i in range(n_x):
        at = pl.ds(i * SUB, SUB)
        filled = occupancy[at].reshape(SUB * width_y, width_z).astype(f32).astype(bf16)
        held[at] = dot(double, filled).reshape(SUB, rows, width_z)
    row = iota((8, width_z), 0)
    odd = (row & 1).astype(f32)
    stays_1 = jnp.broadcast_to(shift_x, (8, width_z)) <= 2
    stays_2 = jnp.broadcast_to(shift_x, (8, width_z)) <= 1
    later = ((row >> 1) + shift_y) >= SUB
    even = ((iota((8, width_z), 1) + shift_z) & 1) == 0
    halves = jnp.where((row & 3) == 3, 0.5, 1.0)
    blank = jnp.zeros((8, width_z), f32)

    def finish(i):
        def straddling(c, j):
            now = cell[i, c, pl.ds(8 * j, 8), :] if j < n_y else blank
            before = cell[i, c, pl.ds(8 * (j - 1), 8), :] if j > 0 else blank
            return jnp.where(later, before, now)

        for t in range(tiles_y):
            blocks = [
                straddling(q & 3, 2 * t + (q >> 2)) if 2 * t + (q >> 2) <= n_y else blank
                for q in range(8)
            ]
            tile = fold(blocks) * halves
            partner = jnp.where(even, pltpu.roll(tile, width_z - 1, 1), pltpu.roll(tile, 1, 1))
            sums[i, pl.ds(8 * t, 8), :] += tile + partner

    def gather(i):
        for b in range(n_y):
            at = pl.ds(8 * b, 8)
            filled = [held[i * SUB + r, at, :] for r in range(SUB)]
            live = [f > odd for f in filled]
            for c in range(4):
                v = filled
                if c < 3:
                    v = [jnp.where(live[r], out[c, i * SUB + r, at, :], 0.0) for r in range(SUB)]
                front = v[0] + v[1]
                back = v[3] + v[2]
                stay = jnp.where(stays_1, jnp.where(stays_2, front + v[2], front), v[0])
                move = jnp.where(stays_1, jnp.where(stays_2, v[3], back), back + v[1])
                cell[i, c, at, :] = stay if i == 0 else cell[i, c, at, :] + stay
                cell[i + 1, c, at, :] = move

    for i in range(n_x):
        chunks[i].wait()
        gather(i)
        if i > 0:
            finish(i - 1)
    finish(n_x - 1)
    finish(n_x)

    pl.semaphore_wait(barrier, len(around))

    def exchange(step):
        mine = src.at[step, OWN, pl.ds(0, 4)]
        copies = {}
        for a, b in AROUND:
            k = slot_of(a, b)
            copies[k] = remote(
                mine, src.at[step, 8 - k, pl.ds(0, 4)],
                src_send.at[step, k], src_got.at[step, 8 - k], device(a, b),
            )
            copies[k].start()
        return list(copies.values())

    sends = exchange(0)

    at_low, at_high = (pl.ds(0, 4), pl.ds(n_y * SUB, 4))
    every = pl.ds(0, n_x + 1)
    halo = [
        (sums.at[n_x], halo_x.at[0], (1, 0)),
        (sums.at[0], halo_x.at[1], (-1, 0)),
        (sums.at[every, at_high], halo_y.at[0, every, at_low], (0, 1)),
        (sums.at[every, at_low], halo_y.at[1, every, at_low], (0, -1)),
        (sums.at[n_x, at_high], halo_c.at[0, at_low], (1, 1)),
        (sums.at[n_x, at_low], halo_c.at[1, at_low], (1, -1)),
        (sums.at[0, at_high], halo_c.at[2, at_low], (-1, 1)),
        (sums.at[0, at_low], halo_c.at[3, at_low], (-1, -1)),
    ]
    halo = [
        remote(source, target, halo_send.at[k], halo_got.at[k], device(*where))
        for k, (source, target, where) in enumerate(halo)
    ]
    for copy in halo:
        copy.start()
    edges = [
        (index.at[0], edge_x, (-1, 0)),
        (index.at[pl.ds(0, n_x), 0], edge_y, (0, -1)),
        (index.at[0, pl.ds(0, 1)], edge_c.at[pl.ds(0, 1)], (-1, -1)),
    ]
    edges = [
        remote(source, target, edge_send.at[k], edge_got.at[k], device(*where))
        for k, (source, target, where) in enumerate(edges)
    ]
    for copy in edges:
        copy.start()

    steps = ((width_z // 2) / cutoff, n_x / cutoff, n_y / cutoff)
    columns_x = sides(me_x)
    quick, slow = columns_x[1:]

    def source(step, a, b):
        return reader(src.at[step], slot_of(a, b), a, b, steps)

    def arrived(step, a, b):
        slot = slot_of(a, b)
        remote(
            src.at[step, OWN, pl.ds(0, 4)], src.at[step, slot, pl.ds(0, 4)],
            src_send.at[step, slot], src_got.at[step, slot], device(0, 1),
        ).wait_recv()

    def early_forces(step):
        for b in (-1, 1):
            arrived(step, 0, b)
        force_pass(own, force, [source(step, 0, b) for b in (0, -1, 1)], True)
        for b in (-1, 0, 1):
            arrived(step, quick, b)
        force_pass(own, force, [source(step, quick, b) for b in (-1, 0, 1)], False)

    def late_arrivals(step):
        for b in (-1, 0, 1):
            arrived(step, slow, b)

    def late_forces(step):
        late_arrivals(step)
        force_pass(own, force, [source(step, slow, b) for b in (-1, 0, 1)], False)
        return force_rows(force)

    own_columns(own, src[0, OWN])
    early_forces(0)
    push = late_forces(0)

    for copy in halo:
        copy.wait_recv()
    total[...] = sums[...]
    total[0] += halo_x[0]
    total[n_x] += halo_x[1]
    for i in range(n_x + 1):
        total[i, at_low, :] += halo_y[0, i, at_low, :]
        total[i, at_high, :] += halo_y[1, i, at_low, :]
    total[0, at_low, :] += halo_c[0, at_low, :]
    total[0, at_high, :] += halo_c[1, at_low, :]
    total[n_x, at_low, :] += halo_c[2, at_low, :]
    total[n_x, at_high, :] += halo_c[3, at_low, :]
    for copy in edges:
        copy.wait_recv()

    chosen = (iota((width_z, slots), 0) == layer_z).astype(f32).astype(bf16)
    block = total[...].reshape((n_x + 1) * tiles_y * 8, width_z)
    at_z = sum(dot(term, chosen) for term in terms(block, 2)[::-1])
    picked = jnp.zeros((8, slots), f32)
    for i in range(n_x + 1):
        for t in range(tiles_y):
            n = 8 * (i * tiles_y + t)
            picked = picked + jnp.where(in_tile(i, t), at_z[n : n + 8], 0.0)
    picked = picked + pltpu.roll(picked, 4, 0)
    numbers = jnp.concatenate(
        [index[...].reshape(n_x * n_y, width_z), edge_x[...], edge_y[...], edge_c[...]], axis=0
    )
    at_z = dot(numbers.astype(bf16), chosen)
    wanted = [place - comp == i * (n_y + 1) for i in range(n_x + 1)]
    wanted.append(place - comp * (n_y + 1) == n_y)
    wanted.append(jnp.logical_and(comp == 0, place == n_x * (n_y + 1) + n_y))
    found = jnp.zeros((8, slots), f32)
    for n, mask in enumerate(wanted):
        found = found + jnp.where(mask, at_z[8 * n : 8 * n + 8], 0.0)
    found = jnp.sum(found, axis=0, keepdims=True)
    heavy = jnp.maximum(picked[3:4], fill_mass)
    mean = [picked[c : c + 1] / heavy for c in range(3)]
    n = axes_of(found)
    rel = [vel[c, 0] - mean[c] for c in range(3)]
    cross = [n[1] * rel[2] - n[2] * rel[1], n[2] * rel[0] - n[0] * rel[2], n[0] * rel[1] - n[1] * rel[0]]
    along = n[0] * rel[0] + n[1] * rel[1] + n[2] * rel[2]
    speed = stacked([
        mean[c] + cos_angle * rel[c] + sin_angle * cross[c] + (1.0 - cos_angle) * along * n[c]
        for c in range(3)
    ])
    place_now = start

    def cell_fields(i, rows_of):
        for b in range(n_y):
            pair = [
                [jnp.where(later, total[i, pl.ds(4 * (b + 1) + c, 1), :], total[i, pl.ds(4 * b + c, 1), :])
                 for c in range(4)],
                [jnp.where(later, normals[c, pl.ds(rows_of(b + 1), 1), :], normals[c, pl.ds(rows_of(b), 1), :])
                 for c in range(3)],
            ]
            scale = 1.0 / jnp.maximum(pair[0][3], fill_mass)
            for c in range(3):
                fields[i, b, c] = pair[0][c] * scale
                fields[i, b, 3 + c] = pair[1][c]

    def turn(x, carry):
        at_cell = (x + shift_x) >> 2
        for b in range(n_y):
            at = pl.ds(8 * b, 8)
            mean = [fields[at_cell, b, c] for c in range(3)]
            n = [fields[at_cell, b, 3 + c] for c in range(3)]
            old = [out[c, x, at, :] for c in range(3)]
            rel = [old[c] - mean[c] for c in range(3)]
            along = (1.0 - cos_angle) * (n[0] * rel[0] + n[1] * rel[1] + n[2] * rel[2])
            cross = [
                n[1] * rel[2] - n[2] * rel[1],
                n[2] * rel[0] - n[0] * rel[2],
                n[0] * rel[1] - n[1] * rel[0],
            ]
            live = held[x, at, :] > odd
            for c in range(3):
                new = mean[c] + cos_angle * rel[c] + sin_angle * cross[c] + along * n[c]
                out[c, x, at, :] = jnp.where(live, new, old[c])
        return carry

    def idle_work(step):
        if step == 1:
            for c, part in enumerate(axes_of(numbers)):
                normals[c] = part

            def inner(i, carry):
                cell_fields(i, lambda b: i * n_y + b if b < n_y else n_x * n_y + 8 + i)
                return carry

            lax.fori_loop(0, n_x, inner, 0)
            cell_fields(n_x, lambda b: n_x * n_y + b if b < n_y else n_x * n_y + 16)
            lax.fori_loop(0, width_x // 2, turn, 0)
        if step == 2:
            lax.fori_loop(width_x // 2, width_x, turn, 0)

    speed = speed + push * kick
    place_now = place_now + timestep * speed
    src[1, OWN] = place_now * (1.0 / cutoff)
    sends = sends + exchange(1)
    own_columns(own, src[1, OWN])
    idle_work(1)
    early_forces(1)
    push = late_forces(1)

    speed = speed + push * kick
    place_now = place_now + timestep * speed
    def at_wide(a, b):
        return wide_slot(a, b, size_y)

    mine = at_wide(0, 0)
    wide[mine] = place_now * (1.0 / cutoff)
    spread = {}
    for a, b in around:
        k, target = (at_wide(a, b), at_wide(-a, -b))
        spread[a, b] = remote(
            wide.at[mine, pl.ds(0, 4)], wide.at[target, pl.ds(0, 4)],
            wide_send.at[k], wide_got.at[target], device(a, b),
        )
        spread[a, b].start()

    def wide_arrived(a):
        for b in (-1, 0, 1, -2, 2):
            if (isinstance(a, int) and b == 0) or folded(b, size_y) != b:
                continue
            k = at_wide(a, b)
            remote(
                wide.at[mine, pl.ds(0, 4)], wide.at[k, pl.ds(0, 4)],
                wide_send.at[k], wide_got.at[k], device(0, 1),
            ).wait_recv()

    idle_work(2)
    first[...] = src[0]
    second[...] = src[1]
    tiles[0] = place_now
    tiles[1] = speed
    tiles[2] = stacked([pos[c, 0] for c in range(3)])
    tiles[3] = stacked([vel[c, 0] for c in range(3)])
    tiles[4] = jnp.broadcast_to(jnp.where(alive, 1.0, 0.0), (8, slots))
    for k, a in enumerate(columns_x[:2]):
        wide_arrived(a)
        block = flipped([wide[at_wide(a, b)] for b in (-1, 0, 1)])
        for m in range(3):
            for c in range(3):
                column = block[:, 8 * m + c : 8 * m + c + 1]
                early[3 * k + m, c] = jnp.broadcast_to(column, (slots, slots))
        for m in range(3):
            around_m = [reader(wide, at_wide(a, m - 1 + q), a, q, steps) for q in (-1, 0, 1)]
            force_pass(early.at[m], begun.at[m], around_m, k == 0)
    wide_arrived(slow)
    for a in (-2 * quick, 2 * quick):
        wide_arrived(a)
    third[...] = wide[...]
    for copy in sends + halo + edges + list(spread.values()):
        copy.wait_send()


def finish_kernel(
    shape, turned, first, second, third, tiles, early, begun,
    out, pos_out, vel_out, own, force, later, sums, sem
):
    width_x, width_y, width_z = shape
    n_x, n_y = (width_x // SUB, width_y // SUB)
    slots = first.shape[2]
    size_y = lax.axis_size("yz")
    columns_x = sides(lax.axis_index("gx"))
    copies = []
    for c in range(3):
        copies.append(pltpu.make_async_copy(turned.at[c], out.at[c], sem.at[c]))
        copies[-1].start()

    steps = ((width_z // 2) / cutoff, n_x / cutoff, n_y / cutoff)
    block = 16 if slots % 16 == 0 else 8
    half = slots // 2
    group = [(k, b) for k in range(3) for b in (-1, 0, 1)]

    def at_wide(k, b, p=0):
        return wide_slot(columns_x[k] + p, b, size_y)

    def halves(most, work):
        work(0)
        pl.when(most * block > half)(lambda: work(half))

    def columns(tiles, most):
        sums[...] = flipped(tiles)

        def work(start):
            at = pl.ds(start, half)
            for n in range(len(tiles)):
                for c in range(3):
                    column = sums[at, 8 * n + c : 8 * n + c + 1]
                    own[n, c, at, :] = jnp.broadcast_to(column, (half, slots))

        halves(most, work)

    def pushes(m, columns_of, trips, sources, before=None):
        def body(r, carry):
            at = pl.ds(pl.multiple_of(r * block, block), block)
            rows = [columns_of[c, at, :] for c in range(3)]
            total = None if before is None else [before[c, at, :] for c in range(3)]
            for source in sources:
                parts = pair_sums(rows, source())
                total = parts if total is None else [t + p for t, p in zip(total, parts)]
            for c in range(3):
                force[m, c, at, :] = total[c]
            return carry

        lax.fori_loop(0, trips, body, 0)

    def rows_of(number, most):
        lane = iota((half, slots), 1)

        def work(start):
            at = pl.ds(start, half)
            block = jnp.zeros((half, slots), f32)
            for n in range(number):
                for c in range(3):
                    total = jnp.sum(force[n, c, at, :], axis=1, keepdims=True)
                    block = jnp.where(lane == 8 * n + c, total, block)
            sums[at, :] = block

        halves(most, work)
        return sums[...].T

    dead = [third[at_wide(k, b), pl.ds(0, 1), :] > 0.1 * far_away for k, b in group]
    trips = [
        (jnp.sum(jnp.where(gone, 0.0, 1.0)).astype(jnp.int32) + (block - 1)) // block for gone in dead
    ]
    most = functools.reduce(jnp.maximum, trips)
    columns([third[at_wide(2, b)] for b in (-1, 0, 1)], most)
    for m, (k, b) in enumerate(group):
        if k == 0:
            slow = columns_x[2]
            around_m = [reader(third, at_wide(2, b + q), slow, q, steps) for q in (-1, 0, 1)]
            pushes(m, early.at[m], trips[m], around_m, begun.at[m])
        else:
            around_m = [
                reader(third, at_wide(k, b + q, p), p, q, steps) for p in (-1, 0, 1) for q in (-1, 0, 1)
            ]
            pushes(m, early.at[m] if k == 1 else own.at[m - 6], trips[m], around_m)
    push = rows_of(len(group), most)
    speed, place = (tiles[1], tiles[0])
    for m, (k, b) in enumerate(group):
        near = slot_of(columns_x[k], b)
        now = third[at_wide(k, b)]
        mine = push[8 * m : 8 * m + 8]
        kick = jnp.broadcast_to(first[near, pl.ds(3, 1), :], (8, slots))
        if (k, b) == (0, 0):
            speed = speed + mine * kick
            place = place + timestep * speed
            moved = place * (1.0 / cutoff)
            own_kick, own_trips = (kick, trips[m])
        else:
            moved = now + (now - second[near]) + (timestep / cutoff) * (mine * kick)
        later[m] = jnp.where(jnp.broadcast_to(dead[m], (8, slots)), now, moved)
    columns([later[1]], own_trips)
    around_m = [reader(later, m, columns_x[k], b, steps) for m, (k, b) in enumerate(group)]
    pushes(0, own.at[0], own_trips, around_m)
    speed = speed + rows_of(1, own_trips)[:8] * own_kick
    place = place + timestep * speed
    alive = tiles[4] > 0
    place = jnp.where(alive, place, tiles[2])
    speed = jnp.where(alive, speed, tiles[3])
    for c in range(3):
        pos_out[c, 0] = place[c : c + 1]
        vel_out[c, 0] = speed[c : c + 1]
    for copy in copies:
        copy.wait()


def per_device(
    solvent_vel, occupancy, grid_shift, axis_index, colloid_pos, colloid_vel, colloid_mass, colloid_count
):
    shape = occupancy.shape
    width_x, width_y, width_z = shape
    rows = 2 * width_y
    n_x, n_y = (width_x // SUB, width_y // SUB)
    slots = colloid_mass.shape[2]
    solvent = solvent_vel.reshape(3, width_x, rows, width_z)
    smem = pl.BlockSpec(memory_space=pltpu.SMEM)
    vmem = pl.BlockSpec(memory_space=pltpu.VMEM)
    hbm = pl.BlockSpec(memory_space=pltpu.HBM)
    tall = (n_y + 2) // 2 * 8
    dma = pltpu.SemaphoreType.DMA

    def in_hbm(x):
        return pltpu.with_memory_space_constraint(x, pltpu.HBM)

    turned, *states = pl.pallas_call(
        functools.partial(collide_kernel, shape),
        out_shape=[
            pltpu.VMEM(solvent.shape, f32),
            pltpu.VMEM((9, 8, slots), f32),
            pltpu.VMEM((9, 8, slots), f32),
            pltpu.VMEM((25, 8, slots), f32),
            pltpu.VMEM((5, 8, slots), f32),
            pltpu.VMEM((6, 3, slots, slots), f32),
            pltpu.VMEM((3, 3, slots, slots), f32),
        ],
        in_specs=[hbm, smem] + [hbm] * 6,
        out_specs=[vmem] * 7,
        scratch_shapes=[
            pltpu.SMEM(grid_shift.shape, jnp.int32),
            pltpu.VMEM(colloid_pos.shape, f32),
            pltpu.VMEM(colloid_vel.shape, f32),
            pltpu.VMEM(colloid_mass.shape, f32),
            pltpu.VMEM(axis_index.shape, jnp.int32),
            pltpu.VMEM(shape, jnp.int32),
            pltpu.VMEM((width_x, rows, width_z), f32),
            pltpu.VMEM((n_x + 1, 4, rows, width_z), f32),
            pltpu.VMEM((n_x + 1, tall, width_z), f32),
            pltpu.VMEM((n_x + 1, tall, width_z), f32),
            pltpu.VMEM((n_x, n_y, width_z), f32),
            pltpu.VMEM((8, width_z), f32),
            pltpu.VMEM((8, width_z), f32),
            pltpu.VMEM((8, width_z), f32),
            pltpu.VMEM((3, n_x * n_y + 24, width_z), f32),
            pltpu.VMEM((n_x + 1, n_y, 6, 8, width_z), f32),
            pltpu.VMEM((2, tall, width_z), f32),
            pltpu.VMEM((2, n_x + 1, 8, width_z), f32),
            pltpu.VMEM((4, 8, width_z), f32),
            pltpu.VMEM((2, 9, 8, slots), f32),
            pltpu.VMEM((25, 8, slots), f32),
            pltpu.VMEM((3, slots, slots), f32),
            pltpu.VMEM((3, slots, slots), f32),
            dma((6,)),
            dma((n_x,)),
            dma((8,)),
            dma((8,)),
            dma((3,)),
            dma((3,)),
            dma((2, 9)),
            dma((2, 9)),
            dma((25,)),
            dma((25,)),
        ],
        compiler_params=pltpu.CompilerParams(
            collective_id=0, has_side_effects=True, vmem_limit_bytes=32 * 2**20
        ),
        name="collide",
    )(
        in_hbm(grid_shift), colloid_count, in_hbm(solvent), in_hbm(occupancy), in_hbm(axis_index),
        in_hbm(colloid_pos), in_hbm(colloid_vel), in_hbm(colloid_mass),
    )

    solvent_out, pos_out, vel_out = pl.pallas_call(
        functools.partial(finish_kernel, shape),
        out_shape=[
            jax.ShapeDtypeStruct(solvent.shape, f32),
            jax.ShapeDtypeStruct(colloid_pos.shape, f32),
            jax.ShapeDtypeStruct(colloid_vel.shape, f32),
        ],
        in_specs=[vmem] * 7,
        out_specs=[hbm, vmem, vmem],
        scratch_shapes=[
            pltpu.VMEM((3, 3, slots, slots), f32),
            pltpu.VMEM((9, 3, slots, slots), f32),
            pltpu.VMEM((9, 8, slots), f32),
            pltpu.VMEM((slots, slots), f32),
            dma((3,)),
        ],
        compiler_params=pltpu.CompilerParams(vmem_limit_bytes=16 * 2**20),
        name="finish",
    )(turned, *states)
    return (solvent_out.reshape(solvent_vel.shape), pos_out, vel_out)


def solution(mesh):
    return jax.shard_map(
        per_device,
        mesh=mesh,
        in_specs=(
            P(None, "gx", "yz", None, None),
            P("gx", "yz", None),
            P(),
            P("gx", "yz", None),
            P(None, "gx", "yz", None),
            P(None, "gx", "yz", None),
            P("gx", "yz", None),
            P("gx", "yz"),
        ),
        out_specs=(
            P(None, "gx", "yz", None, None),
            P(None, "gx", "yz", None),
            P(None, "gx", "yz", None),
        ),
        check_vma=False,
    )
```

```python
import functools
import math

import jax
import jax.numpy as jnp
from jax import lax
from jax.experimental import pallas as pl
from jax.experimental.pallas import tpu as pltpu
from jax.sharding import PartitionSpec as P

SUB = 4
SUBSTEPS = 4
DIRECTIONS = 64

turn_angle = 130.0 * math.pi / 180.0
cos_angle = math.cos(turn_angle)
sin_angle = math.sin(turn_angle)
golden = math.pi * (3.0 - math.sqrt(5.0))
cutoff = 1.5
stiffness = 20.0
timestep = 0.05
fill_mass = 16.0
far_away = 1.0e9
MESH = pl.DeviceIdType.MESH
f32 = jnp.float32
bf16 = jnp.bfloat16
RING = [(a, b) for a in (-1, 0, 1) for b in (-1, 0, 1)]
AROUND = [pair for pair in RING if pair != (0, 0)]
OWN = 4


def iota(shape, dim):
    return lax.broadcasted_iota(jnp.int32, shape, dim)


def slot_of(a, b):
    return (a + 1) * 3 + b + 1


def folded(b, size_y):
    return 2 if b == -2 and size_y == 4 else b


def wide_slot(a, b, size_y):
    return (a + 2) * 5 + folded(b, size_y) + 2


def wide_pairs(size_y):
    return [
        (a, b) for a in (-1, 1, -2, 2, 0) for b in (-1, 0, 1, -2, 2)
        if (a, b) != (0, 0) and folded(b, size_y) == b
    ]


def sides(me_x):
    quick = 1 - 2 * (me_x & 1)
    return (0, quick, -quick)


def reader(ref, slot, p, q, steps):
    period, step_x, step_y = steps

    def read():
        x, y, z = [ref[slot, pl.ds(c, 1), :] for c in range(3)]
        if not isinstance(p, int):
            x = x + p.astype(f32) * step_x
        elif p != 0:
            x = x + p * step_x
        return (x, y if q == 0 else y + q * step_y, z, period)

    return read


def terms(value, number):
    out = []
    for _ in range(number - 1):
        part = value.astype(bf16)
        out.append(part)
        value = value - part.astype(f32)
    return out + [value.astype(bf16)]


def dot(left, right, contract=((1,), (0,))):
    return lax.dot_general(left, right, (contract, ((), ())), preferred_element_type=f32)


def wrapped(value, size):
    return jnp.where(value >= size, value - size, value)


def layer_of(row, scale, width):
    return jnp.clip(jnp.floor(row * scale).astype(jnp.int32), 0, width - 1)


def fold(values):
    row = iota(values[0].shape, 0)
    low = row < 4
    values = [
        jnp.where(low, a, b) + pltpu.roll(jnp.where(low, b, a), 4, 0)
        for a, b in zip(values[:4], values[4:])
    ]
    for dist in (2, 1):
        low = (row & dist) == 0
        values = [
            jnp.where(low, a, b) + jnp.where(low, pltpu.roll(a, 8 - dist, 0), pltpu.roll(b, dist, 0))
            for a, b in zip(values[:dist], values[dist:])
        ]
    return values[0]


def stacked(rows):
    comp = iota((8, rows[0].shape[1]), 0)
    out = jnp.zeros((8, rows[0].shape[1]), f32)
    for c, row in enumerate(rows):
        out = jnp.where(comp == c, row, out)
    return out


def axes_of(number):
    height = 1.0 - (2.0 * number + 1.0) / DIRECTIONS
    radius = jnp.sqrt(1.0 - height * height)
    phase = number * golden
    return [radius * jnp.cos(phase), radius * jnp.sin(phase), height]


def pair_sums(own_rows, source):
    dx, dy, dz = [o - s for o, s in zip(own_rows, source[:3])]
    period = source[3]
    half = 0.5 * period
    dz = dz + jnp.where(dz > half, -period, jnp.where(dz < -half, period, 0.0))
    reach = jnp.maximum(1.0 - (dx * dx + dy * dy + dz * dz), 0.0)
    weight = reach * reach
    return [weight * dx, weight * dy, weight * dz]


def force_pass(own, force, sources, first, straight=False):
    slots = own.shape[-1]
    wide = 32 if slots % 32 == 0 else 8

    def block(r, carry):
        at = pl.ds(r * wide if straight else pl.multiple_of(r * wide, wide), wide)
        rows = [own[c, at, :] for c in range(3)]
        total = None if first else [force[c, at, :] for c in range(3)]
        for source in sources:
            parts = pair_sums(rows, source())
            total = parts if total is None else [t + p for t, p in zip(total, parts)]
        for c in range(3):
            force[c, at, :] = total[c]
        return carry

    if straight:
        for r in range(slots // wide):
            block(r, 0)
    else:
        lax.fori_loop(0, slots // wide, block, 0)


def force_rows(force):
    slots = force.shape[1]
    comp = iota((8, slots), 0)
    out = None
    for c in range(3):
        pick = (comp == c).astype(f32).astype(bf16)
        for term in terms(force[c], 2)[::-1]:
            part = dot(pick, term, ((1,), (1,)))
            out = part if out is None else out + part
    return out


def flipped(tiles):
    slots = tiles[0].shape[1]
    pad = jnp.zeros((slots - 8 * len(tiles), slots), f32)
    return jnp.concatenate(tiles + [pad], axis=0).T


def own_columns(own, tile):
    slots = tile.shape[1]
    block = flipped([tile])
    for c in range(3):
        own[c] = jnp.broadcast_to(block[:, c : c + 1], (slots, slots))


def collide_kernel(
    shape, shift_hbm, count, solvent_hbm, occupancy_hbm, axis_hbm, pos_hbm, vel_hbm, mass_hbm,
    out, first, second, third, tiles, early, begun,
    shift, pos, vel, mass, axis, occupancy, held, cell, sums, total, index, edge_x, edge_y, edge_c,
    normals, fields, halo_x, halo_y, halo_c, src, wide, force, own, table,
    small_sem, chunk_sem, halo_send, halo_got, edge_send, edge_got, src_send, src_got,
    wide_send, wide_got,
):
    width_x, width_y, width_z = shape
    n_x, n_y = (width_x // SUB, width_y // SUB)
    rows = 2 * width_y
    slots = mass.shape[2]
    me_x, me_y = (lax.axis_index("gx"), lax.axis_index("yz"))
    size_x, size_y = (lax.axis_size("gx"), lax.axis_size("yz"))

    def device(a, b):
        return (lax.rem(me_x + a + size_x, size_x), lax.rem(me_y + b + size_y, size_y))

    def remote(source, target, send, receive, where):
        return pltpu.make_async_remote_copy(
            src_ref=source, dst_ref=target, send_sem=send, recv_sem=receive,
            device_id=where, device_id_type=MESH,
        )

    around = wide_pairs(size_y)
    edge_c[...] = jnp.zeros_like(edge_c)
    small = [
        pltpu.make_async_copy(source, target, small_sem.at[k])
        for k, (source, target) in enumerate(
            [
                (shift_hbm, shift), (pos_hbm, pos), (vel_hbm, vel),
                (mass_hbm, mass), (axis_hbm, axis), (occupancy_hbm, occupancy),
            ]
        )
    ]
    chunks = [
        pltpu.make_async_copy(
            solvent_hbm.at[:, pl.ds(i * SUB, SUB)], out.at[:, pl.ds(i * SUB, SUB)], chunk_sem.at[i]
        )
        for i in range(n_x)
    ]
    barrier = pltpu.get_barrier_semaphore()

    def greet(pairs):
        for a, b in pairs:
            pl.semaphore_signal(barrier, inc=1, device_id=device(a, b), device_id_type=MESH)

    for copy in small:
        copy.start()
    greet(around[:6])
    for copy in chunks:
        copy.start()
    greet(around[6:])
    for copy in small[:-1]:
        copy.wait()
    shift_x, shift_y, shift_z = (shift[0], shift[1], shift[2])

    alive = iota((1, slots), 1) < count[0, 0]
    cell_x = (layer_of(pos[0, 0], SUB, width_x) + shift_x) >> 2
    cell_y = (layer_of(pos[1, 0], SUB, width_y) + shift_y) >> 2
    layer_z = layer_of(pos[2, 0], 2.0, width_z)
    cell_z = wrapped(layer_z + shift_z, width_z) >> 1
    place = cell_x * (n_y + 1) + cell_y
    weight = jnp.where(alive, mass[0], 0.0)
    comp = iota((8, slots), 0)
    four = comp & 3
    values = jnp.where(
        four == 0, vel[0, 0] * weight,
        jnp.where(four == 1, vel[1, 0] * weight, jnp.where(four == 2, vel[2, 0] * weight, weight)),
    )
    place_half = place - (comp >> 2)
    place_last = jnp.where(comp < 4, place, -1)
    tiles_y = (n_y + 2) // 2

    def in_tile(i, t):
        return (place_half if 2 * t < n_y else place_last) == i * (n_y + 1) + 2 * t

    spread = [
        jnp.where(in_tile(i, t), values, 0.0) for i in range(n_x + 1) for t in range(tiles_y)
    ]
    near = (wrapped(iota((width_z, slots), 0) + shift_z, width_z) >> 1) == cell_z
    near = near.astype(f32).astype(bf16)
    deposit = sum(
        dot(term, near, ((1,), (1,))) for term in terms(jnp.concatenate(spread, axis=0), 3)[::-1]
    )
    sums[...] = deposit.reshape(n_x + 1, tiles_y * 8, width_z)

    cell_row = wrapped(iota((width_z // 2, width_z), 1) + shift_z, width_z) >> 1
    expand = (cell_row == iota((width_z // 2, width_z), 0)).astype(f32).astype(bf16)
    number = axis[...].reshape(n_x * n_y, width_z // 2).astype(f32).astype(bf16)
    index[...] = dot(number, expand).reshape(n_x, n_y, width_z)

    for c, part in enumerate(axes_of(iota((DIRECTIONS, slots), 0).astype(f32))):
        table[c] = part
    start = stacked([jnp.where(alive, pos[0, 0], far_away), pos[1, 0], pos[2, 0]])
    kick = jnp.broadcast_to((timestep * stiffness * cutoff) / mass[0], (8, slots))
    src[0, OWN] = jnp.where(comp == 3, kick, start * (1.0 / cutoff))

    double = (iota((SUB * rows, SUB * width_y), 0) >> 1 == iota((SUB * rows, SUB * width_y), 1)).astype(bf16)
    small[-1].wait()
    for i in range(n_x):
        at = pl.ds(i * SUB, SUB)
        filled = occupancy[at].reshape(SUB * width_y, width_z).astype(f32).astype(bf16)
        held[at] = dot(double, filled).reshape(SUB, rows, width_z)
    row = iota((8, width_z), 0)
    odd = (row & 1).astype(f32)
    stays_1 = jnp.broadcast_to(shift_x, (8, width_z)) <= 2
    stays_2 = jnp.broadcast_to(shift_x, (8, width_z)) <= 1
    later = ((row >> 1) + shift_y) >= SUB
    even = ((iota((8, width_z), 1) + shift_z) & 1) == 0
    halves = jnp.where((row & 3) == 3, 0.5, 1.0)
    blank = jnp.zeros((8, width_z), f32)

    def finish(i):
        def straddling(c, j):
            now = cell[i, c, pl.ds(8 * j, 8), :] if j < n_y else blank
            before = cell[i, c, pl.ds(8 * (j - 1), 8), :] if j > 0 else blank
            return jnp.where(later, before, now)

        for t in range(tiles_y):
            blocks = [
                straddling(q & 3, 2 * t + (q >> 2)) if 2 * t + (q >> 2) <= n_y else blank
                for q in range(8)
            ]
            tile = fold(blocks) * halves
            partner = jnp.where(even, pltpu.roll(tile, width_z - 1, 1), pltpu.roll(tile, 1, 1))
            sums[i, pl.ds(8 * t, 8), :] += tile + partner

    def gather(i):
        for b in range(n_y):
            at = pl.ds(8 * b, 8)
            filled = [held[i * SUB + r, at, :] for r in range(SUB)]
            live = [f > odd for f in filled]
            for c in range(4):
                v = filled
                if c < 3:
                    v = [jnp.where(live[r], out[c, i * SUB + r, at, :], 0.0) for r in range(SUB)]
                front = v[0] + v[1]
                back = v[3] + v[2]
                stay = jnp.where(stays_1, jnp.where(stays_2, front + v[2], front), v[0])
                move = jnp.where(stays_1, jnp.where(stays_2, v[3], back), back + v[1])
                cell[i, c, at, :] = stay if i == 0 else cell[i, c, at, :] + stay
                cell[i + 1, c, at, :] = move

    for i in range(n_x):
        chunks[i].wait()
        gather(i)
        if i > 0:
            finish(i - 1)
    finish(n_x - 1)
    finish(n_x)

    pl.semaphore_wait(barrier, len(around))

    def exchange(step):
        mine = src.at[step, OWN, pl.ds(0, 4)]
        copies = {}
        for a, b in AROUND:
            k = slot_of(a, b)
            copies[k] = remote(
                mine, src.at[step, 8 - k, pl.ds(0, 4)],
                src_send.at[step, k], src_got.at[step, 8 - k], device(a, b),
            )
            copies[k].start()
        return list(copies.values())

    sends = exchange(0)

    at_low, at_high = (pl.ds(0, 4), pl.ds(n_y * SUB, 4))
    every = pl.ds(0, n_x + 1)
    halo = [
        (sums.at[n_x], halo_x.at[0], (1, 0)),
        (sums.at[0], halo_x.at[1], (-1, 0)),
        (sums.at[every, at_high], halo_y.at[0, every, at_low], (0, 1)),
        (sums.at[every, at_low], halo_y.at[1, every, at_low], (0, -1)),
        (sums.at[n_x, at_high], halo_c.at[0, at_low], (1, 1)),
        (sums.at[n_x, at_low], halo_c.at[1, at_low], (1, -1)),
        (sums.at[0, at_high], halo_c.at[2, at_low], (-1, 1)),
        (sums.at[0, at_low], halo_c.at[3, at_low], (-1, -1)),
    ]
    halo = [
        remote(source, target, halo_send.at[k], halo_got.at[k], device(*where))
        for k, (source, target, where) in enumerate(halo)
    ]
    for copy in halo:
        copy.start()
    edges = [
        (index.at[0], edge_x, (-1, 0)),
        (index.at[pl.ds(0, n_x), 0], edge_y, (0, -1)),
        (index.at[0, pl.ds(0, 1)], edge_c.at[pl.ds(0, 1)], (-1, -1)),
    ]
    edges = [
        remote(source, target, edge_send.at[k], edge_got.at[k], device(*where))
        for k, (source, target, where) in enumerate(edges)
    ]
    for copy in edges:
        copy.start()

    steps = ((width_z // 2) / cutoff, n_x / cutoff, n_y / cutoff)
    columns_x = sides(me_x)
    quick, slow = columns_x[1:]

    def source(step, a, b):
        return reader(src.at[step], slot_of(a, b), a, b, steps)

    def arrived(step, a, b):
        slot = slot_of(a, b)
        remote(
            src.at[step, OWN, pl.ds(0, 4)], src.at[step, slot, pl.ds(0, 4)],
            src_send.at[step, slot], src_got.at[step, slot], device(0, 1),
        ).wait_recv()

    def early_forces(step):
        for b in (-1, 1):
            arrived(step, 0, b)
        force_pass(own, force, [source(step, 0, b) for b in (0, -1, 1)], True)
        for b in (-1, 0, 1):
            arrived(step, quick, b)
        force_pass(own, force, [source(step, quick, b) for b in (-1, 0, 1)], False)

    def late_arrivals(step):
        for b in (-1, 0, 1):
            arrived(step, slow, b)

    def late_forces(step):
        force_pass(own, force, [source(step, slow, b) for b in (-1, 0, 1)], False, True)
        return force_rows(force)

    own_columns(own, src[0, OWN])
    early_forces(0)
    late_arrivals(0)
    for copy in edges + halo:
        copy.wait_recv()
    push = late_forces(0)

    total[...] = sums[...]
    total[0] += halo_x[0]
    total[n_x] += halo_x[1]
    for i in range(n_x + 1):
        total[i, at_low, :] += halo_y[0, i, at_low, :]
        total[i, at_high, :] += halo_y[1, i, at_low, :]
    total[0, at_low, :] += halo_c[0, at_low, :]
    total[0, at_high, :] += halo_c[1, at_low, :]
    total[n_x, at_low, :] += halo_c[2, at_low, :]
    total[n_x, at_high, :] += halo_c[3, at_low, :]

    chosen = (iota((width_z, slots), 0) == layer_z).astype(f32).astype(bf16)
    block = total[...].reshape((n_x + 1) * tiles_y * 8, width_z)
    at_z = sum(dot(term, chosen) for term in terms(block, 2)[::-1])
    picked = jnp.zeros((8, slots), f32)
    for i in range(n_x + 1):
        for t in range(tiles_y):
            n = 8 * (i * tiles_y + t)
            picked = picked + jnp.where(in_tile(i, t), at_z[n : n + 8], 0.0)
    picked = picked + pltpu.roll(picked, 4, 0)
    numbers = jnp.concatenate(
        [index[...].reshape(n_x * n_y, width_z), edge_x[...], edge_y[...], edge_c[...]], axis=0
    )
    at_z = dot(numbers.astype(bf16), chosen)
    wanted = [place - comp == i * (n_y + 1) for i in range(n_x + 1)]
    wanted.append(place - comp * (n_y + 1) == n_y)
    wanted.append(jnp.logical_and(comp == 0, place == n_x * (n_y + 1) + n_y))
    found = jnp.zeros((8, slots), f32)
    for n, mask in enumerate(wanted):
        found = found + jnp.where(mask, at_z[8 * n : 8 * n + 8], 0.0)
    name = jnp.sum(found, axis=0, keepdims=True).astype(jnp.int32)
    heavy = jnp.maximum(picked[3:4], fill_mass)
    mean = [picked[c : c + 1] / heavy for c in range(3)]
    n = []
    for c in range(3):
        hit = [
            jnp.where(iota((8, slots), 0) + 8 * r == name, table[c, pl.ds(8 * r, 8), :], 0.0)
            for r in range(DIRECTIONS // 8)
        ]
        n.append(jnp.sum(sum(hit), axis=0, keepdims=True))
    rel = [vel[c, 0] - mean[c] for c in range(3)]
    cross = [n[1] * rel[2] - n[2] * rel[1], n[2] * rel[0] - n[0] * rel[2], n[0] * rel[1] - n[1] * rel[0]]
    along = n[0] * rel[0] + n[1] * rel[1] + n[2] * rel[2]
    speed = stacked([
        mean[c] + cos_angle * rel[c] + sin_angle * cross[c] + (1.0 - cos_angle) * along * n[c]
        for c in range(3)
    ])
    place_now = start

    def cell_fields(i, rows_of):
        for b in range(n_y):
            pair = [
                [jnp.where(later, total[i, pl.ds(4 * (b + 1) + c, 1), :], total[i, pl.ds(4 * b + c, 1), :])
                 for c in range(4)],
                [jnp.where(later, normals[c, pl.ds(rows_of(b + 1), 1), :], normals[c, pl.ds(rows_of(b), 1), :])
                 for c in range(3)],
            ]
            scale = 1.0 / jnp.maximum(pair[0][3], fill_mass)
            for c in range(3):
                fields[i, b, c] = pair[0][c] * scale
                fields[i, b, 3 + c] = pair[1][c]

    def turn(x, carry):
        at_cell = (x + shift_x) >> 2
        for b in range(n_y):
            at = pl.ds(8 * b, 8)
            mean = [fields[at_cell, b, c] for c in range(3)]
            n = [fields[at_cell, b, 3 + c] for c in range(3)]
            old = [out[c, x, at, :] for c in range(3)]
            rel = [old[c] - mean[c] for c in range(3)]
            along = (1.0 - cos_angle) * (n[0] * rel[0] + n[1] * rel[1] + n[2] * rel[2])
            cross = [
                n[1] * rel[2] - n[2] * rel[1],
                n[2] * rel[0] - n[0] * rel[2],
                n[0] * rel[1] - n[1] * rel[0],
            ]
            live = held[x, at, :] > odd
            for c in range(3):
                new = mean[c] + cos_angle * rel[c] + sin_angle * cross[c] + along * n[c]
                out[c, x, at, :] = jnp.where(live, new, old[c])
        return carry

    def idle_work(step):
        if step == 1:
            for c, part in enumerate(axes_of(numbers)):
                normals[c] = part

            def inner(i, carry):
                cell_fields(i, lambda b: i * n_y + b if b < n_y else n_x * n_y + 8 + i)
                return carry

            lax.fori_loop(0, n_x, inner, 0)
            cell_fields(n_x, lambda b: n_x * n_y + b if b < n_y else n_x * n_y + 16)
            lax.fori_loop(0, width_x // 2, turn, 0)
        if step == 2:
            lax.fori_loop(width_x // 2, width_x, turn, 0)

    speed = speed + push * kick
    place_now = place_now + timestep * speed
    src[1, OWN] = place_now * (1.0 / cutoff)
    sends = sends + exchange(1)
    own_columns(own, src[1, OWN])
    idle_work(1)
    early_forces(1)
    late_arrivals(1)
    push = late_forces(1)

    speed = speed + push * kick
    place_now = place_now + timestep * speed
    def at_wide(a, b):
        return wide_slot(a, b, size_y)

    mine = at_wide(0, 0)
    wide[mine] = place_now * (1.0 / cutoff)
    spread = {}
    for a, b in around:
        k, target = (at_wide(a, b), at_wide(-a, -b))
        spread[a, b] = remote(
            wide.at[mine, pl.ds(0, 4)], wide.at[target, pl.ds(0, 4)],
            wide_send.at[k], wide_got.at[target], device(a, b),
        )
        spread[a, b].start()

    def wide_arrived(a):
        for b in (-1, 0, 1, -2, 2):
            if (isinstance(a, int) and b == 0) or folded(b, size_y) != b:
                continue
            k = at_wide(a, b)
            remote(
                wide.at[mine, pl.ds(0, 4)], wide.at[k, pl.ds(0, 4)],
                wide_send.at[k], wide_got.at[k], device(0, 1),
            ).wait_recv()

    idle_work(2)
    first[...] = src[0]
    second[...] = src[1]
    tiles[0] = place_now
    tiles[1] = speed
    tiles[2] = stacked([pos[c, 0] for c in range(3)])
    tiles[3] = stacked([vel[c, 0] for c in range(3)])
    tiles[4] = jnp.broadcast_to(jnp.where(alive, 1.0, 0.0), (8, slots))
    for k, a in enumerate(columns_x[:2]):
        wide_arrived(a)
        block = flipped([wide[at_wide(a, b)] for b in (-1, 0, 1)])
        for m in range(3):
            for c in range(3):
                column = block[:, 8 * m + c : 8 * m + c + 1]
                early[3 * k + m, c] = jnp.broadcast_to(column, (slots, slots))
        for m in range(3):
            around_m = [reader(wide, at_wide(a, m - 1 + q), a, q, steps) for q in (-1, 0, 1)]
            force_pass(early.at[m], begun.at[m], around_m, k == 0)
    wide_arrived(slow)
    for a in (-2 * quick, 2 * quick):
        wide_arrived(a)
    third[...] = wide[...]
    for copy in sends + halo + edges + list(spread.values()):
        copy.wait_send()


def finish_kernel(
    shape, turned, first, second, third, tiles, early, begun,
    out, pos_out, vel_out, own, force, later, sums, sem
):
    width_x, width_y, width_z = shape
    n_x, n_y = (width_x // SUB, width_y // SUB)
    slots = first.shape[2]
    size_y = lax.axis_size("yz")
    columns_x = sides(lax.axis_index("gx"))
    copies = []
    for c in range(3):
        copies.append(pltpu.make_async_copy(turned.at[c], out.at[c], sem.at[c]))
        copies[-1].start()

    steps = ((width_z // 2) / cutoff, n_x / cutoff, n_y / cutoff)
    block = 16 if slots % 16 == 0 else 8
    half = slots // 2
    group = [(k, b) for k in range(3) for b in (-1, 0, 1)]

    def at_wide(k, b, p=0):
        return wide_slot(columns_x[k] + p, b, size_y)

    def halves(most, work):
        work(0)
        pl.when(most * block > half)(lambda: work(half))

    def columns(tiles, most):
        sums[...] = flipped(tiles)

        def work(start):
            at = pl.ds(start, half)
            for n in range(len(tiles)):
                for c in range(3):
                    column = sums[at, 8 * n + c : 8 * n + c + 1]
                    own[n, c, at, :] = jnp.broadcast_to(column, (half, slots))

        halves(most, work)

    def pushes(m, columns_of, trips, sources, before=None):
        def body(r, carry):
            at = pl.ds(pl.multiple_of(r * block, block), block)
            rows = [columns_of[c, at, :] for c in range(3)]
            total = None if before is None else [before[c, at, :] for c in range(3)]
            for source in sources:
                parts = pair_sums(rows, source())
                total = parts if total is None else [t + p for t, p in zip(total, parts)]
            for c in range(3):
                force[m, c, at, :] = total[c]
            return carry

        lax.fori_loop(0, trips, body, 0)

    def rows_of(number, most):
        lane = iota((half, slots), 1)

        def work(start):
            at = pl.ds(start, half)
            block = jnp.zeros((half, slots), f32)
            for n in range(number):
                for c in range(3):
                    total = jnp.sum(force[n, c, at, :], axis=1, keepdims=True)
                    block = jnp.where(lane == 8 * n + c, total, block)
            sums[at, :] = block

        halves(most, work)
        return sums[...].T

    dead = [third[at_wide(k, b), pl.ds(0, 1), :] > 0.1 * far_away for k, b in group]
    trips = [
        (jnp.sum(jnp.where(gone, 0.0, 1.0)).astype(jnp.int32) + (block - 1)) // block for gone in dead
    ]
    most = functools.reduce(jnp.maximum, trips)
    columns([third[at_wide(2, b)] for b in (-1, 0, 1)], most)
    for m, (k, b) in enumerate(group):
        if k == 0:
            slow = columns_x[2]
            around_m = [reader(third, at_wide(2, b + q), slow, q, steps) for q in (-1, 0, 1)]
            pushes(m, early.at[m], trips[m], around_m, begun.at[m])
        else:
            around_m = [
                reader(third, at_wide(k, b + q, p), p, q, steps) for p in (-1, 0, 1) for q in (-1, 0, 1)
            ]
            pushes(m, early.at[m] if k == 1 else own.at[m - 6], trips[m], around_m)
    push = rows_of(len(group), most)
    speed, place = (tiles[1], tiles[0])
    for m, (k, b) in enumerate(group):
        near = slot_of(columns_x[k], b)
        now = third[at_wide(k, b)]
        mine = push[8 * m : 8 * m + 8]
        kick = jnp.broadcast_to(first[near, pl.ds(3, 1), :], (8, slots))
        if (k, b) == (0, 0):
            speed = speed + mine * kick
            place = place + timestep * speed
            moved = place * (1.0 / cutoff)
            own_kick, own_trips = (kick, trips[m])
        else:
            moved = now + (now - second[near]) + (timestep / cutoff) * (mine * kick)
        later[m] = jnp.where(jnp.broadcast_to(dead[m], (8, slots)), now, moved)
    columns([later[1]], own_trips)
    around_m = [reader(later, m, columns_x[k], b, steps) for m, (k, b) in enumerate(group)]
    pushes(0, own.at[0], own_trips, around_m)
    speed = speed + rows_of(1, own_trips)[:8] * own_kick
    place = place + timestep * speed
    alive = tiles[4] > 0
    place = jnp.where(alive, place, tiles[2])
    speed = jnp.where(alive, speed, tiles[3])
    for c in range(3):
        pos_out[c, 0] = place[c : c + 1]
        vel_out[c, 0] = speed[c : c + 1]
    for copy in copies:
        copy.wait()


def per_device(
    solvent_vel, occupancy, grid_shift, axis_index, colloid_pos, colloid_vel, colloid_mass, colloid_count
):
    shape = occupancy.shape
    width_x, width_y, width_z = shape
    rows = 2 * width_y
    n_x, n_y = (width_x // SUB, width_y // SUB)
    slots = colloid_mass.shape[2]
    solvent = solvent_vel.reshape(3, width_x, rows, width_z)
    smem = pl.BlockSpec(memory_space=pltpu.SMEM)
    vmem = pl.BlockSpec(memory_space=pltpu.VMEM)
    hbm = pl.BlockSpec(memory_space=pltpu.HBM)
    tall = (n_y + 2) // 2 * 8
    dma = pltpu.SemaphoreType.DMA

    def in_hbm(x):
        return pltpu.with_memory_space_constraint(x, pltpu.HBM)

    turned, *states = pl.pallas_call(
        functools.partial(collide_kernel, shape),
        out_shape=[
            pltpu.VMEM(solvent.shape, f32),
            pltpu.VMEM((9, 8, slots), f32),
            pltpu.VMEM((9, 8, slots), f32),
            pltpu.VMEM((25, 8, slots), f32),
            pltpu.VMEM((5, 8, slots), f32),
            pltpu.VMEM((6, 3, slots, slots), f32),
            pltpu.VMEM((3, 3, slots, slots), f32),
        ],
        in_specs=[hbm, smem] + [hbm] * 6,
        out_specs=[vmem] * 7,
        scratch_shapes=[
            pltpu.SMEM(grid_shift.shape, jnp.int32),
            pltpu.VMEM(colloid_pos.shape, f32),
            pltpu.VMEM(colloid_vel.shape, f32),
            pltpu.VMEM(colloid_mass.shape, f32),
            pltpu.VMEM(axis_index.shape, jnp.int32),
            pltpu.VMEM(shape, jnp.int32),
            pltpu.VMEM((width_x, rows, width_z), f32),
            pltpu.VMEM((n_x + 1, 4, rows, width_z), f32),
            pltpu.VMEM((n_x + 1, tall, width_z), f32),
            pltpu.VMEM((n_x + 1, tall, width_z), f32),
            pltpu.VMEM((n_x, n_y, width_z), f32),
            pltpu.VMEM((8, width_z), f32),
            pltpu.VMEM((8, width_z), f32),
            pltpu.VMEM((8, width_z), f32),
            pltpu.VMEM((3, n_x * n_y + 24, width_z), f32),
            pltpu.VMEM((n_x + 1, n_y, 6, 8, width_z), f32),
            pltpu.VMEM((2, tall, width_z), f32),
            pltpu.VMEM((2, n_x + 1, 8, width_z), f32),
            pltpu.VMEM((4, 8, width_z), f32),
            pltpu.VMEM((2, 9, 8, slots), f32),
            pltpu.VMEM((25, 8, slots), f32),
            pltpu.VMEM((3, slots, slots), f32),
            pltpu.VMEM((3, slots, slots), f32),
            pltpu.VMEM((3, DIRECTIONS, slots), f32),
            dma((6,)),
            dma((n_x,)),
            dma((8,)),
            dma((8,)),
            dma((3,)),
            dma((3,)),
            dma((2, 9)),
            dma((2, 9)),
            dma((25,)),
            dma((25,)),
        ],
        compiler_params=pltpu.CompilerParams(
            collective_id=0, has_side_effects=True, vmem_limit_bytes=32 * 2**20
        ),
        name="collide",
    )(
        in_hbm(grid_shift), colloid_count, in_hbm(solvent), in_hbm(occupancy), in_hbm(axis_index),
        in_hbm(colloid_pos), in_hbm(colloid_vel), in_hbm(colloid_mass),
    )

    solvent_out, pos_out, vel_out = pl.pallas_call(
        functools.partial(finish_kernel, shape),
        out_shape=[
            jax.ShapeDtypeStruct(solvent.shape, f32),
            jax.ShapeDtypeStruct(colloid_pos.shape, f32),
            jax.ShapeDtypeStruct(colloid_vel.shape, f32),
        ],
        in_specs=[vmem] * 7,
        out_specs=[hbm, vmem, vmem],
        scratch_shapes=[
            pltpu.VMEM((3, 3, slots, slots), f32),
            pltpu.VMEM((9, 3, slots, slots), f32),
            pltpu.VMEM((9, 8, slots), f32),
            pltpu.VMEM((slots, slots), f32),
            dma((3,)),
        ],
        compiler_params=pltpu.CompilerParams(vmem_limit_bytes=16 * 2**20),
        name="finish",
    )(turned, *states)
    return (solvent_out.reshape(solvent_vel.shape), pos_out, vel_out)


def solution(mesh):
    return jax.shard_map(
        per_device,
        mesh=mesh,
        in_specs=(
            P(None, "gx", "yz", None, None),
            P("gx", "yz", None),
            P(),
            P("gx", "yz", None),
            P(None, "gx", "yz", None),
            P(None, "gx", "yz", None),
            P("gx", "yz", None),
            P("gx", "yz"),
        ),
        out_specs=(
            P(None, "gx", "yz", None, None),
            P(None, "gx", "yz", None),
            P(None, "gx", "yz", None),
        ),
        check_vma=False,
    )
```

```python
import functools
import math

import jax
import jax.numpy as jnp
from jax import lax
from jax.experimental import pallas as pl
from jax.experimental.pallas import tpu as pltpu
from jax.sharding import PartitionSpec as P

SUB = 4
SUBSTEPS = 4
DIRECTIONS = 64

turn_angle = 130.0 * math.pi / 180.0
cos_angle = math.cos(turn_angle)
sin_angle = math.sin(turn_angle)
golden = math.pi * (3.0 - math.sqrt(5.0))
cutoff = 1.5
stiffness = 20.0
timestep = 0.05
fill_mass = 16.0
far_away = 1.0e9
MESH = pl.DeviceIdType.MESH
f32 = jnp.float32
bf16 = jnp.bfloat16
RING = [(a, b) for a in (-1, 0, 1) for b in (-1, 0, 1)]
AROUND = [pair for pair in RING if pair != (0, 0)]
OWN = 4


def iota(shape, dim):
    return lax.broadcasted_iota(jnp.int32, shape, dim)


def slot_of(a, b):
    return (a + 1) * 3 + b + 1


def folded(b, size_y):
    return 2 if b == -2 and size_y == 4 else b


def wide_slot(a, b, size_y):
    return (a + 2) * 5 + folded(b, size_y) + 2


def wide_pairs(size_y):
    return [
        (a, b) for a in (-1, 1, -2, 2, 0) for b in (-1, 0, 1, -2, 2)
        if (a, b) != (0, 0) and folded(b, size_y) == b
    ]


def sides(me_x):
    quick = 1 - 2 * (me_x & 1)
    return (0, quick, -quick)


def reader(ref, slot, p, q, steps):
    period, step_x, step_y = steps

    def read():
        x, y, z = [ref[slot, pl.ds(c, 1), :] for c in range(3)]
        if not isinstance(p, int):
            x = x + p.astype(f32) * step_x
        elif p != 0:
            x = x + p * step_x
        return (x, y if q == 0 else y + q * step_y, z, period)

    return read


def terms(value, number):
    out = []
    for _ in range(number - 1):
        part = value.astype(bf16)
        out.append(part)
        value = value - part.astype(f32)
    return out + [value.astype(bf16)]


def dot(left, right, contract=((1,), (0,))):
    return lax.dot_general(left, right, (contract, ((), ())), preferred_element_type=f32)


def wrapped(value, size):
    return jnp.where(value >= size, value - size, value)


def layer_of(row, scale, width):
    return jnp.clip(jnp.floor(row * scale).astype(jnp.int32), 0, width - 1)


def fold(values):
    row = iota(values[0].shape, 0)
    low = row < 4
    values = [
        jnp.where(low, a, b) + pltpu.roll(jnp.where(low, b, a), 4, 0)
        for a, b in zip(values[:4], values[4:])
    ]
    for dist in (2, 1):
        low = (row & dist) == 0
        values = [
            jnp.where(low, a, b) + jnp.where(low, pltpu.roll(a, 8 - dist, 0), pltpu.roll(b, dist, 0))
            for a, b in zip(values[:dist], values[dist:])
        ]
    return values[0]


def stacked(rows):
    comp = iota((8, rows[0].shape[1]), 0)
    out = jnp.zeros((8, rows[0].shape[1]), f32)
    for c, row in enumerate(rows):
        out = jnp.where(comp == c, row, out)
    return out


def axes_of(number):
    height = 1.0 - (2.0 * number + 1.0) / DIRECTIONS
    radius = jnp.sqrt(1.0 - height * height)
    phase = number * golden
    return [radius * jnp.cos(phase), radius * jnp.sin(phase), height]


def pair_sums(own_rows, source):
    dx, dy, dz = [o - s for o, s in zip(own_rows, source[:3])]
    period = source[3]
    half = 0.5 * period
    dz = dz + jnp.where(dz > half, -period, jnp.where(dz < -half, period, 0.0))
    reach = jnp.maximum(1.0 - (dx * dx + dy * dy + dz * dz), 0.0)
    weight = reach * reach
    return [weight * dx, weight * dy, weight * dz]


def force_pass(own, force, sources, first, straight=False):
    slots = own.shape[-1]
    wide = 32 if slots % 32 == 0 else 8

    def block(r, carry):
        at = pl.ds(r * wide if straight else pl.multiple_of(r * wide, wide), wide)
        rows = [own[c, at, :] for c in range(3)]
        total = None if first else [force[c, at, :] for c in range(3)]
        for source in sources:
            parts = pair_sums(rows, source())
            total = parts if total is None else [t + p for t, p in zip(total, parts)]
        for c in range(3):
            force[c, at, :] = total[c]
        return carry

    if straight:
        for r in range(slots // wide):
            block(r, 0)
    else:
        lax.fori_loop(0, slots // wide, block, 0)


def force_rows(force):
    slots = force.shape[1]
    comp = iota((8, slots), 0)
    out = None
    for c in range(3):
        pick = (comp == c).astype(f32).astype(bf16)
        for term in terms(force[c], 2)[::-1]:
            part = dot(pick, term, ((1,), (1,)))
            out = part if out is None else out + part
    return out


def flipped(tiles):
    slots = tiles[0].shape[1]
    pad = jnp.zeros((slots - 8 * len(tiles), slots), f32)
    return jnp.concatenate(tiles + [pad], axis=0).T


def own_columns(own, tile):
    slots = tile.shape[1]
    block = flipped([tile])
    for c in range(3):
        own[c] = jnp.broadcast_to(block[:, c : c + 1], (slots, slots))


def collide_kernel(
    shape, shift_hbm, count, solvent_hbm, occupancy_hbm, axis_hbm, pos_hbm, vel_hbm, mass_hbm,
    out, first, second, third, tiles, early, begun,
    shift, pos, vel, mass, axis, occupancy, held, cell, sums, total, index, edge_x, edge_y, edge_c,
    normals, fields, halo_x, halo_y, halo_c, src, wide, force, own, table,
    small_sem, chunk_sem, halo_send, halo_got, edge_send, edge_got, src_send, src_got,
    wide_send, wide_got,
):
    width_x, width_y, width_z = shape
    n_x, n_y = (width_x // SUB, width_y // SUB)
    rows = 2 * width_y
    slots = mass.shape[2]
    me_x, me_y = (lax.axis_index("gx"), lax.axis_index("yz"))
    size_x, size_y = (lax.axis_size("gx"), lax.axis_size("yz"))

    def device(a, b):
        return (lax.rem(me_x + a + size_x, size_x), lax.rem(me_y + b + size_y, size_y))

    def remote(source, target, send, receive, where):
        return pltpu.make_async_remote_copy(
            src_ref=source, dst_ref=target, send_sem=send, recv_sem=receive,
            device_id=where, device_id_type=MESH,
        )

    around = wide_pairs(size_y)
    edge_c[...] = jnp.zeros_like(edge_c)
    small = [
        pltpu.make_async_copy(source, target, small_sem.at[k])
        for k, (source, target) in enumerate(
            [
                (shift_hbm, shift), (pos_hbm, pos), (vel_hbm, vel),
                (mass_hbm, mass), (axis_hbm, axis), (occupancy_hbm, occupancy),
            ]
        )
    ]
    chunks = [
        pltpu.make_async_copy(
            solvent_hbm.at[:, pl.ds(i * SUB, SUB)], out.at[:, pl.ds(i * SUB, SUB)], chunk_sem.at[i]
        )
        for i in range(n_x)
    ]
    barrier = pltpu.get_barrier_semaphore()

    def greet(pairs):
        for a, b in pairs:
            pl.semaphore_signal(barrier, inc=1, device_id=device(a, b), device_id_type=MESH)

    for copy in small:
        copy.start()
    greet(around[:6])
    for copy in chunks:
        copy.start()
    greet(around[6:])
    for copy in small[:-1]:
        copy.wait()
    shift_x, shift_y, shift_z = (shift[0], shift[1], shift[2])

    alive = iota((1, slots), 1) < count[0, 0]
    cell_x = (layer_of(pos[0, 0], SUB, width_x) + shift_x) >> 2
    cell_y = (layer_of(pos[1, 0], SUB, width_y) + shift_y) >> 2
    layer_z = layer_of(pos[2, 0], 2.0, width_z)
    cell_z = wrapped(layer_z + shift_z, width_z) >> 1
    place = cell_x * (n_y + 1) + cell_y
    weight = jnp.where(alive, mass[0], 0.0)
    comp = iota((8, slots), 0)
    four = comp & 3
    values = jnp.where(
        four == 0, vel[0, 0] * weight,
        jnp.where(four == 1, vel[1, 0] * weight, jnp.where(four == 2, vel[2, 0] * weight, weight)),
    )
    place_half = place - (comp >> 2)
    place_last = jnp.where(comp < 4, place, -1)
    tiles_y = (n_y + 2) // 2

    def in_tile(i, t):
        return (place_half if 2 * t < n_y else place_last) == i * (n_y + 1) + 2 * t

    spread = [
        jnp.where(in_tile(i, t), values, 0.0) for i in range(n_x + 1) for t in range(tiles_y)
    ]
    near = (wrapped(iota((width_z, slots), 0) + shift_z, width_z) >> 1) == cell_z
    near = near.astype(f32).astype(bf16)
    deposit = sum(
        dot(term, near, ((1,), (1,))) for term in terms(jnp.concatenate(spread, axis=0), 3)[::-1]
    )
    sums[...] = deposit.reshape(n_x + 1, tiles_y * 8, width_z)

    cell_row = wrapped(iota((width_z // 2, width_z), 1) + shift_z, width_z) >> 1
    expand = (cell_row == iota((width_z // 2, width_z), 0)).astype(f32).astype(bf16)
    number = axis[...].reshape(n_x * n_y, width_z // 2).astype(f32).astype(bf16)
    index[...] = dot(number, expand).reshape(n_x, n_y, width_z)

    for c, part in enumerate(axes_of(iota((DIRECTIONS, slots), 0).astype(f32))):
        table[c] = part
    start = stacked([jnp.where(alive, pos[0, 0], far_away), pos[1, 0], pos[2, 0]])
    kick = jnp.broadcast_to((timestep * stiffness * cutoff) / mass[0], (8, slots))
    src[0, OWN] = jnp.where(comp == 3, kick, start * (1.0 / cutoff))

    double = (iota((SUB * rows, SUB * width_y), 0) >> 1 == iota((SUB * rows, SUB * width_y), 1)).astype(bf16)
    small[-1].wait()
    for i in range(n_x):
        at = pl.ds(i * SUB, SUB)
        filled = occupancy[at].reshape(SUB * width_y, width_z).astype(f32).astype(bf16)
        held[at] = dot(double, filled).reshape(SUB, rows, width_z)
    row = iota((8, width_z), 0)
    odd = (row & 1).astype(f32)
    stays_1 = jnp.broadcast_to(shift_x, (8, width_z)) <= 2
    stays_2 = jnp.broadcast_to(shift_x, (8, width_z)) <= 1
    later = ((row >> 1) + shift_y) >= SUB
    even = ((iota((8, width_z), 1) + shift_z) & 1) == 0
    halves = jnp.where((row & 3) == 3, 0.5, 1.0)
    blank = jnp.zeros((8, width_z), f32)

    def finish(i):
        def straddling(c, j):
            now = cell[i, c, pl.ds(8 * j, 8), :] if j < n_y else blank
            before = cell[i, c, pl.ds(8 * (j - 1), 8), :] if j > 0 else blank
            return jnp.where(later, before, now)

        for t in range(tiles_y):
            blocks = [
                straddling(q & 3, 2 * t + (q >> 2)) if 2 * t + (q >> 2) <= n_y else blank
                for q in range(8)
            ]
            tile = fold(blocks) * halves
            partner = jnp.where(even, pltpu.roll(tile, width_z - 1, 1), pltpu.roll(tile, 1, 1))
            sums[i, pl.ds(8 * t, 8), :] += tile + partner

    def gather(i):
        for b in range(n_y):
            at = pl.ds(8 * b, 8)
            filled = [held[i * SUB + r, at, :] for r in range(SUB)]
            live = [f > odd for f in filled]
            for c in range(4):
                v = filled
                if c < 3:
                    v = [jnp.where(live[r], out[c, i * SUB + r, at, :], 0.0) for r in range(SUB)]
                front = v[0] + v[1]
                back = v[3] + v[2]
                stay = jnp.where(stays_1, jnp.where(stays_2, front + v[2], front), v[0])
                move = jnp.where(stays_1, jnp.where(stays_2, v[3], back), back + v[1])
                cell[i, c, at, :] = stay if i == 0 else cell[i, c, at, :] + stay
                cell[i + 1, c, at, :] = move

    for i in range(n_x):
        chunks[i].wait()
        gather(i)
        if i > 0:
            finish(i - 1)
    finish(n_x - 1)
    finish(n_x)

    pl.semaphore_wait(barrier, len(around))

    def exchange(step):
        mine = src.at[step, OWN, pl.ds(0, 4)]
        copies = {}
        for a, b in AROUND:
            k = slot_of(a, b)
            copies[k] = remote(
                mine, src.at[step, 8 - k, pl.ds(0, 4)],
                src_send.at[step, k], src_got.at[step, 8 - k], device(a, b),
            )
            copies[k].start()
        return list(copies.values())

    sends = exchange(0)

    at_low, at_high = (pl.ds(0, 4), pl.ds(n_y * SUB, 4))
    every = pl.ds(0, n_x + 1)
    halo = [
        (sums.at[n_x], halo_x.at[0], (1, 0)),
        (sums.at[0], halo_x.at[1], (-1, 0)),
        (sums.at[every, at_high], halo_y.at[0, every, at_low], (0, 1)),
        (sums.at[every, at_low], halo_y.at[1, every, at_low], (0, -1)),
        (sums.at[n_x, at_high], halo_c.at[0, at_low], (1, 1)),
        (sums.at[n_x, at_low], halo_c.at[1, at_low], (1, -1)),
        (sums.at[0, at_high], halo_c.at[2, at_low], (-1, 1)),
        (sums.at[0, at_low], halo_c.at[3, at_low], (-1, -1)),
    ]
    halo = [
        remote(source, target, halo_send.at[k], halo_got.at[k], device(*where))
        for k, (source, target, where) in enumerate(halo)
    ]
    for copy in halo:
        copy.start()
    edges = [
        (index.at[0], edge_x, (-1, 0)),
        (index.at[pl.ds(0, n_x), 0], edge_y, (0, -1)),
        (index.at[0, pl.ds(0, 1)], edge_c.at[pl.ds(0, 1)], (-1, -1)),
    ]
    edges = [
        remote(source, target, edge_send.at[k], edge_got.at[k], device(*where))
        for k, (source, target, where) in enumerate(edges)
    ]
    for copy in edges:
        copy.start()

    steps = ((width_z // 2) / cutoff, n_x / cutoff, n_y / cutoff)
    columns_x = sides(me_x)
    quick, slow = columns_x[1:]

    def source(step, a, b):
        return reader(src.at[step], slot_of(a, b), a, b, steps)

    def arrived(step, a, b):
        slot = slot_of(a, b)
        remote(
            src.at[step, OWN, pl.ds(0, 4)], src.at[step, slot, pl.ds(0, 4)],
            src_send.at[step, slot], src_got.at[step, slot], device(0, 1),
        ).wait_recv()

    def early_forces(step):
        for b in (-1, 1):
            arrived(step, 0, b)
        force_pass(own, force, [source(step, 0, b) for b in (0, -1, 1)], True)
        for b in (-1, 0, 1):
            arrived(step, quick, b)
        force_pass(own, force, [source(step, quick, b) for b in (-1, 0, 1)], False)

    def late_arrivals(step):
        for b in (-1, 0, 1):
            arrived(step, slow, b)

    def late_forces(step):
        force_pass(own, force, [source(step, slow, b) for b in (-1, 0, 1)], False, True)
        return force_rows(force)

    own_columns(own, src[0, OWN])
    early_forces(0)
    late_arrivals(0)
    for copy in edges + halo:
        copy.wait_recv()
    push = late_forces(0)

    total[...] = sums[...]
    total[0] += halo_x[0]
    total[n_x] += halo_x[1]
    for i in range(n_x + 1):
        total[i, at_low, :] += halo_y[0, i, at_low, :]
        total[i, at_high, :] += halo_y[1, i, at_low, :]
    total[0, at_low, :] += halo_c[0, at_low, :]
    total[0, at_high, :] += halo_c[1, at_low, :]
    total[n_x, at_low, :] += halo_c[2, at_low, :]
    total[n_x, at_high, :] += halo_c[3, at_low, :]

    chosen = (iota((width_z, slots), 0) == layer_z).astype(f32).astype(bf16)
    block = total[...].reshape((n_x + 1) * tiles_y * 8, width_z)
    at_z = sum(dot(term, chosen) for term in terms(block, 2)[::-1])
    picked = jnp.zeros((8, slots), f32)
    for i in range(n_x + 1):
        for t in range(tiles_y):
            n = 8 * (i * tiles_y + t)
            picked = picked + jnp.where(in_tile(i, t), at_z[n : n + 8], 0.0)
    picked = picked + pltpu.roll(picked, 4, 0)
    numbers = jnp.concatenate(
        [index[...].reshape(n_x * n_y, width_z), edge_x[...], edge_y[...], edge_c[...]], axis=0
    )
    at_z = dot(numbers.astype(bf16), chosen)
    wanted = [place - comp == i * (n_y + 1) for i in range(n_x + 1)]
    wanted.append(place - comp * (n_y + 1) == n_y)
    wanted.append(jnp.logical_and(comp == 0, place == n_x * (n_y + 1) + n_y))
    found = jnp.zeros((8, slots), f32)
    for n, mask in enumerate(wanted):
        found = found + jnp.where(mask, at_z[8 * n : 8 * n + 8], 0.0)
    name = jnp.sum(found, axis=0, keepdims=True).astype(jnp.int32)
    heavy = jnp.maximum(picked[3:4], fill_mass)
    mean = [picked[c : c + 1] / heavy for c in range(3)]
    n = []
    for c in range(3):
        hit = [
            jnp.where(iota((8, slots), 0) + 8 * r == name, table[c, pl.ds(8 * r, 8), :], 0.0)
            for r in range(DIRECTIONS // 8)
        ]
        n.append(jnp.sum(sum(hit), axis=0, keepdims=True))
    rel = [vel[c, 0] - mean[c] for c in range(3)]
    cross = [n[1] * rel[2] - n[2] * rel[1], n[2] * rel[0] - n[0] * rel[2], n[0] * rel[1] - n[1] * rel[0]]
    along = n[0] * rel[0] + n[1] * rel[1] + n[2] * rel[2]
    speed = stacked([
        mean[c] + cos_angle * rel[c] + sin_angle * cross[c] + (1.0 - cos_angle) * along * n[c]
        for c in range(3)
    ])
    place_now = start

    def cell_fields(i, rows_of):
        for b in range(n_y):
            pair = [
                [jnp.where(later, total[i, pl.ds(4 * (b + 1) + c, 1), :], total[i, pl.ds(4 * b + c, 1), :])
                 for c in range(4)],
                [jnp.where(later, normals[c, pl.ds(rows_of(b + 1), 1), :], normals[c, pl.ds(rows_of(b), 1), :])
                 for c in range(3)],
            ]
            scale = 1.0 / jnp.maximum(pair[0][3], fill_mass)
            for c in range(3):
                fields[i, b, c] = pair[0][c] * scale
                fields[i, b, 3 + c] = pair[1][c]

    def turn(x, carry):
        at_cell = (x + shift_x) >> 2
        for b in range(n_y):
            at = pl.ds(8 * b, 8)
            mean = [fields[at_cell, b, c] for c in range(3)]
            n = [fields[at_cell, b, 3 + c] for c in range(3)]
            old = [out[c, x, at, :] for c in range(3)]
            rel = [old[c] - mean[c] for c in range(3)]
            along = (1.0 - cos_angle) * (n[0] * rel[0] + n[1] * rel[1] + n[2] * rel[2])
            cross = [
                n[1] * rel[2] - n[2] * rel[1],
                n[2] * rel[0] - n[0] * rel[2],
                n[0] * rel[1] - n[1] * rel[0],
            ]
            live = held[x, at, :] > odd
            for c in range(3):
                new = mean[c] + cos_angle * rel[c] + sin_angle * cross[c] + along * n[c]
                out[c, x, at, :] = jnp.where(live, new, old[c])
        return carry

    def idle_work(step):
        if step == 1:
            for c, part in enumerate(axes_of(numbers)):
                normals[c] = part

            def inner(i, carry):
                cell_fields(i, lambda b: i * n_y + b if b < n_y else n_x * n_y + 8 + i)
                return carry

            lax.fori_loop(0, n_x, inner, 0)
            cell_fields(n_x, lambda b: n_x * n_y + b if b < n_y else n_x * n_y + 16)
            lax.fori_loop(0, width_x // 2, turn, 0)
        if step == 2:
            lax.fori_loop(width_x // 2, width_x, turn, 0)

    speed = speed + push * kick
    place_now = place_now + timestep * speed
    src[1, OWN] = place_now * (1.0 / cutoff)
    sends = sends + exchange(1)
    own_columns(own, src[1, OWN])
    idle_work(1)
    early_forces(1)
    late_arrivals(1)
    push = late_forces(1)

    speed = speed + push * kick
    place_now = place_now + timestep * speed
    def at_wide(a, b):
        return wide_slot(a, b, size_y)

    mine = at_wide(0, 0)
    wide[mine] = place_now * (1.0 / cutoff)
    spread = {}
    for a, b in around:
        k, target = (at_wide(a, b), at_wide(-a, -b))
        spread[a, b] = remote(
            wide.at[mine, pl.ds(0, 4)], wide.at[target, pl.ds(0, 4)],
            wide_send.at[k], wide_got.at[target], device(a, b),
        )
        spread[a, b].start()

    def wide_arrived(a):
        for b in (-1, 0, 1, -2, 2):
            if (isinstance(a, int) and b == 0) or folded(b, size_y) != b:
                continue
            k = at_wide(a, b)
            remote(
                wide.at[mine, pl.ds(0, 4)], wide.at[k, pl.ds(0, 4)],
                wide_send.at[k], wide_got.at[k], device(0, 1),
            ).wait_recv()

    idle_work(2)
    first[...] = src[0]
    second[...] = src[1]
    tiles[0] = place_now
    tiles[1] = speed
    tiles[2] = stacked([pos[c, 0] for c in range(3)])
    tiles[3] = stacked([vel[c, 0] for c in range(3)])
    tiles[4] = jnp.broadcast_to(jnp.where(alive, 1.0, 0.0), (8, slots))
    for k, a in enumerate(columns_x[:2]):
        wide_arrived(a)
        block = flipped([wide[at_wide(a, b)] for b in (-1, 0, 1)])
        for m in range(3):
            for c in range(3):
                column = block[:, 8 * m + c : 8 * m + c + 1]
                early[3 * k + m, c] = jnp.broadcast_to(column, (slots, slots))
        for m in range(3):
            around_m = [reader(wide, at_wide(a, m - 1 + q), a, q, steps) for q in (-1, 0, 1)]
            force_pass(early.at[m], begun.at[m], around_m, k == 0)
    wide_arrived(slow)
    for a in (-2 * quick, 2 * quick):
        wide_arrived(a)
    third[...] = wide[...]
    for copy in sends + halo + edges + list(spread.values()):
        copy.wait_send()


def finish_kernel(
    shape, turned, first, second, third, tiles, early, begun,
    out, pos_out, vel_out, own, force, later, sums, placed, packed, counts, sem
):
    width_x, width_y, width_z = shape
    n_x, n_y = (width_x // SUB, width_y // SUB)
    slots = first.shape[2]
    size_y = lax.axis_size("yz")
    columns_x = sides(lax.axis_index("gx"))
    copies = []
    for c in range(3):
        copies.append(pltpu.make_async_copy(turned.at[c], out.at[c], sem.at[c]))
        copies[-1].start()

    steps = ((width_z // 2) / cutoff, n_x / cutoff, n_y / cutoff)
    block = 16 if slots % 16 == 0 else 8
    half = slots // 2
    group = [(k, b) for k in range(3) for b in (-1, 0, 1)]

    def at_wide(k, b, p=0):
        return wide_slot(columns_x[k] + p, b, size_y)

    def halves(most, work):
        work(0)
        pl.when(most * block > half)(lambda: work(half))

    def columns(tiles, most):
        sums[...] = flipped(tiles)

        def work(start):
            at = pl.ds(start, half)
            for n in range(len(tiles)):
                for c in range(3):
                    column = sums[at, 8 * n + c : 8 * n + c + 1]
                    own[n, c, at, :] = jnp.broadcast_to(column, (half, slots))

        halves(most, work)

    def pushes(m, columns_of, trips, sources, before=None, moved=None):
        def body(r, carry):
            at = pl.ds(pl.multiple_of(r * block, block), block)
            rows = [columns_of[c, at, :] for c in range(3)]
            if moved is not None:
                rows = [rows[0] + moved[0], rows[1] + moved[1], rows[2]]
            total = None if before is None else [before[c, at, :] for c in range(3)]
            for source in sources:
                parts = pair_sums(rows, source())
                total = parts if total is None else [t + p for t, p in zip(total, parts)]
            for c in range(3):
                force[m, c, at, :] = total[c]
            return carry

        lax.fori_loop(0, trips, body, 0)

    def rows_of(number, most):
        lane = iota((half, slots), 1)

        def work(start):
            at = pl.ds(start, half)
            block = jnp.zeros((half, slots), f32)
            for n in range(number):
                for c in range(3):
                    total = jnp.sum(force[n, c, at, :], axis=1, keepdims=True)
                    block = jnp.where(lane == 8 * n + c, total, block)
            sums[at, :] = block

        halves(most, work)
        return sums[...].T

    comp = iota((8, slots), 0)
    for a in range(-2, 3):
        for b in range(-2, 3):
            tile = third[wide_slot(a, b, size_y)]
            offset = jnp.where(comp == 0, a * steps[1], jnp.where(comp == 1, b * steps[2], 0.0))
            placed[(a + 2) * 5 + b + 2] = tile + offset
            live = jnp.where(tile[:1] > 0.1 * far_away, 0.0, 1.0)
            counts[(a + 2) * 5 + b + 2] = jnp.sum(live).astype(jnp.int32)

    def at_placed(k, b, p=0):
        return (columns_x[k] + p + 2) * 5 + b + 2

    dead = [third[at_wide(k, b), pl.ds(0, 1), :] > 0.1 * far_away for k, b in group]
    trips = [(counts[at_placed(k, b)] + (block - 1)) // block for k, b in group]
    lane_of = iota((8, slots), 1)

    def pack(n, k, b):
        at = [at_placed(k, b + q, p) for p, q in RING]
        held = [counts[t] for t in at]
        best, which, single = (held[0], 0, at[0])
        for t in range(1, 9):
            larger = held[t] > best
            best = jnp.where(larger, held[t], best)
            which = jnp.where(larger, t, which)
            single = jnp.where(larger, at[t], single)
        for t in range(8):
            held[t] = jnp.where(which == t, held[8], held[t])
            at[t] = jnp.where(which == t, at[8], at[t])
        fits = None
        for t in range(4):
            size = held[2 * t]
            both = jnp.where(
                lane_of < size, placed[at[2 * t]], pltpu.roll(placed[at[2 * t + 1]], size, 1)
            )
            packed[4 * n + t] = both
            fit = size + held[2 * t + 1] <= slots
            fits = fit if fits is None else jnp.logical_and(fits, fit)
        return fits, single

    packs = [pack(n, k, b) for n, (k, b) in enumerate(group[3:])]
    most = functools.reduce(jnp.maximum, trips)
    columns([third[at_wide(2, b)] for b in (-1, 0, 1)], most)
    for m, (k, b) in enumerate(group):
        if k == 0:
            slow = columns_x[2]
            around_m = [reader(third, at_wide(2, b + q), slow, q, steps) for q in (-1, 0, 1)]
            pushes(m, early.at[m], trips[m], around_m, begun.at[m])
        else:
            around_m = [
                reader(third, at_wide(k, b + q, p), p, q, steps) for p in (-1, 0, 1) for q in (-1, 0, 1)
            ]
            own_m = early.at[m] if k == 1 else own.at[m - 6]
            fits, single = packs[m - 3]
            tight = [reader(packed, 4 * (m - 3) + t, 0, 0, steps) for t in range(4)]
            tight.append(reader(placed, single, 0, 0, steps))
            moved = (columns_x[k].astype(f32) * steps[1], b * steps[2])
            pushes(m, own_m, jnp.where(fits, trips[m], 0), tight, None, moved)
            pushes(m, own_m, jnp.where(fits, 0, trips[m]), around_m)
    push = rows_of(len(group), most)
    speed, place = (tiles[1], tiles[0])
    for m, (k, b) in enumerate(group):
        near = slot_of(columns_x[k], b)
        now = third[at_wide(k, b)]
        mine = push[8 * m : 8 * m + 8]
        kick = jnp.broadcast_to(first[near, pl.ds(3, 1), :], (8, slots))
        if (k, b) == (0, 0):
            speed = speed + mine * kick
            place = place + timestep * speed
            moved = place * (1.0 / cutoff)
            own_kick, own_trips = (kick, trips[m])
        else:
            moved = now + (now - second[near]) + (timestep / cutoff) * (mine * kick)
        later[m] = jnp.where(jnp.broadcast_to(dead[m], (8, slots)), now, moved)
    columns([later[1]], own_trips)
    around_m = [reader(later, m, columns_x[k], b, steps) for m, (k, b) in enumerate(group)]
    pushes(0, own.at[0], own_trips, around_m)
    speed = speed + rows_of(1, own_trips)[:8] * own_kick
    place = place + timestep * speed
    alive = tiles[4] > 0
    place = jnp.where(alive, place, tiles[2])
    speed = jnp.where(alive, speed, tiles[3])
    for c in range(3):
        pos_out[c, 0] = place[c : c + 1]
        vel_out[c, 0] = speed[c : c + 1]
    for copy in copies:
        copy.wait()


def per_device(
    solvent_vel, occupancy, grid_shift, axis_index, colloid_pos, colloid_vel, colloid_mass, colloid_count
):
    shape = occupancy.shape
    width_x, width_y, width_z = shape
    rows = 2 * width_y
    n_x, n_y = (width_x // SUB, width_y // SUB)
    slots = colloid_mass.shape[2]
    solvent = solvent_vel.reshape(3, width_x, rows, width_z)
    smem = pl.BlockSpec(memory_space=pltpu.SMEM)
    vmem = pl.BlockSpec(memory_space=pltpu.VMEM)
    hbm = pl.BlockSpec(memory_space=pltpu.HBM)
    tall = (n_y + 2) // 2 * 8
    dma = pltpu.SemaphoreType.DMA

    def in_hbm(x):
        return pltpu.with_memory_space_constraint(x, pltpu.HBM)

    turned, *states = pl.pallas_call(
        functools.partial(collide_kernel, shape),
        out_shape=[
            pltpu.VMEM(solvent.shape, f32),
            pltpu.VMEM((9, 8, slots), f32),
            pltpu.VMEM((9, 8, slots), f32),
            pltpu.VMEM((25, 8, slots), f32),
            pltpu.VMEM((5, 8, slots), f32),
            pltpu.VMEM((6, 3, slots, slots), f32),
            pltpu.VMEM((3, 3, slots, slots), f32),
        ],
        in_specs=[hbm, smem] + [hbm] * 6,
        out_specs=[vmem] * 7,
        scratch_shapes=[
            pltpu.SMEM(grid_shift.shape, jnp.int32),
            pltpu.VMEM(colloid_pos.shape, f32),
            pltpu.VMEM(colloid_vel.shape, f32),
            pltpu.VMEM(colloid_mass.shape, f32),
            pltpu.VMEM(axis_index.shape, jnp.int32),
            pltpu.VMEM(shape, jnp.int32),
            pltpu.VMEM((width_x, rows, width_z), f32),
            pltpu.VMEM((n_x + 1, 4, rows, width_z), f32),
            pltpu.VMEM((n_x + 1, tall, width_z), f32),
            pltpu.VMEM((n_x + 1, tall, width_z), f32),
            pltpu.VMEM((n_x, n_y, width_z), f32),
            pltpu.VMEM((8, width_z), f32),
            pltpu.VMEM((8, width_z), f32),
            pltpu.VMEM((8, width_z), f32),
            pltpu.VMEM((3, n_x * n_y + 24, width_z), f32),
            pltpu.VMEM((n_x + 1, n_y, 6, 8, width_z), f32),
            pltpu.VMEM((2, tall, width_z), f32),
            pltpu.VMEM((2, n_x + 1, 8, width_z), f32),
            pltpu.VMEM((4, 8, width_z), f32),
            pltpu.VMEM((2, 9, 8, slots), f32),
            pltpu.VMEM((25, 8, slots), f32),
            pltpu.VMEM((3, slots, slots), f32),
            pltpu.VMEM((3, slots, slots), f32),
            pltpu.VMEM((3, DIRECTIONS, slots), f32),
            dma((6,)),
            dma((n_x,)),
            dma((8,)),
            dma((8,)),
            dma((3,)),
            dma((3,)),
            dma((2, 9)),
            dma((2, 9)),
            dma((25,)),
            dma((25,)),
        ],
        compiler_params=pltpu.CompilerParams(
            collective_id=0, has_side_effects=True, vmem_limit_bytes=32 * 2**20
        ),
        name="collide",
    )(
        in_hbm(grid_shift), colloid_count, in_hbm(solvent), in_hbm(occupancy), in_hbm(axis_index),
        in_hbm(colloid_pos), in_hbm(colloid_vel), in_hbm(colloid_mass),
    )

    solvent_out, pos_out, vel_out = pl.pallas_call(
        functools.partial(finish_kernel, shape),
        out_shape=[
            jax.ShapeDtypeStruct(solvent.shape, f32),
            jax.ShapeDtypeStruct(colloid_pos.shape, f32),
            jax.ShapeDtypeStruct(colloid_vel.shape, f32),
        ],
        in_specs=[vmem] * 7,
        out_specs=[hbm, vmem, vmem],
        scratch_shapes=[
            pltpu.VMEM((3, 3, slots, slots), f32),
            pltpu.VMEM((9, 3, slots, slots), f32),
            pltpu.VMEM((9, 8, slots), f32),
            pltpu.VMEM((slots, slots), f32),
            pltpu.VMEM((25, 8, slots), f32),
            pltpu.VMEM((24, 8, slots), f32),
            pltpu.SMEM((25,), jnp.int32),
            dma((3,)),
        ],
        compiler_params=pltpu.CompilerParams(vmem_limit_bytes=16 * 2**20),
        name="finish",
    )(turned, *states)
    return (solvent_out.reshape(solvent_vel.shape), pos_out, vel_out)


def solution(mesh):
    return jax.shard_map(
        per_device,
        mesh=mesh,
        in_specs=(
            P(None, "gx", "yz", None, None),
            P("gx", "yz", None),
            P(),
            P("gx", "yz", None),
            P(None, "gx", "yz", None),
            P(None, "gx", "yz", None),
            P("gx", "yz", None),
            P("gx", "yz"),
        ),
        out_specs=(
            P(None, "gx", "yz", None, None),
            P(None, "gx", "yz", None),
            P(None, "gx", "yz", None),
        ),
        check_vma=False,
    )
```

```python
import functools
import math

import jax
import jax.numpy as jnp
from jax import lax
from jax.experimental import pallas as pl
from jax.experimental.pallas import tpu as pltpu
from jax.sharding import PartitionSpec as P

SUB = 4
SUBSTEPS = 4
DIRECTIONS = 64

turn_angle = 130.0 * math.pi / 180.0
cos_angle = math.cos(turn_angle)
sin_angle = math.sin(turn_angle)
golden = math.pi * (3.0 - math.sqrt(5.0))
cutoff = 1.5
stiffness = 20.0
timestep = 0.05
fill_mass = 16.0
far_away = 1.0e9
MESH = pl.DeviceIdType.MESH
f32 = jnp.float32
bf16 = jnp.bfloat16
RING = [(a, b) for a in (-1, 0, 1) for b in (-1, 0, 1)]
AROUND = [pair for pair in RING if pair != (0, 0)]
OWN = 4


def iota(shape, dim):
    return lax.broadcasted_iota(jnp.int32, shape, dim)


def slot_of(a, b):
    return (a + 1) * 3 + b + 1


def folded(b, size_y):
    return 2 if b == -2 and size_y == 4 else b


def wide_slot(a, b, size_y):
    return (a + 2) * 5 + folded(b, size_y) + 2


def wide_pairs(size_y):
    return [
        (a, b) for a in (-1, 1, -2, 2, 0) for b in (-1, 0, 1, -2, 2)
        if (a, b) != (0, 0) and folded(b, size_y) == b
    ]


def sides(me_x):
    quick = 1 - 2 * (me_x & 1)
    return (0, quick, -quick)


def reader(ref, slot, p, q, steps):
    period, step_x, step_y = steps

    def read():
        x, y, z = [ref[slot, pl.ds(c, 1), :] for c in range(3)]
        if not isinstance(p, int):
            x = x + p.astype(f32) * step_x
        elif p != 0:
            x = x + p * step_x
        return (x, y if q == 0 else y + q * step_y, z, period)

    return read


def terms(value, number):
    out = []
    for _ in range(number - 1):
        part = value.astype(bf16)
        out.append(part)
        value = value - part.astype(f32)
    return out + [value.astype(bf16)]


def dot(left, right, contract=((1,), (0,))):
    return lax.dot_general(left, right, (contract, ((), ())), preferred_element_type=f32)


def wrapped(value, size):
    return jnp.where(value >= size, value - size, value)


def layer_of(row, scale, width):
    return jnp.clip(jnp.floor(row * scale).astype(jnp.int32), 0, width - 1)


def fold(values):
    row = iota(values[0].shape, 0)
    low = row < 4
    values = [
        jnp.where(low, a, b) + pltpu.roll(jnp.where(low, b, a), 4, 0)
        for a, b in zip(values[:4], values[4:])
    ]
    for dist in (2, 1):
        low = (row & dist) == 0
        values = [
            jnp.where(low, a, b) + jnp.where(low, pltpu.roll(a, 8 - dist, 0), pltpu.roll(b, dist, 0))
            for a, b in zip(values[:dist], values[dist:])
        ]
    return values[0]


def stacked(rows):
    comp = iota((8, rows[0].shape[1]), 0)
    out = jnp.zeros((8, rows[0].shape[1]), f32)
    for c, row in enumerate(rows):
        out = jnp.where(comp == c, row, out)
    return out


def axes_of(number):
    height = 1.0 - (2.0 * number + 1.0) / DIRECTIONS
    radius = jnp.sqrt(1.0 - height * height)
    phase = number * golden
    return [radius * jnp.cos(phase), radius * jnp.sin(phase), height]


def pair_sums(own_rows, source):
    dx, dy, dz = [o - s for o, s in zip(own_rows, source[:3])]
    period = source[3]
    half = 0.5 * period
    dz = dz + jnp.where(dz > half, -period, jnp.where(dz < -half, period, 0.0))
    reach = jnp.maximum(1.0 - (dx * dx + dy * dy + dz * dz), 0.0)
    weight = reach * reach
    return [weight * dx, weight * dy, weight * dz]


def force_pass(own, force, sources, first, straight=False):
    slots = own.shape[-1]
    wide = 32 if slots % 32 == 0 else 8

    def block(r, carry):
        at = pl.ds(r * wide if straight else pl.multiple_of(r * wide, wide), wide)
        rows = [own[c, at, :] for c in range(3)]
        total = None if first else [force[c, at, :] for c in range(3)]
        for source in sources:
            parts = pair_sums(rows, source())
            total = parts if total is None else [t + p for t, p in zip(total, parts)]
        for c in range(3):
            force[c, at, :] = total[c]
        return carry

    if straight:
        for r in range(slots // wide):
            block(r, 0)
    else:
        lax.fori_loop(0, slots // wide, block, 0)


def force_rows(force):
    slots = force.shape[1]
    comp = iota((8, slots), 0)
    out = None
    for c in range(3):
        pick = (comp == c).astype(f32).astype(bf16)
        for term in terms(force[c], 2)[::-1]:
            part = dot(pick, term, ((1,), (1,)))
            out = part if out is None else out + part
    return out


def flipped(tiles):
    slots = tiles[0].shape[1]
    pad = jnp.zeros((slots - 8 * len(tiles), slots), f32)
    return jnp.concatenate(tiles + [pad], axis=0).T


def own_columns(own, tile):
    slots = tile.shape[1]
    block = flipped([tile])
    for c in range(3):
        own[c] = jnp.broadcast_to(block[:, c : c + 1], (slots, slots))


def collide_kernel(
    shape, shift_hbm, count, solvent_hbm, occupancy_hbm, axis_hbm, pos_hbm, vel_hbm, mass_hbm,
    out, first, second, third, tiles, early, begun,
    shift, pos, vel, mass, axis, occupancy, held, cell, sums, total, index, edge_x, edge_y, edge_c,
    normals, fields, halo_x, halo_y, halo_c, src, wide, force, own, table,
    small_sem, chunk_sem, halo_send, halo_got, edge_send, edge_got, src_send, src_got,
    wide_send, wide_got,
):
    width_x, width_y, width_z = shape
    n_x, n_y = (width_x // SUB, width_y // SUB)
    rows = 2 * width_y
    slots = mass.shape[2]
    me_x, me_y = (lax.axis_index("gx"), lax.axis_index("yz"))
    size_x, size_y = (lax.axis_size("gx"), lax.axis_size("yz"))

    def device(a, b):
        return (lax.rem(me_x + a + size_x, size_x), lax.rem(me_y + b + size_y, size_y))

    def remote(source, target, send, receive, where):
        return pltpu.make_async_remote_copy(
            src_ref=source, dst_ref=target, send_sem=send, recv_sem=receive,
            device_id=where, device_id_type=MESH,
        )

    around = wide_pairs(size_y)
    edge_c[...] = jnp.zeros_like(edge_c)
    small = [
        pltpu.make_async_copy(source, target, small_sem.at[k])
        for k, (source, target) in enumerate(
            [
                (shift_hbm, shift), (pos_hbm, pos), (vel_hbm, vel),
                (mass_hbm, mass), (axis_hbm, axis), (occupancy_hbm, occupancy),
            ]
        )
    ]
    chunks = [
        pltpu.make_async_copy(
            solvent_hbm.at[:, pl.ds(i * SUB, SUB)], out.at[:, pl.ds(i * SUB, SUB)], chunk_sem.at[i]
        )
        for i in range(n_x)
    ]
    barrier = pltpu.get_barrier_semaphore()

    def greet(pairs):
        for a, b in pairs:
            pl.semaphore_signal(barrier, inc=1, device_id=device(a, b), device_id_type=MESH)

    for copy in small:
        copy.start()
    greet(around[:6])
    for copy in chunks:
        copy.start()
    greet(around[6:])
    for copy in small[:-1]:
        copy.wait()
    shift_x, shift_y, shift_z = (shift[0], shift[1], shift[2])

    alive = iota((1, slots), 1) < count[0, 0]
    cell_x = (layer_of(pos[0, 0], SUB, width_x) + shift_x) >> 2
    cell_y = (layer_of(pos[1, 0], SUB, width_y) + shift_y) >> 2
    layer_z = layer_of(pos[2, 0], 2.0, width_z)
    cell_z = wrapped(layer_z + shift_z, width_z) >> 1
    place = cell_x * (n_y + 1) + cell_y
    weight = jnp.where(alive, mass[0], 0.0)
    comp = iota((8, slots), 0)
    four = comp & 3
    values = jnp.where(
        four == 0, vel[0, 0] * weight,
        jnp.where(four == 1, vel[1, 0] * weight, jnp.where(four == 2, vel[2, 0] * weight, weight)),
    )
    place_half = place - (comp >> 2)
    place_last = jnp.where(comp < 4, place, -1)
    tiles_y = (n_y + 2) // 2

    def in_tile(i, t):
        return (place_half if 2 * t < n_y else place_last) == i * (n_y + 1) + 2 * t

    spread = [
        jnp.where(in_tile(i, t), values, 0.0) for i in range(n_x + 1) for t in range(tiles_y)
    ]
    near = (wrapped(iota((width_z, slots), 0) + shift_z, width_z) >> 1) == cell_z
    near = near.astype(f32).astype(bf16)
    deposit = sum(
        dot(term, near, ((1,), (1,))) for term in terms(jnp.concatenate(spread, axis=0), 3)[::-1]
    )
    sums[...] = deposit.reshape(n_x + 1, tiles_y * 8, width_z)

    cell_row = wrapped(iota((width_z // 2, width_z), 1) + shift_z, width_z) >> 1
    expand = (cell_row == iota((width_z // 2, width_z), 0)).astype(f32).astype(bf16)
    number = axis[...].reshape(n_x * n_y, width_z // 2).astype(f32).astype(bf16)
    index[...] = dot(number, expand).reshape(n_x, n_y, width_z)

    for c, part in enumerate(axes_of(iota((DIRECTIONS, slots), 0).astype(f32))):
        table[c] = part
    start = stacked([jnp.where(alive, pos[0, 0], far_away), pos[1, 0], pos[2, 0]])
    kick = jnp.broadcast_to((timestep * stiffness * cutoff) / mass[0], (8, slots))
    src[0, OWN] = jnp.where(comp == 3, kick, start * (1.0 / cutoff))

    double = (iota((SUB * rows, SUB * width_y), 0) >> 1 == iota((SUB * rows, SUB * width_y), 1)).astype(bf16)
    small[-1].wait()
    for i in range(n_x):
        at = pl.ds(i * SUB, SUB)
        filled = occupancy[at].reshape(SUB * width_y, width_z).astype(f32).astype(bf16)
        held[at] = dot(double, filled).reshape(SUB, rows, width_z)
    row = iota((8, width_z), 0)
    odd = (row & 1).astype(f32)
    stays_1 = jnp.broadcast_to(shift_x, (8, width_z)) <= 2
    stays_2 = jnp.broadcast_to(shift_x, (8, width_z)) <= 1
    later = ((row >> 1) + shift_y) >= SUB
    even = ((iota((8, width_z), 1) + shift_z) & 1) == 0
    halves = jnp.where((row & 3) == 3, 0.5, 1.0)
    blank = jnp.zeros((8, width_z), f32)

    def finish(i):
        def straddling(c, j):
            now = cell[i, c, pl.ds(8 * j, 8), :] if j < n_y else blank
            before = cell[i, c, pl.ds(8 * (j - 1), 8), :] if j > 0 else blank
            return jnp.where(later, before, now)

        for t in range(tiles_y):
            blocks = [
                straddling(q & 3, 2 * t + (q >> 2)) if 2 * t + (q >> 2) <= n_y else blank
                for q in range(8)
            ]
            tile = fold(blocks) * halves
            partner = jnp.where(even, pltpu.roll(tile, width_z - 1, 1), pltpu.roll(tile, 1, 1))
            sums[i, pl.ds(8 * t, 8), :] += tile + partner

    def gather(i):
        for b in range(n_y):
            at = pl.ds(8 * b, 8)
            filled = [held[i * SUB + r, at, :] for r in range(SUB)]
            live = [f > odd for f in filled]
            for c in range(4):
                v = filled
                if c < 3:
                    v = [jnp.where(live[r], out[c, i * SUB + r, at, :], 0.0) for r in range(SUB)]
                front = v[0] + v[1]
                back = v[3] + v[2]
                stay = jnp.where(stays_1, jnp.where(stays_2, front + v[2], front), v[0])
                move = jnp.where(stays_1, jnp.where(stays_2, v[3], back), back + v[1])
                cell[i, c, at, :] = stay if i == 0 else cell[i, c, at, :] + stay
                cell[i + 1, c, at, :] = move

    for i in range(n_x):
        chunks[i].wait()
        gather(i)
        if i > 0:
            finish(i - 1)
    finish(n_x - 1)
    finish(n_x)

    pl.semaphore_wait(barrier, len(around))

    def exchange(step):
        mine = src.at[step, OWN, pl.ds(0, 4)]
        copies = {}
        for a, b in AROUND:
            k = slot_of(a, b)
            copies[k] = remote(
                mine, src.at[step, 8 - k, pl.ds(0, 4)],
                src_send.at[step, k], src_got.at[step, 8 - k], device(a, b),
            )
            copies[k].start()
        return list(copies.values())

    sends = exchange(0)

    at_low, at_high = (pl.ds(0, 4), pl.ds(n_y * SUB, 4))
    every = pl.ds(0, n_x + 1)
    halo = [
        (sums.at[n_x], halo_x.at[0], (1, 0)),
        (sums.at[0], halo_x.at[1], (-1, 0)),
        (sums.at[every, at_high], halo_y.at[0, every, at_low], (0, 1)),
        (sums.at[every, at_low], halo_y.at[1, every, at_low], (0, -1)),
        (sums.at[n_x, at_high], halo_c.at[0, at_low], (1, 1)),
        (sums.at[n_x, at_low], halo_c.at[1, at_low], (1, -1)),
        (sums.at[0, at_high], halo_c.at[2, at_low], (-1, 1)),
        (sums.at[0, at_low], halo_c.at[3, at_low], (-1, -1)),
    ]
    halo = [
        remote(source, target, halo_send.at[k], halo_got.at[k], device(*where))
        for k, (source, target, where) in enumerate(halo)
    ]
    for copy in halo:
        copy.start()
    edges = [
        (index.at[0], edge_x, (-1, 0)),
        (index.at[pl.ds(0, n_x), 0], edge_y, (0, -1)),
        (index.at[0, pl.ds(0, 1)], edge_c.at[pl.ds(0, 1)], (-1, -1)),
    ]
    edges = [
        remote(source, target, edge_send.at[k], edge_got.at[k], device(*where))
        for k, (source, target, where) in enumerate(edges)
    ]
    for copy in edges:
        copy.start()

    steps = ((width_z // 2) / cutoff, n_x / cutoff, n_y / cutoff)
    columns_x = sides(me_x)
    quick, slow = columns_x[1:]

    def source(step, a, b):
        return reader(src.at[step], slot_of(a, b), a, b, steps)

    def arrived(step, a, b):
        slot = slot_of(a, b)
        remote(
            src.at[step, OWN, pl.ds(0, 4)], src.at[step, slot, pl.ds(0, 4)],
            src_send.at[step, slot], src_got.at[step, slot], device(0, 1),
        ).wait_recv()

    def early_forces(step):
        for b in (-1, 1):
            arrived(step, 0, b)
        force_pass(own, force, [source(step, 0, b) for b in (0, -1, 1)], True)
        for b in (-1, 0, 1):
            arrived(step, quick, b)
        force_pass(own, force, [source(step, quick, b) for b in (-1, 0, 1)], False)

    def late_arrivals(step):
        for b in (-1, 0, 1):
            arrived(step, slow, b)

    def late_forces(step):
        force_pass(own, force, [source(step, slow, b) for b in (-1, 0, 1)], False, True)
        return force_rows(force)

    own_columns(own, src[0, OWN])
    early_forces(0)
    late_arrivals(0)
    for copy in edges + halo:
        copy.wait_recv()
    push = late_forces(0)

    total[...] = sums[...]
    total[0] += halo_x[0]
    total[n_x] += halo_x[1]
    for i in range(n_x + 1):
        total[i, at_low, :] += halo_y[0, i, at_low, :]
        total[i, at_high, :] += halo_y[1, i, at_low, :]
    total[0, at_low, :] += halo_c[0, at_low, :]
    total[0, at_high, :] += halo_c[1, at_low, :]
    total[n_x, at_low, :] += halo_c[2, at_low, :]
    total[n_x, at_high, :] += halo_c[3, at_low, :]

    chosen = (iota((width_z, slots), 0) == layer_z).astype(f32).astype(bf16)
    block = total[...].reshape((n_x + 1) * tiles_y * 8, width_z)
    at_z = sum(dot(term, chosen) for term in terms(block, 2)[::-1])
    picked = jnp.zeros((8, slots), f32)
    for i in range(n_x + 1):
        for t in range(tiles_y):
            n = 8 * (i * tiles_y + t)
            picked = picked + jnp.where(in_tile(i, t), at_z[n : n + 8], 0.0)
    picked = picked + pltpu.roll(picked, 4, 0)
    numbers = jnp.concatenate(
        [index[...].reshape(n_x * n_y, width_z), edge_x[...], edge_y[...], edge_c[...]], axis=0
    )
    at_z = dot(numbers.astype(bf16), chosen)
    wanted = [place - comp == i * (n_y + 1) for i in range(n_x + 1)]
    wanted.append(place - comp * (n_y + 1) == n_y)
    wanted.append(jnp.logical_and(comp == 0, place == n_x * (n_y + 1) + n_y))
    found = jnp.zeros((8, slots), f32)
    for n, mask in enumerate(wanted):
        found = found + jnp.where(mask, at_z[8 * n : 8 * n + 8], 0.0)
    name = jnp.sum(found, axis=0, keepdims=True).astype(jnp.int32)
    heavy = jnp.maximum(picked[3:4], fill_mass)
    mean = [picked[c : c + 1] / heavy for c in range(3)]
    n = []
    for c in range(3):
        hit = [
            jnp.where(iota((8, slots), 0) + 8 * r == name, table[c, pl.ds(8 * r, 8), :], 0.0)
            for r in range(DIRECTIONS // 8)
        ]
        n.append(jnp.sum(sum(hit), axis=0, keepdims=True))
    rel = [vel[c, 0] - mean[c] for c in range(3)]
    cross = [n[1] * rel[2] - n[2] * rel[1], n[2] * rel[0] - n[0] * rel[2], n[0] * rel[1] - n[1] * rel[0]]
    along = n[0] * rel[0] + n[1] * rel[1] + n[2] * rel[2]
    speed = stacked([
        mean[c] + cos_angle * rel[c] + sin_angle * cross[c] + (1.0 - cos_angle) * along * n[c]
        for c in range(3)
    ])
    place_now = start

    def cell_fields(i, rows_of):
        for b in range(n_y):
            pair = [
                [jnp.where(later, total[i, pl.ds(4 * (b + 1) + c, 1), :], total[i, pl.ds(4 * b + c, 1), :])
                 for c in range(4)],
                [jnp.where(later, normals[c, pl.ds(rows_of(b + 1), 1), :], normals[c, pl.ds(rows_of(b), 1), :])
                 for c in range(3)],
            ]
            scale = 1.0 / jnp.maximum(pair[0][3], fill_mass)
            for c in range(3):
                fields[i, b, c] = pair[0][c] * scale
                fields[i, b, 3 + c] = pair[1][c]

    def turn(x, carry):
        at_cell = (x + shift_x) >> 2
        for b in range(n_y):
            at = pl.ds(8 * b, 8)
            mean = [fields[at_cell, b, c] for c in range(3)]
            n = [fields[at_cell, b, 3 + c] for c in range(3)]
            old = [out[c, x, at, :] for c in range(3)]
            rel = [old[c] - mean[c] for c in range(3)]
            along = (1.0 - cos_angle) * (n[0] * rel[0] + n[1] * rel[1] + n[2] * rel[2])
            cross = [
                n[1] * rel[2] - n[2] * rel[1],
                n[2] * rel[0] - n[0] * rel[2],
                n[0] * rel[1] - n[1] * rel[0],
            ]
            live = held[x, at, :] > odd
            for c in range(3):
                new = mean[c] + cos_angle * rel[c] + sin_angle * cross[c] + along * n[c]
                out[c, x, at, :] = jnp.where(live, new, old[c])
        return carry

    def idle_work(step):
        if step == 1:
            for c, part in enumerate(axes_of(numbers)):
                normals[c] = part

            def inner(i, carry):
                cell_fields(i, lambda b: i * n_y + b if b < n_y else n_x * n_y + 8 + i)
                return carry

            lax.fori_loop(0, n_x, inner, 0)
            cell_fields(n_x, lambda b: n_x * n_y + b if b < n_y else n_x * n_y + 16)
            lax.fori_loop(0, width_x // 2, turn, 0)
        if step == 2:
            lax.fori_loop(width_x // 2, width_x, turn, 0)

    speed = speed + push * kick
    place_now = place_now + timestep * speed
    src[1, OWN] = place_now * (1.0 / cutoff)
    sends = sends + exchange(1)
    own_columns(own, src[1, OWN])
    idle_work(1)
    early_forces(1)
    late_arrivals(1)
    push = late_forces(1)

    speed = speed + push * kick
    place_now = place_now + timestep * speed
    def at_wide(a, b):
        return wide_slot(a, b, size_y)

    mine = at_wide(0, 0)
    wide[mine] = place_now * (1.0 / cutoff)
    spread = {}
    for a, b in around:
        k, target = (at_wide(a, b), at_wide(-a, -b))
        spread[a, b] = remote(
            wide.at[mine, pl.ds(0, 4)], wide.at[target, pl.ds(0, 4)],
            wide_send.at[k], wide_got.at[target], device(a, b),
        )
        spread[a, b].start()

    def wide_arrived(a):
        for b in (-1, 0, 1, -2, 2):
            if (isinstance(a, int) and b == 0) or folded(b, size_y) != b:
                continue
            k = at_wide(a, b)
            remote(
                wide.at[mine, pl.ds(0, 4)], wide.at[k, pl.ds(0, 4)],
                wide_send.at[k], wide_got.at[k], device(0, 1),
            ).wait_recv()

    idle_work(2)
    first[...] = src[0]
    second[...] = src[1]
    tiles[0] = place_now
    tiles[1] = speed
    tiles[2] = stacked([pos[c, 0] for c in range(3)])
    tiles[3] = stacked([vel[c, 0] for c in range(3)])
    tiles[4] = jnp.broadcast_to(jnp.where(alive, 1.0, 0.0), (8, slots))
    for copy in sends + halo + edges:
        copy.wait_send()
    for k, a in enumerate(columns_x[:2]):
        wide_arrived(a)
        block = flipped([wide[at_wide(a, b)] for b in (-1, 0, 1)])
        for m in range(3):
            for c in range(3):
                column = block[:, 8 * m + c : 8 * m + c + 1]
                early[3 * k + m, c] = jnp.broadcast_to(column, (slots, slots))
        for m in range(3):
            around_m = [reader(wide, at_wide(a, m - 1 + q), a, q, steps) for q in (-1, 0, 1)]
            force_pass(early.at[m], begun.at[m], around_m, k == 0)
    wide_arrived(slow)
    for a in (-2 * quick, 2 * quick):
        wide_arrived(a)
    third[...] = wide[...]
    for copy in spread.values():
        copy.wait_send()


def finish_kernel(
    shape, turned, first, second, third, tiles, early, begun,
    out, pos_out, vel_out, own, force, later, sums, placed, packed, counts, sem
):
    width_x, width_y, width_z = shape
    n_x, n_y = (width_x // SUB, width_y // SUB)
    slots = first.shape[2]
    size_y = lax.axis_size("yz")
    columns_x = sides(lax.axis_index("gx"))
    copies = []
    for c in range(3):
        copies.append(pltpu.make_async_copy(turned.at[c], out.at[c], sem.at[c]))
        copies[-1].start()

    steps = ((width_z // 2) / cutoff, n_x / cutoff, n_y / cutoff)
    block = 16 if slots % 16 == 0 else 8
    half = slots // 2
    group = [(k, b) for k in range(3) for b in (-1, 0, 1)]

    def at_wide(k, b, p=0):
        return wide_slot(columns_x[k] + p, b, size_y)

    def halves(most, work):
        work(0)
        pl.when(most * block > half)(lambda: work(half))

    def columns(tiles, most):
        sums[...] = flipped(tiles)

        def work(start):
            at = pl.ds(start, half)
            for n in range(len(tiles)):
                for c in range(3):
                    column = sums[at, 8 * n + c : 8 * n + c + 1]
                    own[n, c, at, :] = jnp.broadcast_to(column, (half, slots))

        halves(most, work)

    def pushes(m, columns_of, trips, sources, before=None, moved=None):
        def body(r, carry):
            at = pl.ds(pl.multiple_of(r * block, block), block)
            rows = [columns_of[c, at, :] for c in range(3)]
            if moved is not None:
                rows = [rows[0] + moved[0], rows[1] + moved[1], rows[2]]
            total = None if before is None else [before[c, at, :] for c in range(3)]
            for source in sources:
                parts = pair_sums(rows, source())
                total = parts if total is None else [t + p for t, p in zip(total, parts)]
            for c in range(3):
                force[m, c, at, :] = total[c]
            return carry

        lax.fori_loop(0, trips, body, 0)

    def rows_of(trips):
        lane = iota((half, slots), 1)

        def work(start, group, block):
            at = pl.ds(start, half)
            for n in group:
                for c in range(3):
                    total = jnp.sum(force[n, c, at, :], axis=1, keepdims=True)
                    block = jnp.where(lane == 8 * n + c, total, block)
            sums[at, :] = block

        work(0, range(len(trips)), jnp.zeros((half, slots), f32))
        for n, number in enumerate(trips):
            pl.when(number * block > half)(lambda n=n: work(half, [n], sums[pl.ds(half, half), :]))
        return sums[...].T

    comp = iota((8, slots), 0)
    for a in range(-2, 3):
        for b in range(-2, 3):
            tile = third[wide_slot(a, b, size_y)]
            offset = jnp.where(comp == 0, a * steps[1], jnp.where(comp == 1, b * steps[2], 0.0))
            placed[(a + 2) * 5 + b + 2] = tile + offset
            live = jnp.where(tile[:1] > 0.1 * far_away, 0.0, 1.0)
            counts[(a + 2) * 5 + b + 2] = jnp.sum(live).astype(jnp.int32)

    def at_placed(k, b, p=0):
        return (columns_x[k] + p + 2) * 5 + b + 2

    dead = [third[at_wide(k, b), pl.ds(0, 1), :] > 0.1 * far_away for k, b in group]
    trips = [(counts[at_placed(k, b)] + (block - 1)) // block for k, b in group]
    lane_of = iota((8, slots), 1)

    def pack(n, k, b):
        at = [at_placed(k, b + q, p) for p, q in RING]
        held = [counts[t] for t in at]
        best, which, single = (held[0], 0, at[0])
        for t in range(1, 9):
            larger = held[t] > best
            best = jnp.where(larger, held[t], best)
            which = jnp.where(larger, t, which)
            single = jnp.where(larger, at[t], single)
        for t in range(8):
            held[t] = jnp.where(which == t, held[8], held[t])
            at[t] = jnp.where(which == t, at[8], at[t])
        fits = None
        for t in range(4):
            size = held[2 * t]
            both = jnp.where(
                lane_of < size, placed[at[2 * t]], pltpu.roll(placed[at[2 * t + 1]], size, 1)
            )
            packed[4 * n + t] = both
            fit = size + held[2 * t + 1] <= slots
            fits = fit if fits is None else jnp.logical_and(fits, fit)
        return fits, single

    packs = [pack(n, k, b) for n, (k, b) in enumerate(group[3:])]
    most = functools.reduce(jnp.maximum, trips)
    columns([third[at_wide(2, b)] for b in (-1, 0, 1)], most)
    for m, (k, b) in enumerate(group):
        if k == 0:
            slow = columns_x[2]
            around_m = [reader(third, at_wide(2, b + q), slow, q, steps) for q in (-1, 0, 1)]
            pushes(m, early.at[m], trips[m], around_m, begun.at[m])
        else:
            around_m = [
                reader(third, at_wide(k, b + q, p), p, q, steps) for p in (-1, 0, 1) for q in (-1, 0, 1)
            ]
            own_m = early.at[m] if k == 1 else own.at[m - 6]
            fits, single = packs[m - 3]
            tight = [reader(packed, 4 * (m - 3) + t, 0, 0, steps) for t in range(4)]
            tight.append(reader(placed, single, 0, 0, steps))
            moved = (columns_x[k].astype(f32) * steps[1], b * steps[2])
            pushes(m, own_m, jnp.where(fits, trips[m], 0), tight, None, moved)
            pushes(m, own_m, jnp.where(fits, 0, trips[m]), around_m)
    push = rows_of(trips)
    speed, place = (tiles[1], tiles[0])
    for m, (k, b) in enumerate(group):
        near = slot_of(columns_x[k], b)
        now = third[at_wide(k, b)]
        mine = push[8 * m : 8 * m + 8]
        kick = jnp.broadcast_to(first[near, pl.ds(3, 1), :], (8, slots))
        if (k, b) == (0, 0):
            speed = speed + mine * kick
            place = place + timestep * speed
            moved = place * (1.0 / cutoff)
            own_kick, own_trips = (kick, trips[m])
        else:
            moved = now + (now - second[near]) + (timestep / cutoff) * (mine * kick)
        later[m] = jnp.where(jnp.broadcast_to(dead[m], (8, slots)), now, moved)
    columns([later[1]], own_trips)
    around_m = [reader(later, m, columns_x[k], b, steps) for m, (k, b) in enumerate(group)]
    pushes(0, own.at[0], own_trips, around_m)
    speed = speed + rows_of([own_trips])[:8] * own_kick
    place = place + timestep * speed
    alive = tiles[4] > 0
    place = jnp.where(alive, place, tiles[2])
    speed = jnp.where(alive, speed, tiles[3])
    for c in range(3):
        pos_out[c, 0] = place[c : c + 1]
        vel_out[c, 0] = speed[c : c + 1]
    for copy in copies:
        copy.wait()


def per_device(
    solvent_vel, occupancy, grid_shift, axis_index, colloid_pos, colloid_vel, colloid_mass, colloid_count
):
    shape = occupancy.shape
    width_x, width_y, width_z = shape
    rows = 2 * width_y
    n_x, n_y = (width_x // SUB, width_y // SUB)
    slots = colloid_mass.shape[2]
    solvent = solvent_vel.reshape(3, width_x, rows, width_z)
    smem = pl.BlockSpec(memory_space=pltpu.SMEM)
    vmem = pl.BlockSpec(memory_space=pltpu.VMEM)
    hbm = pl.BlockSpec(memory_space=pltpu.HBM)
    tall = (n_y + 2) // 2 * 8
    dma = pltpu.SemaphoreType.DMA

    def in_hbm(x):
        return pltpu.with_memory_space_constraint(x, pltpu.HBM)

    turned, *states = pl.pallas_call(
        functools.partial(collide_kernel, shape),
        out_shape=[
            pltpu.VMEM(solvent.shape, f32),
            pltpu.VMEM((9, 8, slots), f32),
            pltpu.VMEM((9, 8, slots), f32),
            pltpu.VMEM((25, 8, slots), f32),
            pltpu.VMEM((5, 8, slots), f32),
            pltpu.VMEM((6, 3, slots, slots), f32),
            pltpu.VMEM((3, 3, slots, slots), f32),
        ],
        in_specs=[hbm, smem] + [hbm] * 6,
        out_specs=[vmem] * 7,
        scratch_shapes=[
            pltpu.SMEM(grid_shift.shape, jnp.int32),
            pltpu.VMEM(colloid_pos.shape, f32),
            pltpu.VMEM(colloid_vel.shape, f32),
            pltpu.VMEM(colloid_mass.shape, f32),
            pltpu.VMEM(axis_index.shape, jnp.int32),
            pltpu.VMEM(shape, jnp.int32),
            pltpu.VMEM((width_x, rows, width_z), f32),
            pltpu.VMEM((n_x + 1, 4, rows, width_z), f32),
            pltpu.VMEM((n_x + 1, tall, width_z), f32),
            pltpu.VMEM((n_x + 1, tall, width_z), f32),
            pltpu.VMEM((n_x, n_y, width_z), f32),
            pltpu.VMEM((8, width_z), f32),
            pltpu.VMEM((8, width_z), f32),
            pltpu.VMEM((8, width_z), f32),
            pltpu.VMEM((3, n_x * n_y + 24, width_z), f32),
            pltpu.VMEM((n_x + 1, n_y, 6, 8, width_z), f32),
            pltpu.VMEM((2, tall, width_z), f32),
            pltpu.VMEM((2, n_x + 1, 8, width_z), f32),
            pltpu.VMEM((4, 8, width_z), f32),
            pltpu.VMEM((2, 9, 8, slots), f32),
            pltpu.VMEM((25, 8, slots), f32),
            pltpu.VMEM((3, slots, slots), f32),
            pltpu.VMEM((3, slots, slots), f32),
            pltpu.VMEM((3, DIRECTIONS, slots), f32),
            dma((6,)),
            dma((n_x,)),
            dma((8,)),
            dma((8,)),
            dma((3,)),
            dma((3,)),
            dma((2, 9)),
            dma((2, 9)),
            dma((25,)),
            dma((25,)),
        ],
        compiler_params=pltpu.CompilerParams(
            collective_id=0, has_side_effects=True, vmem_limit_bytes=32 * 2**20
        ),
        name="collide",
    )(
        in_hbm(grid_shift), colloid_count, in_hbm(solvent), in_hbm(occupancy), in_hbm(axis_index),
        in_hbm(colloid_pos), in_hbm(colloid_vel), in_hbm(colloid_mass),
    )

    solvent_out, pos_out, vel_out = pl.pallas_call(
        functools.partial(finish_kernel, shape),
        out_shape=[
            jax.ShapeDtypeStruct(solvent.shape, f32),
            jax.ShapeDtypeStruct(colloid_pos.shape, f32),
            jax.ShapeDtypeStruct(colloid_vel.shape, f32),
        ],
        in_specs=[vmem] * 7,
        out_specs=[hbm, vmem, vmem],
        scratch_shapes=[
            pltpu.VMEM((3, 3, slots, slots), f32),
            pltpu.VMEM((9, 3, slots, slots), f32),
            pltpu.VMEM((9, 8, slots), f32),
            pltpu.VMEM((slots, slots), f32),
            pltpu.VMEM((25, 8, slots), f32),
            pltpu.VMEM((24, 8, slots), f32),
            pltpu.SMEM((25,), jnp.int32),
            dma((3,)),
        ],
        compiler_params=pltpu.CompilerParams(vmem_limit_bytes=16 * 2**20),
        name="finish",
    )(turned, *states)
    return (solvent_out.reshape(solvent_vel.shape), pos_out, vel_out)


def solution(mesh):
    return jax.shard_map(
        per_device,
        mesh=mesh,
        in_specs=(
            P(None, "gx", "yz", None, None),
            P("gx", "yz", None),
            P(),
            P("gx", "yz", None),
            P(None, "gx", "yz", None),
            P(None, "gx", "yz", None),
            P("gx", "yz", None),
            P("gx", "yz"),
        ),
        out_specs=(
            P(None, "gx", "yz", None, None),
            P(None, "gx", "yz", None),
            P(None, "gx", "yz", None),
        ),
        check_vma=False,
    )
```

```python
import functools
import math

import jax
import jax.numpy as jnp
from jax import lax
from jax.experimental import pallas as pl
from jax.experimental.pallas import tpu as pltpu
from jax.sharding import PartitionSpec as P

SUB = 4
SUBSTEPS = 4
DIRECTIONS = 64

turn_angle = 130.0 * math.pi / 180.0
cos_angle = math.cos(turn_angle)
sin_angle = math.sin(turn_angle)
golden = math.pi * (3.0 - math.sqrt(5.0))
cutoff = 1.5
stiffness = 20.0
timestep = 0.05
fill_mass = 16.0
far_away = 1.0e9
MESH = pl.DeviceIdType.MESH
f32 = jnp.float32
bf16 = jnp.bfloat16
RING = [(a, b) for a in (-1, 0, 1) for b in (-1, 0, 1)]
AROUND = [pair for pair in RING if pair != (0, 0)]
OWN = 4


def iota(shape, dim):
    return lax.broadcasted_iota(jnp.int32, shape, dim)


def slot_of(a, b):
    return (a + 1) * 3 + b + 1


def folded(b, size_y):
    return 2 if b == -2 and size_y == 4 else b


def wide_slot(a, b, size_y):
    return (a + 2) * 5 + folded(b, size_y) + 2


def wide_pairs(size_y):
    return [
        (a, b) for a in (-1, 1, -2, 2, 0) for b in (2, -2, 0, -1, 1)
        if (a, b) != (0, 0) and folded(b, size_y) == b
    ]


def sides(me_x):
    quick = 1 - 2 * (me_x & 1)
    return (0, quick, -quick)


def reader(ref, slot, p, q, steps):
    period, step_x, step_y = steps

    def read():
        x, y, z = [ref[slot, pl.ds(c, 1), :] for c in range(3)]
        if not isinstance(p, int):
            x = x + p.astype(f32) * step_x
        elif p != 0:
            x = x + p * step_x
        return (x, y if q == 0 else y + q * step_y, z, period)

    return read


def terms(value, number):
    out = []
    for _ in range(number - 1):
        part = value.astype(bf16)
        out.append(part)
        value = value - part.astype(f32)
    return out + [value.astype(bf16)]


def dot(left, right, contract=((1,), (0,))):
    return lax.dot_general(left, right, (contract, ((), ())), preferred_element_type=f32)


def wrapped(value, size):
    return jnp.where(value >= size, value - size, value)


def layer_of(row, scale, width):
    return jnp.clip(jnp.floor(row * scale).astype(jnp.int32), 0, width - 1)


def fold(values):
    row = iota(values[0].shape, 0)
    low = row < 4
    values = [
        jnp.where(low, a, b) + pltpu.roll(jnp.where(low, b, a), 4, 0)
        for a, b in zip(values[:4], values[4:])
    ]
    for dist in (2, 1):
        low = (row & dist) == 0
        values = [
            jnp.where(low, a, b) + jnp.where(low, pltpu.roll(a, 8 - dist, 0), pltpu.roll(b, dist, 0))
            for a, b in zip(values[:dist], values[dist:])
        ]
    return values[0]


def stacked(rows):
    comp = iota((8, rows[0].shape[1]), 0)
    out = jnp.zeros((8, rows[0].shape[1]), f32)
    for c, row in enumerate(rows):
        out = jnp.where(comp == c, row, out)
    return out


def axes_of(number):
    height = 1.0 - (2.0 * number + 1.0) / DIRECTIONS
    radius = jnp.sqrt(1.0 - height * height)
    phase = number * golden
    return [radius * jnp.cos(phase), radius * jnp.sin(phase), height]


def pair_sums(own_rows, source):
    dx, dy, dz = [o - s for o, s in zip(own_rows, source[:3])]
    period = source[3]
    half = 0.5 * period
    dz = dz + jnp.where(dz > half, -period, jnp.where(dz < -half, period, 0.0))
    reach = jnp.maximum(1.0 - (dx * dx + dy * dy + dz * dz), 0.0)
    weight = reach * reach
    return [weight * dx, weight * dy, weight * dz]


def force_pass(own, force, sources, first, straight=False):
    slots = own.shape[-1]
    wide = 32 if slots % 32 == 0 else 8

    def block(r, carry):
        at = pl.ds(r * wide if straight else pl.multiple_of(r * wide, wide), wide)
        rows = [own[c, at, :] for c in range(3)]
        total = None if first else [force[c, at, :] for c in range(3)]
        for source in sources:
            parts = pair_sums(rows, source())
            total = parts if total is None else [t + p for t, p in zip(total, parts)]
        for c in range(3):
            force[c, at, :] = total[c]
        return carry

    if straight:
        for r in range(slots // wide):
            block(r, 0)
    else:
        lax.fori_loop(0, slots // wide, block, 0)


def force_rows(force):
    slots = force.shape[1]
    comp = iota((8, slots), 0)
    out = None
    for c in range(3):
        pick = (comp == c).astype(f32).astype(bf16)
        for term in terms(force[c], 2)[::-1]:
            part = dot(pick, term, ((1,), (1,)))
            out = part if out is None else out + part
    return out


def flipped(tiles):
    slots = tiles[0].shape[1]
    pad = jnp.zeros((slots - 8 * len(tiles), slots), f32)
    return jnp.concatenate(tiles + [pad], axis=0).T


def own_columns(own, tile):
    slots = tile.shape[1]
    block = flipped([tile])
    for c in range(3):
        own[c] = jnp.broadcast_to(block[:, c : c + 1], (slots, slots))


def collide_kernel(
    shape, shift_hbm, count, solvent_hbm, occupancy_hbm, axis_hbm, pos_hbm, vel_hbm, mass_hbm,
    out, first, second, third, tiles, early, begun,
    shift, pos, vel, mass, axis, occupancy, held, cell, sums, total, index, edge_x, edge_y, edge_c,
    normals, fields, halo_x, halo_y, halo_c, src, wide, force, own, table,
    small_sem, chunk_sem, halo_send, halo_got, edge_send, edge_got, src_send, src_got,
    wide_send, wide_got,
):
    width_x, width_y, width_z = shape
    n_x, n_y = (width_x // SUB, width_y // SUB)
    rows = 2 * width_y
    slots = mass.shape[2]
    me_x, me_y = (lax.axis_index("gx"), lax.axis_index("yz"))
    size_x, size_y = (lax.axis_size("gx"), lax.axis_size("yz"))

    def device(a, b):
        return (lax.rem(me_x + a + size_x, size_x), lax.rem(me_y + b + size_y, size_y))

    def remote(source, target, send, receive, where):
        return pltpu.make_async_remote_copy(
            src_ref=source, dst_ref=target, send_sem=send, recv_sem=receive,
            device_id=where, device_id_type=MESH,
        )

    around = wide_pairs(size_y)
    edge_c[...] = jnp.zeros_like(edge_c)
    small = [
        pltpu.make_async_copy(source, target, small_sem.at[k])
        for k, (source, target) in enumerate(
            [
                (shift_hbm, shift), (pos_hbm, pos), (vel_hbm, vel),
                (mass_hbm, mass), (axis_hbm, axis), (occupancy_hbm, occupancy),
            ]
        )
    ]
    chunks = [
        pltpu.make_async_copy(
            solvent_hbm.at[:, pl.ds(i * SUB, SUB)], out.at[:, pl.ds(i * SUB, SUB)], chunk_sem.at[i]
        )
        for i in range(n_x)
    ]
    barrier = pltpu.get_barrier_semaphore()

    def greet(pairs):
        for a, b in pairs:
            pl.semaphore_signal(barrier, inc=1, device_id=device(a, b), device_id_type=MESH)

    for copy in small:
        copy.start()
    greet(around[:8])
    for copy in chunks:
        copy.start()
    greet(around[8:])
    for copy in small[:-1]:
        copy.wait()
    shift_x, shift_y, shift_z = (shift[0], shift[1], shift[2])

    alive = iota((1, slots), 1) < count[0, 0]
    cell_x = (layer_of(pos[0, 0], SUB, width_x) + shift_x) >> 2
    cell_y = (layer_of(pos[1, 0], SUB, width_y) + shift_y) >> 2
    layer_z = layer_of(pos[2, 0], 2.0, width_z)
    cell_z = wrapped(layer_z + shift_z, width_z) >> 1
    place = cell_x * (n_y + 1) + cell_y
    weight = jnp.where(alive, mass[0], 0.0)
    comp = iota((8, slots), 0)
    four = comp & 3
    values = jnp.where(
        four == 0, vel[0, 0] * weight,
        jnp.where(four == 1, vel[1, 0] * weight, jnp.where(four == 2, vel[2, 0] * weight, weight)),
    )
    place_half = place - (comp >> 2)
    place_last = jnp.where(comp < 4, place, -1)
    tiles_y = (n_y + 2) // 2

    def in_tile(i, t):
        return (place_half if 2 * t < n_y else place_last) == i * (n_y + 1) + 2 * t

    spread = [
        jnp.where(in_tile(i, t), values, 0.0) for i in range(n_x + 1) for t in range(tiles_y)
    ]
    near = (wrapped(iota((width_z, slots), 0) + shift_z, width_z) >> 1) == cell_z
    near = near.astype(f32).astype(bf16)
    deposit = sum(
        dot(term, near, ((1,), (1,))) for term in terms(jnp.concatenate(spread, axis=0), 3)[::-1]
    )
    sums[...] = deposit.reshape(n_x + 1, tiles_y * 8, width_z)

    cell_row = wrapped(iota((width_z // 2, width_z), 1) + shift_z, width_z) >> 1
    expand = (cell_row == iota((width_z // 2, width_z), 0)).astype(f32).astype(bf16)
    number = axis[...].reshape(n_x * n_y, width_z // 2).astype(f32).astype(bf16)
    index[...] = dot(number, expand).reshape(n_x, n_y, width_z)

    for c, part in enumerate(axes_of(iota((DIRECTIONS, slots), 0).astype(f32))):
        table[c] = part
    start = stacked([jnp.where(alive, pos[0, 0], far_away), pos[1, 0], pos[2, 0]])
    kick = jnp.broadcast_to((timestep * stiffness * cutoff) / mass[0], (8, slots))
    src[0, OWN] = jnp.where(comp == 3, kick, start * (1.0 / cutoff))

    double = (iota((SUB * rows, SUB * width_y), 0) >> 1 == iota((SUB * rows, SUB * width_y), 1)).astype(bf16)
    small[-1].wait()
    for i in range(n_x):
        at = pl.ds(i * SUB, SUB)
        filled = occupancy[at].reshape(SUB * width_y, width_z).astype(f32).astype(bf16)
        held[at] = dot(double, filled).reshape(SUB, rows, width_z)
    row = iota((8, width_z), 0)
    odd = (row & 1).astype(f32)
    stays_1 = jnp.broadcast_to(shift_x, (8, width_z)) <= 2
    stays_2 = jnp.broadcast_to(shift_x, (8, width_z)) <= 1
    later = ((row >> 1) + shift_y) >= SUB
    even = ((iota((8, width_z), 1) + shift_z) & 1) == 0
    halves = jnp.where((row & 3) == 3, 0.5, 1.0)
    blank = jnp.zeros((8, width_z), f32)

    def finish(i):
        def straddling(c, j):
            now = cell[i, c, pl.ds(8 * j, 8), :] if j < n_y else blank
            before = cell[i, c, pl.ds(8 * (j - 1), 8), :] if j > 0 else blank
            return jnp.where(later, before, now)

        for t in range(tiles_y):
            blocks = [
                straddling(q & 3, 2 * t + (q >> 2)) if 2 * t + (q >> 2) <= n_y else blank
                for q in range(8)
            ]
            tile = fold(blocks) * halves
            partner = jnp.where(even, pltpu.roll(tile, width_z - 1, 1), pltpu.roll(tile, 1, 1))
            sums[i, pl.ds(8 * t, 8), :] += tile + partner

    def gather(i):
        for b in range(n_y):
            at = pl.ds(8 * b, 8)
            filled = [held[i * SUB + r, at, :] for r in range(SUB)]
            live = [f > odd for f in filled]
            for c in range(4):
                v = filled
                if c < 3:
                    v = [jnp.where(live[r], out[c, i * SUB + r, at, :], 0.0) for r in range(SUB)]
                front = v[0] + v[1]
                back = v[3] + v[2]
                stay = jnp.where(stays_1, jnp.where(stays_2, front + v[2], front), v[0])
                move = jnp.where(stays_1, jnp.where(stays_2, v[3], back), back + v[1])
                cell[i, c, at, :] = stay if i == 0 else cell[i, c, at, :] + stay
                cell[i + 1, c, at, :] = move

    for i in range(n_x):
        chunks[i].wait()
        gather(i)
        if i > 0:
            finish(i - 1)
    finish(n_x - 1)
    finish(n_x)

    pl.semaphore_wait(barrier, len(around))

    def exchange(step):
        mine = src.at[step, OWN, pl.ds(0, 4)]
        copies = {}
        for a, b in AROUND:
            k = slot_of(a, b)
            copies[k] = remote(
                mine, src.at[step, 8 - k, pl.ds(0, 4)],
                src_send.at[step, k], src_got.at[step, 8 - k], device(a, b),
            )
            copies[k].start()
        return list(copies.values())

    sends = exchange(0)

    at_low, at_high = (pl.ds(0, 4), pl.ds(n_y * SUB, 4))
    every = pl.ds(0, n_x + 1)
    halo = [
        (sums.at[n_x], halo_x.at[0], (1, 0)),
        (sums.at[0], halo_x.at[1], (-1, 0)),
        (sums.at[every, at_high], halo_y.at[0, every, at_low], (0, 1)),
        (sums.at[every, at_low], halo_y.at[1, every, at_low], (0, -1)),
        (sums.at[n_x, at_high], halo_c.at[0, at_low], (1, 1)),
        (sums.at[n_x, at_low], halo_c.at[1, at_low], (1, -1)),
        (sums.at[0, at_high], halo_c.at[2, at_low], (-1, 1)),
        (sums.at[0, at_low], halo_c.at[3, at_low], (-1, -1)),
    ]
    halo = [
        remote(source, target, halo_send.at[k], halo_got.at[k], device(*where))
        for k, (source, target, where) in enumerate(halo)
    ]
    for copy in halo:
        copy.start()
    edges = [
        (index.at[0], edge_x, (-1, 0)),
        (index.at[pl.ds(0, n_x), 0], edge_y, (0, -1)),
        (index.at[0, pl.ds(0, 1)], edge_c.at[pl.ds(0, 1)], (-1, -1)),
    ]
    edges = [
        remote(source, target, edge_send.at[k], edge_got.at[k], device(*where))
        for k, (source, target, where) in enumerate(edges)
    ]
    for copy in edges:
        copy.start()

    steps = ((width_z // 2) / cutoff, n_x / cutoff, n_y / cutoff)
    columns_x = sides(me_x)
    quick, slow = columns_x[1:]

    def source(step, a, b):
        return reader(src.at[step], slot_of(a, b), a, b, steps)

    def arrived(step, a, b):
        slot = slot_of(a, b)
        remote(
            src.at[step, OWN, pl.ds(0, 4)], src.at[step, slot, pl.ds(0, 4)],
            src_send.at[step, slot], src_got.at[step, slot], device(0, 1),
        ).wait_recv()

    def early_forces(step):
        for b in (-1, 1):
            arrived(step, 0, b)
        force_pass(own, force, [source(step, 0, b) for b in (0, -1, 1)], True)
        for b in (-1, 0, 1):
            arrived(step, quick, b)
        force_pass(own, force, [source(step, quick, b) for b in (-1, 0, 1)], False)

    def late_arrivals(step):
        for b in (-1, 0, 1):
            arrived(step, slow, b)

    def late_forces(step):
        force_pass(own, force, [source(step, slow, b) for b in (-1, 0, 1)], False, True)
        return force_rows(force)

    own_columns(own, src[0, OWN])
    early_forces(0)
    late_arrivals(0)
    for copy in edges + halo:
        copy.wait_recv()
    push = late_forces(0)

    total[...] = sums[...]
    total[0] += halo_x[0]
    total[n_x] += halo_x[1]
    for i in range(n_x + 1):
        total[i, at_low, :] += halo_y[0, i, at_low, :]
        total[i, at_high, :] += halo_y[1, i, at_low, :]
    total[0, at_low, :] += halo_c[0, at_low, :]
    total[0, at_high, :] += halo_c[1, at_low, :]
    total[n_x, at_low, :] += halo_c[2, at_low, :]
    total[n_x, at_high, :] += halo_c[3, at_low, :]

    chosen = (iota((width_z, slots), 0) == layer_z).astype(f32).astype(bf16)
    block = total[...].reshape((n_x + 1) * tiles_y * 8, width_z)
    at_z = sum(dot(term, chosen) for term in terms(block, 2)[::-1])
    picked = jnp.zeros((8, slots), f32)
    for i in range(n_x + 1):
        for t in range(tiles_y):
            n = 8 * (i * tiles_y + t)
            picked = picked + jnp.where(in_tile(i, t), at_z[n : n + 8], 0.0)
    picked = picked + pltpu.roll(picked, 4, 0)
    numbers = jnp.concatenate(
        [index[...].reshape(n_x * n_y, width_z), edge_x[...], edge_y[...], edge_c[...]], axis=0
    )
    at_z = dot(numbers.astype(bf16), chosen)
    wanted = [place - comp == i * (n_y + 1) for i in range(n_x + 1)]
    wanted.append(place - comp * (n_y + 1) == n_y)
    wanted.append(jnp.logical_and(comp == 0, place == n_x * (n_y + 1) + n_y))
    found = jnp.zeros((8, slots), f32)
    for n, mask in enumerate(wanted):
        found = found + jnp.where(mask, at_z[8 * n : 8 * n + 8], 0.0)
    name = jnp.sum(found, axis=0, keepdims=True).astype(jnp.int32)
    heavy = jnp.maximum(picked[3:4], fill_mass)
    mean = [picked[c : c + 1] / heavy for c in range(3)]
    n = []
    for c in range(3):
        hit = [
            jnp.where(iota((8, slots), 0) + 8 * r == name, table[c, pl.ds(8 * r, 8), :], 0.0)
            for r in range(DIRECTIONS // 8)
        ]
        n.append(jnp.sum(sum(hit), axis=0, keepdims=True))
    rel = [vel[c, 0] - mean[c] for c in range(3)]
    cross = [n[1] * rel[2] - n[2] * rel[1], n[2] * rel[0] - n[0] * rel[2], n[0] * rel[1] - n[1] * rel[0]]
    along = n[0] * rel[0] + n[1] * rel[1] + n[2] * rel[2]
    speed = stacked([
        mean[c] + cos_angle * rel[c] + sin_angle * cross[c] + (1.0 - cos_angle) * along * n[c]
        for c in range(3)
    ])
    place_now = start

    def cell_fields(i, rows_of):
        for b in range(n_y):
            pair = [
                [jnp.where(later, total[i, pl.ds(4 * (b + 1) + c, 1), :], total[i, pl.ds(4 * b + c, 1), :])
                 for c in range(4)],
                [jnp.where(later, normals[c, pl.ds(rows_of(b + 1), 1), :], normals[c, pl.ds(rows_of(b), 1), :])
                 for c in range(3)],
            ]
            scale = 1.0 / jnp.maximum(pair[0][3], fill_mass)
            for c in range(3):
                fields[i, b, c] = pair[0][c] * scale
                fields[i, b, 3 + c] = pair[1][c]

    def turn(x, carry):
        at_cell = (x + shift_x) >> 2
        for b in range(n_y):
            at = pl.ds(8 * b, 8)
            mean = [fields[at_cell, b, c] for c in range(3)]
            n = [fields[at_cell, b, 3 + c] for c in range(3)]
            old = [out[c, x, at, :] for c in range(3)]
            rel = [old[c] - mean[c] for c in range(3)]
            along = (1.0 - cos_angle) * (n[0] * rel[0] + n[1] * rel[1] + n[2] * rel[2])
            cross = [
                n[1] * rel[2] - n[2] * rel[1],
                n[2] * rel[0] - n[0] * rel[2],
                n[0] * rel[1] - n[1] * rel[0],
            ]
            live = held[x, at, :] > odd
            for c in range(3):
                new = mean[c] + cos_angle * rel[c] + sin_angle * cross[c] + along * n[c]
                out[c, x, at, :] = jnp.where(live, new, old[c])
        return carry

    def idle_work(step):
        if step == 1:
            for c, part in enumerate(axes_of(numbers)):
                normals[c] = part

            def inner(i, carry):
                cell_fields(i, lambda b: i * n_y + b if b < n_y else n_x * n_y + 8 + i)
                return carry

            lax.fori_loop(0, n_x, inner, 0)
            cell_fields(n_x, lambda b: n_x * n_y + b if b < n_y else n_x * n_y + 16)
            lax.fori_loop(0, width_x // 2, turn, 0)
        if step == 2:
            lax.fori_loop(width_x // 2, width_x, turn, 0)

    speed = speed + push * kick
    place_now = place_now + timestep * speed
    src[1, OWN] = place_now * (1.0 / cutoff)
    sends = sends + exchange(1)
    own_columns(own, src[1, OWN])
    idle_work(1)
    early_forces(1)
    late_arrivals(1)
    push = late_forces(1)

    speed = speed + push * kick
    place_now = place_now + timestep * speed
    def at_wide(a, b):
        return wide_slot(a, b, size_y)

    mine = at_wide(0, 0)
    wide[mine] = place_now * (1.0 / cutoff)
    spread = {}
    for a, b in around:
        k, target = (at_wide(a, b), at_wide(-a, -b))
        spread[a, b] = remote(
            wide.at[mine, pl.ds(0, 4)], wide.at[target, pl.ds(0, 4)],
            wide_send.at[k], wide_got.at[target], device(a, b),
        )
        spread[a, b].start()

    def wide_arrived(a):
        for b in (-1, 0, 1, -2, 2):
            if (isinstance(a, int) and b == 0) or folded(b, size_y) != b:
                continue
            k = at_wide(a, b)
            remote(
                wide.at[mine, pl.ds(0, 4)], wide.at[k, pl.ds(0, 4)],
                wide_send.at[k], wide_got.at[k], device(0, 1),
            ).wait_recv()

    idle_work(2)
    first[...] = src[0]
    second[...] = src[1]
    tiles[0] = place_now
    tiles[1] = speed
    tiles[2] = stacked([pos[c, 0] for c in range(3)])
    tiles[3] = stacked([vel[c, 0] for c in range(3)])
    tiles[4] = jnp.broadcast_to(jnp.where(alive, 1.0, 0.0), (8, slots))
    for copy in sends + halo + edges:
        copy.wait_send()
    for k, a in enumerate(columns_x[:2]):
        wide_arrived(a)
        block = flipped([wide[at_wide(a, b)] for b in (-1, 0, 1)])
        for m in range(3):
            for c in range(3):
                column = block[:, 8 * m + c : 8 * m + c + 1]
                early[3 * k + m, c] = jnp.broadcast_to(column, (slots, slots))
        for m in range(3):
            around_m = [reader(wide, at_wide(a, m - 1 + q), a, q, steps) for q in (-1, 0, 1)]
            force_pass(early.at[m], begun.at[m], around_m, k == 0)
    wide_arrived(slow)
    for a in (-2 * quick, 2 * quick):
        wide_arrived(a)
    third[...] = wide[...]
    for copy in spread.values():
        copy.wait_send()


def finish_kernel(
    shape, turned, first, second, third, tiles, early, begun,
    out, pos_out, vel_out, own, force, later, sums, placed, packed, counts, sem
):
    width_x, width_y, width_z = shape
    n_x, n_y = (width_x // SUB, width_y // SUB)
    slots = first.shape[2]
    size_y = lax.axis_size("yz")
    columns_x = sides(lax.axis_index("gx"))
    copies = []
    for c in range(3):
        copies.append(pltpu.make_async_copy(turned.at[c], out.at[c], sem.at[c]))
        copies[-1].start()

    steps = ((width_z // 2) / cutoff, n_x / cutoff, n_y / cutoff)
    block = 16 if slots % 16 == 0 else 8
    half = slots // 2
    group = [(k, b) for k in range(3) for b in (-1, 0, 1)]

    def at_wide(k, b, p=0):
        return wide_slot(columns_x[k] + p, b, size_y)

    def halves(most, work):
        work(0)
        pl.when(most * block > half)(lambda: work(half))

    def columns(tiles, most):
        sums[...] = flipped(tiles)

        def work(start):
            at = pl.ds(start, half)
            for n in range(len(tiles)):
                for c in range(3):
                    column = sums[at, 8 * n + c : 8 * n + c + 1]
                    own[n, c, at, :] = jnp.broadcast_to(column, (half, slots))

        halves(most, work)

    def pushes(m, columns_of, trips, sources, before=None, moved=None):
        def body(r, carry):
            at = pl.ds(pl.multiple_of(r * block, block), block)
            rows = [columns_of[c, at, :] for c in range(3)]
            if moved is not None:
                rows = [rows[0] + moved[0], rows[1] + moved[1], rows[2]]
            total = None if before is None else [before[c, at, :] for c in range(3)]
            for source in sources:
                parts = pair_sums(rows, source())
                total = parts if total is None else [t + p for t, p in zip(total, parts)]
            for c in range(3):
                force[m, c, at, :] = total[c]
            return carry

        lax.fori_loop(0, trips, body, 0)

    def rows_of(trips):
        lane = iota((half, slots), 1)

        def work(start, group, block):
            at = pl.ds(start, half)
            for n in group:
                for c in range(3):
                    total = jnp.sum(force[n, c, at, :], axis=1, keepdims=True)
                    block = jnp.where(lane == 8 * n + c, total, block)
            sums[at, :] = block

        work(0, range(len(trips)), jnp.zeros((half, slots), f32))
        for n, number in enumerate(trips):
            pl.when(number * block > half)(lambda n=n: work(half, [n], sums[pl.ds(half, half), :]))
        return sums[...].T

    comp = iota((8, slots), 0)
    for a in range(-2, 3):
        for b in range(-2, 3):
            tile = third[wide_slot(a, b, size_y)]
            offset = jnp.where(comp == 0, a * steps[1], jnp.where(comp == 1, b * steps[2], 0.0))
            placed[(a + 2) * 5 + b + 2] = tile + offset
            live = jnp.where(tile[:1] > 0.1 * far_away, 0.0, 1.0)
            counts[(a + 2) * 5 + b + 2] = jnp.sum(live).astype(jnp.int32)

    def at_placed(k, b, p=0):
        return (columns_x[k] + p + 2) * 5 + b + 2

    dead = [third[at_wide(k, b), pl.ds(0, 1), :] > 0.1 * far_away for k, b in group]
    trips = [(counts[at_placed(k, b)] + (block - 1)) // block for k, b in group]
    lane_of = iota((8, slots), 1)

    def pack(n, k, b):
        at = [at_placed(k, b + q, p) for p, q in RING]
        held = [counts[t] for t in at]
        best, which, single = (held[0], 0, at[0])
        for t in range(1, 9):
            larger = held[t] > best
            best = jnp.where(larger, held[t], best)
            which = jnp.where(larger, t, which)
            single = jnp.where(larger, at[t], single)
        for t in range(8):
            held[t] = jnp.where(which == t, held[8], held[t])
            at[t] = jnp.where(which == t, at[8], at[t])
        fits = None
        for t in range(4):
            size = held[2 * t]
            both = jnp.where(
                lane_of < size, placed[at[2 * t]], pltpu.roll(placed[at[2 * t + 1]], size, 1)
            )
            packed[4 * n + t] = both
            fit = size + held[2 * t + 1] <= slots
            fits = fit if fits is None else jnp.logical_and(fits, fit)
        return fits, single

    packs = [pack(n, k, b) for n, (k, b) in enumerate(group[3:])]
    most = functools.reduce(jnp.maximum, trips)
    columns([third[at_wide(2, b)] for b in (-1, 0, 1)], most)
    for m, (k, b) in enumerate(group):
        if k == 0:
            slow = columns_x[2]
            around_m = [reader(third, at_wide(2, b + q), slow, q, steps) for q in (-1, 0, 1)]
            pushes(m, early.at[m], trips[m], around_m, begun.at[m])
        else:
            around_m = [
                reader(third, at_wide(k, b + q, p), p, q, steps) for p in (-1, 0, 1) for q in (-1, 0, 1)
            ]
            own_m = early.at[m] if k == 1 else own.at[m - 6]
            fits, single = packs[m - 3]
            tight = [reader(packed, 4 * (m - 3) + t, 0, 0, steps) for t in range(4)]
            tight.append(reader(placed, single, 0, 0, steps))
            moved = (columns_x[k].astype(f32) * steps[1], b * steps[2])
            pushes(m, own_m, jnp.where(fits, trips[m], 0), tight, None, moved)
            pushes(m, own_m, jnp.where(fits, 0, trips[m]), around_m)
    push = rows_of(trips)
    speed, place = (tiles[1], tiles[0])
    for m, (k, b) in enumerate(group):
        near = slot_of(columns_x[k], b)
        now = third[at_wide(k, b)]
        mine = push[8 * m : 8 * m + 8]
        kick = jnp.broadcast_to(first[near, pl.ds(3, 1), :], (8, slots))
        if (k, b) == (0, 0):
            speed = speed + mine * kick
            place = place + timestep * speed
            moved = place * (1.0 / cutoff)
            own_kick, own_trips = (kick, trips[m])
        else:
            moved = now + (now - second[near]) + (timestep / cutoff) * (mine * kick)
        later[m] = jnp.where(jnp.broadcast_to(dead[m], (8, slots)), now, moved)
    columns([later[1]], own_trips)
    around_m = [reader(later, m, columns_x[k], b, steps) for m, (k, b) in enumerate(group)]
    pushes(0, own.at[0], own_trips, around_m)
    speed = speed + rows_of([own_trips])[:8] * own_kick
    place = place + timestep * speed
    alive = tiles[4] > 0
    place = jnp.where(alive, place, tiles[2])
    speed = jnp.where(alive, speed, tiles[3])
    for c in range(3):
        pos_out[c, 0] = place[c : c + 1]
        vel_out[c, 0] = speed[c : c + 1]
    for copy in copies:
        copy.wait()


def per_device(
    solvent_vel, occupancy, grid_shift, axis_index, colloid_pos, colloid_vel, colloid_mass, colloid_count
):
    shape = occupancy.shape
    width_x, width_y, width_z = shape
    rows = 2 * width_y
    n_x, n_y = (width_x // SUB, width_y // SUB)
    slots = colloid_mass.shape[2]
    solvent = solvent_vel.reshape(3, width_x, rows, width_z)
    smem = pl.BlockSpec(memory_space=pltpu.SMEM)
    vmem = pl.BlockSpec(memory_space=pltpu.VMEM)
    hbm = pl.BlockSpec(memory_space=pltpu.HBM)
    tall = (n_y + 2) // 2 * 8
    dma = pltpu.SemaphoreType.DMA

    def in_hbm(x):
        return pltpu.with_memory_space_constraint(x, pltpu.HBM)

    turned, *states = pl.pallas_call(
        functools.partial(collide_kernel, shape),
        out_shape=[
            pltpu.VMEM(solvent.shape, f32),
            pltpu.VMEM((9, 8, slots), f32),
            pltpu.VMEM((9, 8, slots), f32),
            pltpu.VMEM((25, 8, slots), f32),
            pltpu.VMEM((5, 8, slots), f32),
            pltpu.VMEM((6, 3, slots, slots), f32),
            pltpu.VMEM((3, 3, slots, slots), f32),
        ],
        in_specs=[hbm, smem] + [hbm] * 6,
        out_specs=[vmem] * 7,
        scratch_shapes=[
            pltpu.SMEM(grid_shift.shape, jnp.int32),
            pltpu.VMEM(colloid_pos.shape, f32),
            pltpu.VMEM(colloid_vel.shape, f32),
            pltpu.VMEM(colloid_mass.shape, f32),
            pltpu.VMEM(axis_index.shape, jnp.int32),
            pltpu.VMEM(shape, jnp.int32),
            pltpu.VMEM((width_x, rows, width_z), f32),
            pltpu.VMEM((n_x + 1, 4, rows, width_z), f32),
            pltpu.VMEM((n_x + 1, tall, width_z), f32),
            pltpu.VMEM((n_x + 1, tall, width_z), f32),
            pltpu.VMEM((n_x, n_y, width_z), f32),
            pltpu.VMEM((8, width_z), f32),
            pltpu.VMEM((8, width_z), f32),
            pltpu.VMEM((8, width_z), f32),
            pltpu.VMEM((3, n_x * n_y + 24, width_z), f32),
            pltpu.VMEM((n_x + 1, n_y, 6, 8, width_z), f32),
            pltpu.VMEM((2, tall, width_z), f32),
            pltpu.VMEM((2, n_x + 1, 8, width_z), f32),
            pltpu.VMEM((4, 8, width_z), f32),
            pltpu.VMEM((2, 9, 8, slots), f32),
            pltpu.VMEM((25, 8, slots), f32),
            pltpu.VMEM((3, slots, slots), f32),
            pltpu.VMEM((3, slots, slots), f32),
            pltpu.VMEM((3, DIRECTIONS, slots), f32),
            dma((6,)),
            dma((n_x,)),
            dma((8,)),
            dma((8,)),
            dma((3,)),
            dma((3,)),
            dma((2, 9)),
            dma((2, 9)),
            dma((25,)),
            dma((25,)),
        ],
        compiler_params=pltpu.CompilerParams(
            collective_id=0, has_side_effects=True, vmem_limit_bytes=32 * 2**20
        ),
        name="collide",
    )(
        in_hbm(grid_shift), colloid_count, in_hbm(solvent), in_hbm(occupancy), in_hbm(axis_index),
        in_hbm(colloid_pos), in_hbm(colloid_vel), in_hbm(colloid_mass),
    )

    solvent_out, pos_out, vel_out = pl.pallas_call(
        functools.partial(finish_kernel, shape),
        out_shape=[
            jax.ShapeDtypeStruct(solvent.shape, f32),
            jax.ShapeDtypeStruct(colloid_pos.shape, f32),
            jax.ShapeDtypeStruct(colloid_vel.shape, f32),
        ],
        in_specs=[vmem] * 7,
        out_specs=[hbm, vmem, vmem],
        scratch_shapes=[
            pltpu.VMEM((3, 3, slots, slots), f32),
            pltpu.VMEM((9, 3, slots, slots), f32),
            pltpu.VMEM((9, 8, slots), f32),
            pltpu.VMEM((slots, slots), f32),
            pltpu.VMEM((25, 8, slots), f32),
            pltpu.VMEM((24, 8, slots), f32),
            pltpu.SMEM((25,), jnp.int32),
            dma((3,)),
        ],
        compiler_params=pltpu.CompilerParams(vmem_limit_bytes=16 * 2**20),
        name="finish",
    )(turned, *states)
    return (solvent_out.reshape(solvent_vel.shape), pos_out, vel_out)


def solution(mesh):
    return jax.shard_map(
        per_device,
        mesh=mesh,
        in_specs=(
            P(None, "gx", "yz", None, None),
            P("gx", "yz", None),
            P(),
            P("gx", "yz", None),
            P(None, "gx", "yz", None),
            P(None, "gx", "yz", None),
            P("gx", "yz", None),
            P("gx", "yz"),
        ),
        out_specs=(
            P(None, "gx", "yz", None, None),
            P(None, "gx", "yz", None),
            P(None, "gx", "yz", None),
        ),
        check_vma=False,
    )
```
